8 devices in a mesh: dp: 1 (over z), tp: 8 (over y, x, core).
Axes of the slice: x: 2, y: 2, z: 1, core: 2. Of those that a mesh axis runs over, the one named last changes fastest.
Arguments:
- x_in: bfloat16 [1, 2048, 2560], P('dp', 'tp')
- x_mid: bfloat16 [1, 2048, 2560], P('dp', 'tp')
- d_out: bfloat16 [1, 2048, 2560], P('dp', 'tp')
- q_saved: bfloat16 [1, 2048, 32, 80], P('dp', None, 'tp')
- k_saved: bfloat16 [1, 2048, 32, 80], P('dp', None, 'tp')
- v_saved: bfloat16 [1, 2048, 32, 80], P('dp', None, 'tp')
- z_saved: bfloat16 [1, 2048, 10240], P('dp', None, 'tp')
- ln1_gain: float32 [2560], replicated
- ln1_bias: float32 [2560], replicated
- ln2_gain: float32 [2560], replicated
- ln2_bias: float32 [2560], replicated
- w_qkv: bfloat16 [3, 2560, 32, 80], P(None, None, 'tp')
- w_proj: bfloat16 [32, 80, 2560], P('tp')
- w_fc1: bfloat16 [2560, 10240], P(None, 'tp')
- w_fc2: bfloat16 [10240, 2560], P('tp')
Outputs:
- output 1: bfloat16 [1, 2048, 2560], P('dp', 'tp')
- output 2: float32 [3, 2560, 32, 80], P('dp', None, 'tp')
- output 3: float32 [3, 32, 80], P('dp', 'tp')
- output 4: float32 [32, 80, 2560], P(('dp', 'tp'))
- output 5: float32 [2560, 10240], P('dp', 'tp')
- output 6: float32 [10240], P(('dp', 'tp'))
- output 7: float32 [10240, 2560], P(('dp', 'tp'))
- output 8: float32 [6, 2560], P('dp')
All inputs are finite; a program needn't handle non-finite values.
Results may differ from the reference program's by a relative error of at most 0.0110037.
Values are sent between devices in bfloat16 or wider.
A program may use at most 1 GiB of HBM per device.

```python
import jax
import jax.numpy as jnp
from jax import lax

BATCH_SEQS = 1
SEQ_LEN = 2048
D_MODEL = 2560
N_HEADS = 32
HEAD_DIM = 80
FF_DIM = 10240
LN_EPS = 1e-5
GELU_COEF = 0.044715
GELU_SCALE = 0.7978845608028654


def draw_normal(key, shape, scale):
    return (scale * jax.random.normal(key, shape, jnp.float32)).astype(jnp.bfloat16)


def setup_inputs(seed: int = 0, part: int = 0) -> dict:
    part_keys = jax.random.split(jax.random.fold_in(jax.random.key(seed), part), 7)
    shared_keys = jax.random.split(jax.random.key(seed + 1), 8)
    tok_shape = (BATCH_SEQS, SEQ_LEN, D_MODEL)
    head_shape = (BATCH_SEQS, SEQ_LEN, N_HEADS, HEAD_DIM)
    return {
        'x_in': draw_normal(part_keys[0], tok_shape, 1.0),
        'x_mid': draw_normal(part_keys[1], tok_shape, 1.0),
        'd_out': draw_normal(part_keys[2], tok_shape, 1.0),
        'q_saved': draw_normal(part_keys[3], head_shape, 1.0),
        'k_saved': draw_normal(part_keys[4], head_shape, 1.0),
        'v_saved': draw_normal(part_keys[5], head_shape, 1.0),
        'z_saved': draw_normal(part_keys[6], (BATCH_SEQS, SEQ_LEN, FF_DIM), 1.5),
        'ln1_gain': jax.random.uniform(shared_keys[0], (D_MODEL,), jnp.float32, 0.5, 1.5),
        'ln1_bias': 0.5 * jax.random.normal(shared_keys[1], (D_MODEL,), jnp.float32),
        'ln2_gain': jax.random.uniform(shared_keys[2], (D_MODEL,), jnp.float32, 0.5, 1.5),
        'ln2_bias': 0.5 * jax.random.normal(shared_keys[3], (D_MODEL,), jnp.float32),
        'w_qkv': draw_normal(shared_keys[4], (3, D_MODEL, N_HEADS, HEAD_DIM), D_MODEL ** -0.5),
        'w_proj': draw_normal(shared_keys[5], (N_HEADS, HEAD_DIM, D_MODEL), D_MODEL ** -0.5),
        'w_fc1': draw_normal(shared_keys[6], (D_MODEL, FF_DIM), D_MODEL ** -0.5),
        'w_fc2': draw_normal(shared_keys[7], (FF_DIM, D_MODEL), FF_DIM ** -0.5),
    }


def layer_norm_fwd(token_rows, norm_gain, norm_bias):
    rows_f32 = token_rows.astype(jnp.float32)
    centered = rows_f32 - jnp.mean(rows_f32, axis=-1, keepdims=True)
    inv_std = lax.rsqrt(jnp.mean(centered * centered, axis=-1, keepdims=True) + LN_EPS)
    x_hat = centered * inv_std
    return x_hat, inv_std, (x_hat * norm_gain + norm_bias).astype(jnp.bfloat16)


def layer_norm_bwd(grad_norm, x_hat, inv_std, norm_gain):
    grad_hat = grad_norm * norm_gain
    centered_grad = grad_hat - jnp.mean(grad_hat, axis=-1, keepdims=True)
    return inv_std * (centered_grad - x_hat * jnp.mean(grad_hat * x_hat, axis=-1, keepdims=True))


def gelu_parts(pre_act):
    tanh_val = jnp.tanh(GELU_SCALE * (pre_act + GELU_COEF * pre_act * pre_act * pre_act))
    act_value = 0.5 * pre_act * (1.0 + tanh_val)
    act_slope = 0.5 * (1.0 + tanh_val) + 0.5 * pre_act * (1.0 - tanh_val * tanh_val) * GELU_SCALE * (1.0 + 3.0 * GELU_COEF * pre_act * pre_act)
    return act_value, act_slope


def head_attention_grads(operands):
    q_head, k_head, v_head, dctx_head = operands
    score_scale = HEAD_DIM ** -0.5
    q_wide = q_head.astype(jnp.float32)
    k_wide = k_head.astype(jnp.float32)
    v_wide = v_head.astype(jnp.float32)
    dctx_wide = dctx_head.astype(jnp.float32)
    scores = jnp.einsum('bqe,bke->bqk', q_wide, k_wide) * score_scale
    row_ids = lax.broadcasted_iota(jnp.int32, (SEQ_LEN, SEQ_LEN), 0)
    col_ids = lax.broadcasted_iota(jnp.int32, (SEQ_LEN, SEQ_LEN), 1)
    scores = jnp.where(row_ids >= col_ids, scores, -1e30)
    attn_probs = jax.nn.softmax(scores, axis=-1)
    probs_low = attn_probs.astype(jnp.bfloat16).astype(jnp.float32)
    context = jnp.einsum('bqk,bke->bqe', probs_low, v_wide).astype(jnp.bfloat16)
    grad_probs = jnp.einsum('bqe,bke->bqk', dctx_wide, v_wide)
    grad_scores = attn_probs * (grad_probs - jnp.sum(grad_probs * attn_probs, axis=-1, keepdims=True)) * score_scale
    scores_low = grad_scores.astype(jnp.bfloat16).astype(jnp.float32)
    grad_q = jnp.einsum('bqk,bke->bqe', scores_low, k_wide).astype(jnp.bfloat16)
    grad_k = jnp.einsum('bqk,bqe->bke', scores_low, q_wide).astype(jnp.bfloat16)
    grad_v = jnp.einsum('bqk,bqe->bke', probs_low, dctx_wide).astype(jnp.bfloat16)
    return context, grad_q, grad_k, grad_v


def reference(x_in, x_mid, d_out, q_saved, k_saved, v_saved, z_saved, ln1_gain, ln1_bias, ln2_gain, ln2_bias, w_qkv, w_proj, w_fc1, w_fc2):
    n_tok = BATCH_SEQS * SEQ_LEN
    norm2_hat, norm2_rstd, h2_norm = layer_norm_fwd(x_mid, ln2_gain, ln2_bias)
    act_value, act_slope = gelu_parts(z_saved.astype(jnp.float32))
    dout_rows = d_out.reshape(n_tok, D_MODEL)
    grad_wfc2 = jnp.dot(act_value.astype(jnp.bfloat16).reshape(n_tok, FF_DIM).T, dout_rows, preferred_element_type=jnp.float32)
    grad_act = jnp.dot(dout_rows, w_fc2.T, preferred_element_type=jnp.float32)
    grad_pre = (grad_act * act_slope.reshape(n_tok, FF_DIM)).astype(jnp.bfloat16)
    grad_wfc1 = jnp.dot(h2_norm.reshape(n_tok, D_MODEL).T, grad_pre, preferred_element_type=jnp.float32)
    grad_bfc1 = jnp.sum(grad_pre.astype(jnp.float32), axis=0)
    grad_h2 = jnp.dot(grad_pre, w_fc1.T, preferred_element_type=jnp.float32).reshape(BATCH_SEQS, SEQ_LEN, D_MODEL)
    grad_mid = (d_out.astype(jnp.float32) + layer_norm_bwd(grad_h2, norm2_hat, norm2_rstd, ln2_gain)).astype(jnp.bfloat16)
    mid_rows = grad_mid.reshape(n_tok, D_MODEL)
    grad_ctx = jnp.dot(mid_rows, w_proj.reshape(D_MODEL, D_MODEL).T, preferred_element_type=jnp.float32).astype(jnp.bfloat16)
    grad_ctx = grad_ctx.reshape(BATCH_SEQS, SEQ_LEN, N_HEADS, HEAD_DIM)
    context, grad_q, grad_k, grad_v = lax.map(head_attention_grads, (jnp.moveaxis(q_saved, 2, 0), jnp.moveaxis(k_saved, 2, 0), jnp.moveaxis(v_saved, 2, 0), jnp.moveaxis(grad_ctx, 2, 0)))
    context_rows = jnp.moveaxis(context, 0, 2).reshape(n_tok, D_MODEL)
    grad_wproj = jnp.dot(context_rows.T, mid_rows, preferred_element_type=jnp.float32).reshape(N_HEADS, HEAD_DIM, D_MODEL)
    norm1_hat, norm1_rstd, h1_norm = layer_norm_fwd(x_in, ln1_gain, ln1_bias)
    qkv_rows = jnp.moveaxis(jnp.stack([grad_q, grad_k, grad_v]), 1, 3).reshape(3, n_tok, D_MODEL).astype(jnp.float32)
    grad_wqkv = jnp.einsum('td,ite->ide', h1_norm.reshape(n_tok, D_MODEL).astype(jnp.float32), qkv_rows).reshape(3, D_MODEL, N_HEADS, HEAD_DIM)
    grad_bqkv = jnp.sum(qkv_rows, axis=1).reshape(3, N_HEADS, HEAD_DIM)
    grad_h1 = jnp.einsum('ite,ide->td', qkv_rows, w_qkv.reshape(3, D_MODEL, D_MODEL).astype(jnp.float32)).reshape(BATCH_SEQS, SEQ_LEN, D_MODEL)
    grad_x = (grad_mid.astype(jnp.float32) + layer_norm_bwd(grad_h1, norm1_hat, norm1_rstd, ln1_gain)).astype(jnp.bfloat16)
    grad_vecs = jnp.stack([
        jnp.sum(grad_h1 * norm1_hat, axis=(0, 1)),
        jnp.sum(grad_h1, axis=(0, 1)),
        jnp.sum(grad_h2 * norm2_hat, axis=(0, 1)),
        jnp.sum(grad_h2, axis=(0, 1)),
        jnp.sum(grad_mid.astype(jnp.float32), axis=(0, 1)),
        jnp.sum(d_out.astype(jnp.float32), axis=(0, 1)),
    ])
    return grad_x, grad_wqkv, grad_bqkv, grad_wproj, grad_wfc1, grad_bfc1, grad_wfc2, grad_vecs
```

```python
import jax
import jax.numpy as jnp
from jax import lax
from jax.experimental import pallas as pl
from jax.experimental.pallas import tpu as pltpu
from jax.sharding import PartitionSpec as P

LN_EPS = 1e-5
GELU_COEF = 0.044715
GELU_SCALE = 0.7978845608028654
LOG2E = 1.4426950408889634
BLK = 512
F32 = jnp.float32
BF16 = jnp.bfloat16


def layer_norm_fwd(token_rows, norm_gain, norm_bias):
    rows_f32 = token_rows.astype(F32)
    centered = rows_f32 - jnp.mean(rows_f32, axis=-1, keepdims=True)
    inv_std = lax.rsqrt(jnp.mean(centered * centered, axis=-1, keepdims=True) + LN_EPS)
    x_hat = centered * inv_std
    return x_hat, inv_std, (x_hat * norm_gain + norm_bias).astype(BF16)


def layer_norm_bwd(grad_norm, x_hat, inv_std, norm_gain):
    grad_hat = grad_norm * norm_gain
    centered_grad = grad_hat - jnp.mean(grad_hat, axis=-1, keepdims=True)
    return inv_std * (centered_grad - x_hat * jnp.mean(grad_hat * x_hat, axis=-1, keepdims=True))


def gelu_parts(pre_act):
    tanh_val = jnp.tanh(GELU_SCALE * (pre_act + GELU_COEF * pre_act * pre_act * pre_act))
    act_value = 0.5 * pre_act * (1.0 + tanh_val)
    act_slope = 0.5 * (1.0 + tanh_val) + 0.5 * pre_act * (1.0 - tanh_val * tanh_val) * GELU_SCALE * (1.0 + 3.0 * GELU_COEF * pre_act * pre_act)
    return act_value, act_slope


def dot(a, b):
    return jnp.dot(a, b, preferred_element_type=F32)


def causal_fill(scores, fill):
    key_ids = lax.broadcasted_iota(jnp.int32, scores.shape, 0)
    query_ids = lax.broadcasted_iota(jnp.int32, scores.shape, 1)
    return jnp.where(query_ids >= key_ids, scores, fill)


def attn_fwd_kernel(q_ref, k_ref, v_ref, ctx_ref, wide_ref, max_ref, inv_ref, k_rows, strip):
    qi = pl.program_id(1)
    exp_scale = q_ref.shape[1] ** -0.5 * LOG2E

    @pl.when(qi == 0)
    def _():
        k_rows[...] = k_ref[0].T

    q_blk = q_ref[0]

    def scores(ki):
        rows = k_rows[pl.ds(pl.multiple_of(ki * BLK, BLK), BLK), :]
        return dot(rows, q_blk)

    def score_step(ki, run_max):
        blk = scores(ki)
        strip[pl.ds(pl.multiple_of(ki * BLK, BLK), BLK), :] = blk
        return jnp.maximum(run_max, jnp.max(blk, axis=0, keepdims=True))

    diag = causal_fill(scores(qi), -1e30)
    strip[pl.ds(pl.multiple_of(qi * BLK, BLK), BLK), :] = diag
    row_max = lax.fori_loop(0, qi, score_step, jnp.max(diag, axis=0, keepdims=True))

    def exp_step(ki, run_sum):
        at = pl.ds(pl.multiple_of(ki * BLK, BLK), BLK)
        probs = jnp.exp2((strip[at, :] - row_max) * exp_scale)
        strip[at, :] = probs
        return run_sum + jnp.sum(probs, axis=0, keepdims=True)

    row_inv = 1.0 / lax.fori_loop(0, qi + 1, exp_step, jnp.zeros_like(row_max))

    def ctx_step(ki, carry):
        high, low = carry
        off = pl.multiple_of(ki * BLK, BLK)
        probs = strip[pl.ds(off, BLK), :] * row_inv
        probs_low = probs.astype(BF16)
        rest = (probs - probs_low.astype(F32)).astype(BF16)
        v_blk = v_ref[0, :, pl.ds(off, BLK)]
        return high + dot(v_blk, probs_low), low + dot(v_blk, rest)

    zero = jnp.zeros((q_ref.shape[1], BLK), F32)
    high, low = lax.fori_loop(0, qi + 1, ctx_step, (zero, zero))
    ctx_ref[0] = high.astype(BF16)
    wide_ref[0] = high + low
    max_ref[0] = row_max
    inv_ref[0] = row_inv


def attn_fwd(q_t, k_t, v_t):
    heads, dim, seq = q_t.shape
    whole = pl.BlockSpec((1, dim, seq), lambda h, i: (h, 0, 0))
    part = pl.BlockSpec((1, dim, BLK), lambda h, i: (h, 0, i))
    row = pl.BlockSpec((1, 1, BLK), lambda h, i: (h, 0, i))
    shape = jax.ShapeDtypeStruct
    return pl.pallas_call(
        attn_fwd_kernel,
        grid=(heads, seq // BLK),
        in_specs=[part, whole, whole],
        out_specs=[part, part, row, row],
        out_shape=[shape((heads, dim, seq), BF16), shape((heads, dim, seq), F32),
                   shape((heads, 1, seq), F32), shape((heads, 1, seq), F32)],
        scratch_shapes=[pltpu.VMEM((seq, dim), BF16), pltpu.VMEM((seq, BLK), F32)],
        cost_estimate=pl.CostEstimate(flops=20_000_000_000, bytes_accessed=12_000_000, transcendentals=10_000_000),
        name="attn_fwd",
    )(q_t, k_t, v_t)


def attn_bwd_kernel(qi_tab, ki_tab, q_ref, k_ref, v_ref, do_ref, wide_ref, max_ref, inv_ref, out_ref,
                    k_rows, v_rows, q_rows, do_rows, delta, dq_acc, dk_acc, dv_acc):
    step = pl.program_id(1)
    scale = q_ref.shape[1] ** -0.5
    exp_scale = scale * LOG2E

    @pl.when(step == 0)
    def _():
        k_rows[...] = k_ref[0].T
        v_rows[...] = v_ref[0].T
        q_rows[...] = q_ref[0].T
        do_rows[...] = do_ref[0].T
        delta[...] = jnp.sum(do_ref[0].astype(F32) * wide_ref[0], axis=0, keepdims=True)
        dq_acc[...] = jnp.zeros_like(dq_acc)
        dk_acc[...] = jnp.zeros_like(dk_acc)
        dv_acc[...] = jnp.zeros_like(dv_acc)

    qi, ki = qi_tab[step], ki_tab[step]
    q_at = pl.ds(pl.multiple_of(qi * BLK, BLK), BLK)
    k_at = pl.ds(pl.multiple_of(ki * BLK, BLK), BLK)

    def block(on_diag):
        scores = dot(k_rows[k_at, :], q_ref[0, :, q_at])
        if on_diag:
            scores = causal_fill(scores, -1e30)
        probs = jnp.exp2((scores - max_ref[0, :, q_at]) * exp_scale) * inv_ref[0, :, q_at]
        grad_probs = dot(v_rows[k_at, :], do_ref[0, :, q_at])
        dv_acc[k_at, :] += dot(probs.astype(BF16), do_rows[q_at, :])
        grad_scores = (probs * (grad_probs - delta[:, q_at]) * scale).astype(BF16)
        dk_acc[k_at, :] += dot(grad_scores, q_rows[q_at, :])
        dq_acc[:, q_at] += dot(k_ref[0, :, k_at], grad_scores)

    @pl.when(qi == ki)
    def _():
        block(True)

    @pl.when(qi != ki)
    def _():
        block(False)

    @pl.when(step == pl.num_programs(1) - 1)
    def _():
        out_ref[0, 0] = dq_acc[...].astype(BF16)
        out_ref[1, 0] = dk_acc[...].T.astype(BF16)
        out_ref[2, 0] = dv_acc[...].T.astype(BF16)


def attn_bwd(q_t, k_t, v_t, do_t, wide, row_max, row_inv):
    heads, dim, seq = q_t.shape
    n_blk = seq // BLK
    pairs = [(qi, ki) for ki in range(n_blk) for qi in range(ki, n_blk)]
    qi_tab = jnp.array([p[0] for p in pairs], jnp.int32)
    ki_tab = jnp.array([p[1] for p in pairs], jnp.int32)
    whole = pl.BlockSpec((1, dim, seq), lambda h, s, *_: (h, 0, 0))
    row = pl.BlockSpec((1, 1, seq), lambda h, s, *_: (h, 0, 0))
    rows = pltpu.VMEM((seq, dim), BF16)
    return pl.pallas_call(
        attn_bwd_kernel,
        grid_spec=pltpu.PrefetchScalarGridSpec(
            num_scalar_prefetch=2,
            grid=(heads, len(pairs)),
            in_specs=[whole] * 5 + [row] * 2,
            out_specs=[pl.BlockSpec((3, 1, dim, seq), lambda h, s, *_: (0, h, 0, 0))],
            scratch_shapes=[rows] * 4 + [pltpu.VMEM((1, seq), F32), pltpu.VMEM((dim, seq), F32),
                                         pltpu.VMEM((seq, dim), F32), pltpu.VMEM((seq, dim), F32)],
        ),
        out_shape=[jax.ShapeDtypeStruct((3, heads, dim, seq), BF16)],
        cost_estimate=pl.CostEstimate(flops=40_000_000_000, bytes_accessed=16_000_000, transcendentals=10_000_000),
        name="attn_bwd",
    )(qi_tab, ki_tab, q_t, k_t, v_t, do_t, wide, row_max, row_inv)[0]


def after(value, *others):
    return lax.optimization_barrier((value,) + others)[0]


def solution(mesh):
    def local_backward(x_in, x_mid, d_out, q_saved, k_saved, v_saved, z_saved, ln1_gain, ln1_bias, ln2_gain, ln2_bias, w_qkv, w_proj, w_fc1, w_fc2):
        x_in, x_mid, d_out, z_saved = x_in[0], x_mid[0], d_out[0], z_saved[0]
        heads, dim = q_saved.shape[2:]
        seq, model = z_saved.shape[0], x_in.shape[1]
        gather = lambda v: lax.all_gather(v, 'tp', axis=0, tiled=True)
        scatter = lambda v: lax.psum_scatter(v, 'tp', scatter_dimension=0, tiled=True).astype(F32)

        dout_full = gather(d_out)
        q_t, k_t, v_t = (v[0].transpose(1, 2, 0) for v in (q_saved, k_saved, v_saved))
        ctx_t, wide_t, row_max, row_inv = attn_fwd(q_t, k_t, v_t)
        norm2_hat, norm2_rstd, h2_local = layer_norm_fwd(x_mid, ln2_gain, ln2_bias)
        norm1_hat, norm1_rstd, h1_local = layer_norm_fwd(x_in, ln1_gain, ln1_bias)

        act_value, act_slope = gelu_parts(z_saved.astype(F32))
        grad_pre = (jnp.einsum('sd,fd->sf', dout_full, w_fc2, preferred_element_type=F32) * act_slope).astype(BF16)
        h2_partial = jnp.einsum('sf,df->sd', grad_pre, w_fc1, preferred_element_type=F32).astype(BF16)
        grad_h2 = scatter(h2_partial)
        grad_wfc2 = jnp.einsum('sf,sd->fd', act_value.astype(BF16), dout_full, preferred_element_type=F32)
        grad_bfc1 = jnp.sum(grad_pre, axis=0, dtype=F32)
        grad_mid = (d_out.astype(F32) + layer_norm_bwd(grad_h2, norm2_hat, norm2_rstd, ln2_gain)).astype(BF16)
        mid_full = gather(grad_mid)

        h1_full = gather(after(h1_local, mid_full))
        do_t = jnp.einsum('hed,sd->hes', w_proj, mid_full, preferred_element_type=F32).astype(BF16)
        qkv_t = attn_bwd(q_t, k_t, v_t, do_t, wide_t, row_max, row_inv)
        grad_wproj = jnp.einsum('hes,sd->hed', ctx_t, mid_full, preferred_element_type=F32)
        qkv_rows = qkv_t.reshape(3 * heads * dim, seq)
        w_rows = w_qkv.transpose(0, 2, 3, 1).reshape(3 * heads * dim, model)
        h1_partial = jnp.einsum('fs,fd->sd', qkv_rows, w_rows, preferred_element_type=F32).astype(BF16)
        grad_h1 = scatter(h1_partial)
        grad_wqkv = jnp.einsum('fs,sd->fd', qkv_rows, h1_full, preferred_element_type=F32)
        grad_wqkv = grad_wqkv.reshape(3, heads, dim, model).transpose(0, 3, 1, 2)
        grad_bqkv = jnp.sum(qkv_t, axis=3, dtype=F32)
        h2_full = gather(after(h2_local, h1_partial))
        grad_wfc1 = jnp.einsum('sd,sf->df', h2_full, grad_pre, preferred_element_type=F32)
        grad_x = (grad_mid.astype(F32) + layer_norm_bwd(grad_h1, norm1_hat, norm1_rstd, ln1_gain)).astype(BF16)
        vec_partial = jnp.stack([
            jnp.sum(grad_h1 * norm1_hat, axis=0),
            jnp.sum(grad_h1, axis=0),
            jnp.sum(grad_h2 * norm2_hat, axis=0),
            jnp.sum(grad_h2, axis=0),
            jnp.sum(grad_mid, axis=0, dtype=F32),
            jnp.sum(d_out, axis=0, dtype=F32),
        ])
        grad_vecs = lax.psum(vec_partial, 'tp')
        return grad_x[None], grad_wqkv, grad_bqkv, grad_wproj, grad_wfc1, grad_bfc1, grad_wfc2, grad_vecs

    tok_spec = P('dp', 'tp', None)
    head_spec = P('dp', None, 'tp', None)
    in_specs = (tok_spec, tok_spec, tok_spec, head_spec, head_spec, head_spec, P('dp', None, 'tp'),
                P(None), P(None), P(None), P(None),
                P(None, None, 'tp', None), P('tp', None, None), P(None, 'tp'), P('tp', None))
    out_specs = (tok_spec, P('dp', None, 'tp', None), P('dp', 'tp', None), P(('dp', 'tp'), None, None),
                 P('dp', 'tp'), P(('dp', 'tp')), P(('dp', 'tp'), None), P('dp', None))
    return jax.shard_map(local_backward, mesh=mesh, in_specs=in_specs, out_specs=out_specs, check_vma=False)
```

```python
import jax
import jax.numpy as jnp
from jax import lax
from jax.experimental import pallas as pl
from jax.experimental.pallas import tpu as pltpu
from jax.sharding import PartitionSpec as P

LN_EPS = 1e-5
GELU_COEF = 0.044715
GELU_SCALE = 0.7978845608028654
LOG2E = 1.4426950408889634
BLK = 512
F32 = jnp.float32
BF16 = jnp.bfloat16


def layer_norm_fwd(token_rows, norm_gain, norm_bias):
    rows_f32 = token_rows.astype(F32)
    centered = rows_f32 - jnp.mean(rows_f32, axis=-1, keepdims=True)
    inv_std = lax.rsqrt(jnp.mean(centered * centered, axis=-1, keepdims=True) + LN_EPS)
    x_hat = centered * inv_std
    return x_hat, inv_std, (x_hat * norm_gain + norm_bias).astype(BF16)


def layer_norm_bwd(grad_norm, x_hat, inv_std, norm_gain):
    grad_hat = grad_norm * norm_gain
    centered_grad = grad_hat - jnp.mean(grad_hat, axis=-1, keepdims=True)
    return inv_std * (centered_grad - x_hat * jnp.mean(grad_hat * x_hat, axis=-1, keepdims=True))


def gelu_parts(pre_act):
    tanh_val = jnp.tanh(GELU_SCALE * (pre_act + GELU_COEF * pre_act * pre_act * pre_act))
    act_value = 0.5 * pre_act * (1.0 + tanh_val)
    act_slope = 0.5 * (1.0 + tanh_val) + 0.5 * pre_act * (1.0 - tanh_val * tanh_val) * GELU_SCALE * (1.0 + 3.0 * GELU_COEF * pre_act * pre_act)
    return act_value, act_slope


def dot(a, b):
    return jnp.dot(a, b, preferred_element_type=F32)


def causal_fill(scores, fill):
    key_ids = lax.broadcasted_iota(jnp.int32, scores.shape, 0)
    query_ids = lax.broadcasted_iota(jnp.int32, scores.shape, 1)
    return jnp.where(query_ids >= key_ids, scores, fill)


class Place:
    def __init__(self):
        self.group = lax.axis_index('dp')
        self.me = lax.axis_index('tp')
        self.core = self.me % 2
        self.dx = 2 - 4 * ((self.me // 2) % 2)
        self.dy = 4 - 8 * (self.me // 4)
        self.dc = 1 - 2 * self.core
        self.peer = {'X': self.me + self.dx, 'Y': self.me + self.dy, 'C': self.me + self.dc}
        self.block = {'O': self.me, 'X': self.me + self.dx, 'Y': self.me + self.dy, 'D': self.me + self.dx + self.dy}
        self.pair = {key: val // 2 for key, val in self.block.items()}

    def barrier(self):
        sem = pltpu.get_barrier_semaphore()
        for key in 'XYC':
            pl.semaphore_signal(sem, inc=1, device_id=(self.group, self.peer[key]), device_id_type=pl.DeviceIdType.MESH)
        pl.semaphore_wait(sem, 3)


class Links:
    def __init__(self, place, send_sem, recv_sem):
        self.place, self.send_sem, self.recv_sem = place, send_sem, recv_sem
        self.copies = {}

    def send(self, name, src, dst, to):
        at = len(self.copies)
        copy = pltpu.make_async_remote_copy(
            src_ref=src, dst_ref=dst, send_sem=self.send_sem.at[at], recv_sem=self.recv_sem.at[at],
            device_id=(self.place.group, self.place.peer[to]), device_id_type=pl.DeviceIdType.MESH)
        copy.start()
        self.copies[name] = copy

    def wait(self, *names):
        for name in names:
            self.copies[name].wait_recv()

    def finish(self):
        for copy in self.copies.values():
            copy.wait_send()


class Gather:
    COPIES = 10

    def __init__(self, place, own, full, send_sem, recv_sem):
        self.place, self.own, self.full = place, own, full
        self.links = Links(place, send_sem, recv_sem)
        half = own.shape[0] // 2
        self.first, self.second = pl.ds(0, half), pl.ds(half, half)

    def start(self):
        me, full, own, send = self.place.me, self.full, self.own, self.links.send
        send('Xa', own.at[self.first], full.at[me, self.first], 'X')
        send('Yb', own.at[self.second], full.at[me, self.second], 'Y')
        send('Xb', own.at[self.second], full.at[me, self.second], 'X')
        send('Ya', own.at[self.first], full.at[me, self.first], 'Y')
        send('CO', own, full.at[me], 'C')

    def relay(self):
        links, full, block = self.links, self.full, self.place.block
        links.wait('Xa')
        links.send('Da', full.at[block['X'], self.first], full.at[block['X'], self.first], 'Y')
        links.wait('Yb')
        links.send('Db', full.at[block['Y'], self.second], full.at[block['Y'], self.second], 'X')

    def forward(self, key):
        first, second = ('Xb', None) if key == 'X' else ('Ya', None) if key == 'Y' else ('Da', 'Db')
        self.links.wait(first)
        if second:
            self.links.wait(second)
        slot = self.full.at[self.place.block[key]]
        self.links.send('C' + key, slot, slot, 'C')


class Scatter:
    COPIES = 10

    def __init__(self, place, part, crecv, diag_recv, last_recv, send_sem, recv_sem):
        self.place, self.part, self.crecv = place, part, crecv
        self.diag_recv, self.last_recv = diag_recv, last_recv
        self.links = Links(place, send_sem, recv_sem)
        half = part.shape[1] // 2
        self.half = {'a': pl.ds(0, half), 'b': pl.ds(half, half)}

    def add_rows(self, slot, start, count, other, other_start):
        step = 64

        def body(i, carry):
            here = pl.ds(pl.multiple_of(start + i * step, step), step)
            there = pl.ds(pl.multiple_of(other_start + i * step, step), step)
            total = self.part[slot, here, :].astype(F32) + other[there, :].astype(F32)
            self.part[slot, here, :] = total.astype(BF16)
            return carry

        lax.fori_loop(0, count // step, body, 0)

    def swap(self, key):
        at = 'OXYD'.index(key)
        self.links.send('C' + key, self.part.at[self.place.block[key] + self.place.dc], self.crecv.at[at], 'C')

    def add_pair(self, key):
        self.links.wait('C' + key)
        at = 'OXYD'.index(key)
        self.add_rows(self.place.block[key], 0, self.part.shape[1], self.crecv.at[at], 0)

    def send_half(self, key, half):
        at = self.half[half]
        src = self.part.at[self.place.block[key], at]
        self.links.send(key + half, src, self.last_recv.at['XY'.index(key), at], key)

    def send_diag(self):
        for i, (key, half) in enumerate((('X', 'a'), ('Y', 'b'))):
            src = self.part.at[self.place.block['D'], self.half[half]]
            self.links.send('D' + half, src, self.diag_recv.at[i], key)

    def add_diag(self):
        rows = self.part.shape[1] // 2
        self.links.wait('Da')
        self.add_rows(self.place.block['Y'], 0, rows, self.diag_recv.at[0], 0)
        self.links.wait('Db')
        self.add_rows(self.place.block['X'], rows, rows, self.diag_recv.at[1], 0)
        self.send_half('Y', 'a')
        self.send_half('X', 'b')

    def wait_last(self):
        self.links.wait('Xa', 'Xb', 'Ya', 'Yb', 'CO')

    def run(self, first_half, second_half):
        second_half('D')
        self.swap('D')
        first_half('X')
        self.add_pair('D')
        self.send_diag()
        second_half('X')
        self.swap('X')
        first_half('Y')
        self.add_pair('X')
        self.send_half('X', 'a')
        second_half('Y')
        self.swap('Y')
        first_half('O')
        self.add_pair('Y')
        self.send_half('Y', 'b')
        second_half('O')
        self.swap('O')
        self.add_diag()
        self.wait_last()

    def total(self, at):
        me = self.place.me
        return (self.part[me, at, :].astype(F32) + self.crecv[0, at, :].astype(F32)
                + self.last_recv[0, at, :].astype(F32) + self.last_recv[1, at, :].astype(F32))


def gelu_slope(pre_act):
    tanh_val = jnp.tanh(GELU_SCALE * (pre_act + GELU_COEF * pre_act * pre_act * pre_act))
    return 0.5 * (1.0 + tanh_val) + 0.5 * pre_act * (1.0 - tanh_val * tanh_val) * GELU_SCALE * (1.0 + 3.0 * GELU_COEF * pre_act * pre_act)


def layer_norm_hat(rows_f32):
    centered = rows_f32 - jnp.mean(rows_f32, axis=-1, keepdims=True)
    inv_std = lax.rsqrt(jnp.mean(centered * centered, axis=-1, keepdims=True) + LN_EPS)
    return centered * inv_std, inv_std


LN_ROWS = 32
TILE = 1280
VMEM = pl.BlockSpec(memory_space=pltpu.VMEM)
HBM = pl.BlockSpec(memory_space=pl.ANY)
DMA = pltpu.SemaphoreType.DMA
shape = jax.ShapeDtypeStruct


def tile_at(i, size):
    return pl.ds(pl.multiple_of(i * size, size), size)


def loop(count, body, start=0):
    def step(i, carry):
        body(i)
        return carry

    lax.fori_loop(start, count, step, 0)


def comm_call(kernel, name, ident, flops, args, in_specs, out_shape, out_specs, scratch):
    return pl.pallas_call(
        kernel, in_specs=in_specs, out_specs=out_specs, out_shape=out_shape, scratch_shapes=scratch, name=name,
        compiler_params=pltpu.CompilerParams(collective_id=ident, has_side_effects=True, vmem_limit_bytes=66_000_000),
        cost_estimate=pl.CostEstimate(flops=flops, bytes_accessed=40_000_000, transcendentals=3_000_000),
    )(*args)


def fwd_kernel(dout_ref, q_ref, k_ref, v_ref, dfull, ctx_ref, wide_ref, max_ref, inv_ref, k_rows, strip, own_sem, *comm_sems):
    place = Place()
    place.barrier()
    gather = Gather(place, dout_ref, dfull, *comm_sems)
    gather.start()
    own_copy = pltpu.make_async_copy(dout_ref, dfull.at[place.me], own_sem)
    own_copy.start()
    heads, dim, seq = q_ref.shape
    exp_scale = dim ** -0.5 * LOG2E

    def head(h):
        k_rows[...] = k_ref[h].T

        def query_block(qi):
            q_at = tile_at(qi, BLK)
            q_blk = q_ref[h, :, q_at]

            def score_step(ki, run_max):
                at = tile_at(ki, BLK)
                blk = dot(k_rows[at, :], q_blk)
                strip[at, :] = blk
                return jnp.maximum(run_max, jnp.max(blk, axis=0, keepdims=True))

            diag = causal_fill(dot(k_rows[q_at, :], q_blk), -1e30)
            strip[q_at, :] = diag
            row_max = lax.fori_loop(0, qi, score_step, jnp.max(diag, axis=0, keepdims=True))

            def exp_step(ki, run_sum):
                at = tile_at(ki, BLK)
                probs = jnp.exp2((strip[at, :] - row_max) * exp_scale)
                strip[at, :] = probs
                return run_sum + jnp.sum(probs, axis=0, keepdims=True)

            row_inv = 1.0 / lax.fori_loop(0, qi + 1, exp_step, jnp.zeros_like(row_max))

            def ctx_step(ki, carry):
                high, low = carry
                at = tile_at(ki, BLK)
                probs = strip[at, :] * row_inv
                probs_low = probs.astype(BF16)
                rest = (probs - probs_low.astype(F32)).astype(BF16)
                v_blk = v_ref[h, :, at]
                return high + dot(v_blk, probs_low), low + dot(v_blk, rest)

            zero = jnp.zeros((dim, BLK), F32)
            high, low = lax.fori_loop(0, qi + 1, ctx_step, (zero, zero))
            ctx_ref[h, :, q_at] = high.astype(BF16)
            wide_ref[h, :, q_at] = high + low
            max_ref[h, :, q_at] = row_max
            inv_ref[h, :, q_at] = row_inv

        loop(seq // BLK, query_block)

    for h in range(heads):
        head(h)
        if h == 1:
            gather.relay()
        if h == 2:
            gather.forward('X')
            gather.forward('Y')
    gather.forward('D')
    gather.links.wait('CO', 'CX', 'CY', 'CD')
    own_copy.wait()
    gather.links.finish()


def fwd_call(d_out, q_t, k_t, v_t):
    heads, dim, seq = q_t.shape
    rows, model = d_out.shape
    return comm_call(
        fwd_kernel, "attn_fwd", 0, 40_000_000_000, (d_out, q_t, k_t, v_t), [VMEM] * 4,
        [shape((seq // rows, rows, model), BF16), shape((heads, dim, seq), BF16), shape((heads, dim, seq), F32),
         shape((heads, 1, seq), F32), shape((heads, 1, seq), F32)],
        [HBM] + [VMEM] * 4,
        [pltpu.VMEM((seq, dim), BF16), pltpu.VMEM((seq, BLK), F32), DMA(())] + [DMA((10,))] * 2)


def dot_t(a, b):
    return lax.dot_general(a, b, (((1,), (1,)), ((), ())), preferred_element_type=F32)


def mlp_kernel(dfull, dout_ref, mid_ref, gain_ref, z_ref, w2_ref, w1_ref,
               dx1_ref, dz_ref, gb1_ref, vec_ref,
               w2v, w1v, zv, dzv, ybuf, part, crecv, diag_recv, last_recv,
               load_sem, y_sem, dz_sem, *comm_sems):
    place = Place()
    place.barrier()
    rows, model = dout_ref.shape
    hidden = w2v.shape[0]
    scatter = Scatter(place, part, crecv, diag_recv, last_recv, *comm_sems)

    def load_pair(key):
        copy = pltpu.make_async_copy(dfull.at[pl.ds(2 * place.pair[key], 2)], ybuf.at['DXYO'.index(key) % 2],
                                     y_sem.at['DXYO'.index(key)])
        copy.start()
        return copy

    pairs = {'D': load_pair('D')}
    loads = [pltpu.make_async_copy(src, dst, load_sem.at[i])
             for i, (src, dst) in enumerate(((w2_ref, w2v), (z_ref, zv), (w1_ref, w1v)))]
    for copy in loads:
        copy.start()
    pairs['X'] = load_pair('X')
    gb1_ref[...] = jnp.zeros_like(gb1_ref)
    vec_ref[...] = jnp.zeros_like(vec_ref)
    dz_copies = []

    def grad_act(key):
        slot = 'DXYO'.index(key) % 2
        at = tile_at(place.pair[key], 2 * rows)
        pairs[key].wait()

        def body(n):
            cols = tile_at(n, TILE)
            acc = dot_t(ybuf[slot].reshape(2 * rows, model), w2v[cols, :])
            grad = (acc * gelu_slope(zv[at, cols].astype(F32))).astype(BF16)
            dzv[at, cols] = grad
            gb1_ref[:, cols] += jnp.sum(grad.astype(F32), axis=0, keepdims=True)

        loop(hidden // TILE, body)
        following = {'D': 'Y', 'X': 'O'}.get(key)
        if following:
            pairs[following] = load_pair(following)
        copy = pltpu.make_async_copy(dzv.at[at], dz_ref.at[at], dz_sem.at['DXYO'.index(key)])
        copy.start()
        dz_copies.append(copy)

    def grad_norm(key):
        at = tile_at(place.pair[key], 2 * rows)
        slot = 2 * place.pair[key]

        def body(n):
            cols = tile_at(n, TILE)
            acc = dot_t(dzv[at, :], w1v[cols, :]).astype(BF16)
            part[slot, :, cols] = acc[:rows]
            part[slot + 1, :, cols] = acc[rows:]

        loop(model // TILE, body)

    loads[0].wait()
    loads[1].wait()
    grad_act('D')
    loads[2].wait()
    scatter.run(grad_act, grad_norm)

    gain = gain_ref[...]

    def norm_rows(i):
        at = tile_at(i, LN_ROWS)
        grad = scatter.total(at)
        x_hat, inv_std = layer_norm_hat(mid_ref[at, :].astype(F32))
        dout_rows = dout_ref[at, :].astype(F32)
        mid = (dout_rows + layer_norm_bwd(grad, x_hat, inv_std, gain)).astype(BF16)
        dx1_ref[at, :] = mid
        for row, val in enumerate((grad * x_hat, grad, mid.astype(F32), dout_rows)):
            vec_ref[row:row + 1, :] += jnp.sum(val, axis=0, keepdims=True)

    loop(rows // LN_ROWS, norm_rows)
    for copy in dz_copies:
        copy.wait()
    scatter.links.finish()


def scatter_scratch(rows, model):
    return [pltpu.VMEM((8, rows, model), BF16), pltpu.VMEM((4, rows, model), BF16),
            pltpu.VMEM((2, rows // 2, model), BF16), pltpu.VMEM((2, rows, model), BF16)]


def mlp_call(dfull, d_out, x_mid, ln2_gain, z_saved, w2, w1):
    rows, model = d_out.shape
    seq, hidden = z_saved.shape
    return comm_call(
        mlp_kernel, "mlp_grads", 1, 60_000_000_000, (dfull, d_out, x_mid, ln2_gain[None], z_saved, w2, w1),
        [HBM] + [VMEM] * 3 + [HBM] * 3,
        [shape((rows, model), BF16), shape((seq, hidden), BF16), shape((1, hidden), F32), shape((8, model), F32)],
        [VMEM, HBM, VMEM, VMEM],
        [pltpu.VMEM((hidden, model), BF16), pltpu.VMEM((model, hidden), BF16),
         pltpu.VMEM((seq, hidden), BF16), pltpu.VMEM((seq, hidden), BF16), pltpu.VMEM((2, 2, rows, model), BF16)]
        + scatter_scratch(rows, model) + [DMA((3,)), DMA((4,)), DMA((4,))] + [DMA((10,))] * 2)


def ctx_kernel(dx1_ref, wo_ref, mfull, do_ref, mbuf, own_sem, m_sem, *comm_sems):
    place = Place()
    place.barrier()
    rows, model = dx1_ref.shape
    gather = Gather(place, dx1_ref, mfull, *comm_sems)
    gather.start()
    own_copy = pltpu.make_async_copy(dx1_ref, mfull.at[place.me], own_sem)
    own_copy.start()

    def grad_ctx(key):
        copy = pltpu.make_async_copy(mfull.at[pl.ds(2 * place.pair[key], 2)], mbuf, m_sem.at['OXYD'.index(key)])
        copy.start()
        copy.wait()
        do_ref[:, tile_at(place.pair[key], 2 * rows)] = dot_t(wo_ref[...], mbuf[...].reshape(2 * rows, model)).astype(BF16)

    gather.links.wait('CO')
    own_copy.wait()
    grad_ctx('O')
    gather.relay()
    gather.forward('X')
    gather.forward('Y')
    gather.links.wait('CX')
    grad_ctx('X')
    gather.links.wait('CY')
    grad_ctx('Y')
    gather.forward('D')
    gather.links.wait('CD')
    grad_ctx('D')
    gather.links.finish()


def ctx_call(dx1, w_rows, seq):
    rows, model = dx1.shape
    feats = w_rows.shape[0]
    return comm_call(
        ctx_kernel, "ctx_grads", 2, 8_000_000_000, (dx1, w_rows), [VMEM] * 2,
        [shape((seq // rows, rows, model), BF16), shape((feats, seq), BF16)], [HBM, VMEM],
        [pltpu.VMEM((2, rows, model), BF16), DMA(()), DMA((4,))] + [DMA((10,))] * 2)


def bwd_kernel(h1_ref, h2_ref, q_ref, k_ref, v_ref, do_ref, wide_ref, max_ref, inv_ref,
               h1full, h2full, out_ref,
               k_rows, v_rows, q_rows, do_rows, delta, dq_acc, dk_acc, dv_acc, own_sem, *comm_sems):
    place = Place()
    place.barrier()
    gather1 = Gather(place, h1_ref, h1full, *comm_sems[0:2])
    gather2 = Gather(place, h2_ref, h2full, *comm_sems[2:4])
    gather1.start()
    own_copies = [pltpu.make_async_copy(src, dst.at[place.me], own_sem.at[i])
                  for i, (src, dst) in enumerate(((h1_ref, h1full), (h2_ref, h2full)))]
    for copy in own_copies:
        copy.start()
    heads, dim, seq = q_ref.shape
    blocks = seq // BLK
    scale = dim ** -0.5
    exp_scale = scale * LOG2E

    def head(h):
        k_rows[...] = k_ref[h].T
        v_rows[...] = v_ref[h].T
        q_rows[...] = q_ref[h].T
        do_rows[...] = do_ref[h].T
        delta[...] = jnp.sum(do_ref[h].astype(F32) * wide_ref[h], axis=0, keepdims=True)
        dq_acc[...] = jnp.zeros_like(dq_acc)
        dk_acc[...] = jnp.zeros_like(dk_acc)
        dv_acc[...] = jnp.zeros_like(dv_acc)

        def block(qi, ki, on_diag):
            q_at, k_at = tile_at(qi, BLK), tile_at(ki, BLK)
            scores = dot(k_rows[k_at, :], q_ref[h, :, q_at])
            if on_diag:
                scores = causal_fill(scores, -1e30)
            probs = jnp.exp2((scores - max_ref[h, :, q_at]) * exp_scale) * inv_ref[h, :, q_at]
            grad_probs = dot(v_rows[k_at, :], do_ref[h, :, q_at])
            dv_acc[k_at, :] += dot(probs.astype(BF16), do_rows[q_at, :])
            grad_scores = (probs * (grad_probs - delta[:, q_at]) * scale).astype(BF16)
            dk_acc[k_at, :] += dot(grad_scores, q_rows[q_at, :])
            dq_acc[:, q_at] += dot(k_ref[h, :, k_at], grad_scores)

        loop(blocks, lambda i: block(i, i, True))
        loop(blocks, lambda ki: loop(blocks, lambda qi: block(qi, ki, False), ki + 1))
        out_ref[0, h] = dq_acc[...].astype(BF16)
        out_ref[1, h] = dk_acc[...].T.astype(BF16)
        out_ref[2, h] = dv_acc[...].T.astype(BF16)

    for h in range(heads):
        head(h)
        if h == 0:
            gather1.relay()
            gather2.start()
        if h == 2:
            gather1.forward('X')
            gather1.forward('Y')
    gather1.forward('D')
    gather2.relay()
    gather2.forward('X')
    gather2.forward('Y')
    gather2.forward('D')
    for gather in (gather1, gather2):
        gather.links.wait('CO', 'CX', 'CY', 'CD')
        gather.links.finish()
    for copy in own_copies:
        copy.wait()


def bwd_call(h1, h2, q_t, k_t, v_t, do_t, wide, row_max, row_inv):
    heads, dim, seq = q_t.shape
    rows, model = h1.shape
    full = shape((seq // rows, rows, model), BF16)
    turned = pltpu.VMEM((seq, dim), BF16)
    return comm_call(
        bwd_kernel, "attn_bwd", 3, 60_000_000_000, (h1, h2, q_t, k_t, v_t, do_t, wide, row_max, row_inv), [VMEM] * 9,
        [full, full, shape((3, heads, dim, seq), BF16)], [HBM, HBM, VMEM],
        [turned] * 4 + [pltpu.VMEM((1, seq), F32), pltpu.VMEM((dim, seq), F32), pltpu.VMEM((seq, dim), F32),
                        pltpu.VMEM((seq, dim), F32), DMA((2,))] + [DMA((10,))] * 4)


def qkv_kernel(qkv_ref, w_ref, dx1_ref, x_ref, gain_ref, vec_ref, dx_ref, vsum_ref,
               turned, part, crecv, diag_recv, last_recv, vsend, vrecv, vsem, *comm_sems):
    place = Place()
    place.barrier()
    rows, model = dx1_ref.shape
    scatter = Scatter(place, part, crecv, diag_recv, last_recv, *comm_sems)

    def turn(key):
        turned[...] = qkv_ref[:, tile_at(place.pair[key], 2 * rows)].T

    def grad_norm(key):
        slot = 2 * place.pair[key]

        def body(n):
            cols = tile_at(n, TILE)
            acc = dot(turned[...], w_ref[:, cols]).astype(BF16)
            part[slot, :, cols] = acc[:rows]
            part[slot + 1, :, cols] = acc[rows:]

        loop(model // TILE, body)

    turn('D')
    scatter.run(turn, grad_norm)
    gain = gain_ref[...]
    vsum_ref[...] = vec_ref[...]

    def norm_rows(i):
        at = tile_at(i, LN_ROWS)
        grad = scatter.total(at)
        x_hat, inv_std = layer_norm_hat(x_ref[at, :].astype(F32))
        dx_ref[at, :] = (dx1_ref[at, :].astype(F32) + layer_norm_bwd(grad, x_hat, inv_std, gain)).astype(BF16)
        vsum_ref[4:5, :] += jnp.sum(grad * x_hat, axis=0, keepdims=True)
        vsum_ref[5:6, :] += jnp.sum(grad, axis=0, keepdims=True)

    loop(rows // LN_ROWS, norm_rows)
    for i, key in enumerate('CXY'):
        vsend[i] = vsum_ref[...]
        copy = pltpu.make_async_remote_copy(
            src_ref=vsend.at[i], dst_ref=vrecv.at[i], send_sem=vsem.at[i], recv_sem=vsem.at[3 + i],
            device_id=(place.group, place.peer[key]), device_id_type=pl.DeviceIdType.MESH)
        copy.start()
        copy.wait()
        vsum_ref[...] += vrecv[i]
    scatter.links.finish()


def qkv_call(qkv_rows, w_rows, dx1, x_in, ln1_gain, vec):
    rows, model = dx1.shape
    feats = qkv_rows.shape[0]
    return comm_call(
        qkv_kernel, "qkv_grads", 4, 20_000_000_000, (qkv_rows, w_rows, dx1, x_in, ln1_gain[None], vec), [VMEM] * 6,
        [shape((rows, model), BF16), shape((8, model), F32)], [VMEM] * 2,
        [pltpu.VMEM((2 * rows, feats), BF16)] + scatter_scratch(rows, model)
        + [pltpu.VMEM((3, 8, model), F32), pltpu.VMEM((3, 8, model), F32), DMA((6,))] + [DMA((10,))] * 2)


def solution(mesh):
    def local_backward(x_in, x_mid, d_out, q_saved, k_saved, v_saved, z_saved, ln1_gain, ln1_bias, ln2_gain, ln2_bias, w_qkv, w_proj, w_fc1, w_fc2):
        x_in, x_mid, d_out, z_saved = x_in[0], x_mid[0], d_out[0], z_saved[0]
        heads, dim = q_saved.shape[2:]
        seq, model = z_saved.shape[0], x_in.shape[1]
        q_t, k_t, v_t = (v[0].transpose(1, 2, 0) for v in (q_saved, k_saved, v_saved))
        _, _, h2_local = layer_norm_fwd(x_mid, ln2_gain, ln2_bias)
        _, _, h1_local = layer_norm_fwd(x_in, ln1_gain, ln1_bias)
        dfull, ctx_t, wide_t, row_max, row_inv = fwd_call(d_out, q_t, k_t, v_t)
        dx1, grad_pre, grad_bfc1, vec = mlp_call(dfull, d_out, x_mid, ln2_gain, z_saved, w_fc2, w_fc1)
        mfull, do_t = ctx_call(dx1, w_proj.reshape(heads * dim, model), seq)
        h1_full, h2_full, qkv_t = bwd_call(h1_local, h2_local, q_t, k_t, v_t, do_t.reshape(heads, dim, seq), wide_t, row_max, row_inv)
        dout_full, mid_full, h1_full, h2_full = (v.reshape(seq, model) for v in (dfull, mfull, h1_full, h2_full))
        qkv_rows = qkv_t.reshape(3 * heads * dim, seq)
        w_rows = w_qkv.transpose(0, 2, 3, 1).reshape(3 * heads * dim, model)
        grad_x, vec_sum = qkv_call(qkv_rows, w_rows, dx1, x_in, ln1_gain, vec)
        act_value, _ = gelu_parts(z_saved.astype(F32))
        grad_wfc2 = jnp.einsum('sf,sd->fd', act_value.astype(BF16), dout_full, preferred_element_type=F32)
        grad_wproj = jnp.einsum('hes,sd->hed', ctx_t, mid_full, preferred_element_type=F32)
        grad_wqkv = jnp.einsum('fs,sd->fd', qkv_rows, h1_full, preferred_element_type=F32)
        grad_wqkv = grad_wqkv.reshape(3, heads, dim, model).transpose(0, 3, 1, 2)
        grad_bqkv = jnp.sum(qkv_t, axis=3, dtype=F32)
        grad_wfc1 = jnp.einsum('sd,sf->df', h2_full, grad_pre, preferred_element_type=F32)
        grad_vecs = jnp.concatenate([vec_sum[4:6], vec_sum[:4]])
        return grad_x[None], grad_wqkv, grad_bqkv, grad_wproj, grad_wfc1, grad_bfc1[0], grad_wfc2, grad_vecs

    tok_spec = P('dp', 'tp', None)
    head_spec = P('dp', None, 'tp', None)
    in_specs = (tok_spec, tok_spec, tok_spec, head_spec, head_spec, head_spec, P('dp', None, 'tp'),
                P(None), P(None), P(None), P(None),
                P(None, None, 'tp', None), P('tp', None, None), P(None, 'tp'), P('tp', None))
    out_specs = (tok_spec, P('dp', None, 'tp', None), P('dp', 'tp', None), P(('dp', 'tp'), None, None),
                 P('dp', 'tp'), P(('dp', 'tp')), P(('dp', 'tp'), None), P('dp', None))
    return jax.shard_map(local_backward, mesh=mesh, in_specs=in_specs, out_specs=out_specs, check_vma=False)
```

```python
import jax
import jax.numpy as jnp
from jax import lax
from jax.experimental import pallas as pl
from jax.experimental.pallas import tpu as pltpu
from jax.sharding import PartitionSpec as P

LN_EPS = 1e-5
GELU_COEF = 0.044715
GELU_SCALE = 0.7978845608028654
LOG2E = 1.4426950408889634
BLK = 512
F32 = jnp.float32
BF16 = jnp.bfloat16


def layer_norm_fwd(token_rows, norm_gain, norm_bias):
    rows_f32 = token_rows.astype(F32)
    centered = rows_f32 - jnp.mean(rows_f32, axis=-1, keepdims=True)
    inv_std = lax.rsqrt(jnp.mean(centered * centered, axis=-1, keepdims=True) + LN_EPS)
    x_hat = centered * inv_std
    return x_hat, inv_std, (x_hat * norm_gain + norm_bias).astype(BF16)


def layer_norm_bwd(grad_norm, x_hat, inv_std, norm_gain):
    grad_hat = grad_norm * norm_gain
    centered_grad = grad_hat - jnp.mean(grad_hat, axis=-1, keepdims=True)
    return inv_std * (centered_grad - x_hat * jnp.mean(grad_hat * x_hat, axis=-1, keepdims=True))


def gelu_parts(pre_act):
    tanh_val = jnp.tanh(GELU_SCALE * (pre_act + GELU_COEF * pre_act * pre_act * pre_act))
    act_value = 0.5 * pre_act * (1.0 + tanh_val)
    act_slope = 0.5 * (1.0 + tanh_val) + 0.5 * pre_act * (1.0 - tanh_val * tanh_val) * GELU_SCALE * (1.0 + 3.0 * GELU_COEF * pre_act * pre_act)
    return act_value, act_slope


def dot(a, b):
    return jnp.dot(a, b, preferred_element_type=F32)


def causal_fill(scores, fill):
    key_ids = lax.broadcasted_iota(jnp.int32, scores.shape, 0)
    query_ids = lax.broadcasted_iota(jnp.int32, scores.shape, 1)
    return jnp.where(query_ids >= key_ids, scores, fill)


class Place:
    def __init__(self):
        self.group = lax.axis_index('dp')
        self.me = lax.axis_index('tp')
        self.core = self.me % 2
        self.dx = 2 - 4 * ((self.me // 2) % 2)
        self.dy = 4 - 8 * (self.me // 4)
        self.dc = 1 - 2 * self.core
        self.peer = {'X': self.me + self.dx, 'Y': self.me + self.dy, 'C': self.me + self.dc}
        self.block = {'O': self.me, 'X': self.me + self.dx, 'Y': self.me + self.dy, 'D': self.me + self.dx + self.dy}
        self.pair = {key: val // 2 for key, val in self.block.items()}

    def barrier(self):
        sem = pltpu.get_barrier_semaphore()
        for key in 'XYC':
            pl.semaphore_signal(sem, inc=1, device_id=(self.group, self.peer[key]), device_id_type=pl.DeviceIdType.MESH)
        pl.semaphore_wait(sem, 3)


class Links:
    def __init__(self, place, send_sem, recv_sem):
        self.place, self.send_sem, self.recv_sem = place, send_sem, recv_sem
        self.copies = {}

    def send(self, name, src, dst, to):
        at = len(self.copies)
        copy = pltpu.make_async_remote_copy(
            src_ref=src, dst_ref=dst, send_sem=self.send_sem.at[at], recv_sem=self.recv_sem.at[at],
            device_id=(self.place.group, self.place.peer[to]), device_id_type=pl.DeviceIdType.MESH)
        copy.start()
        self.copies[name] = copy

    def wait(self, *names):
        for name in names:
            self.copies[name].wait_recv()

    def finish(self):
        for copy in self.copies.values():
            copy.wait_send()


class Gather:
    COPIES = 10

    def __init__(self, place, own, full, send_sem, recv_sem):
        self.place, self.own, self.full = place, own, full
        self.links = Links(place, send_sem, recv_sem)
        half = own.shape[0] // 2
        self.first, self.second = pl.ds(0, half), pl.ds(half, half)

    def start(self):
        me, full, own, send = self.place.me, self.full, self.own, self.links.send
        send('Xa', own.at[self.first], full.at[me, self.first], 'X')
        send('Yb', own.at[self.second], full.at[me, self.second], 'Y')
        send('Xb', own.at[self.second], full.at[me, self.second], 'X')
        send('Ya', own.at[self.first], full.at[me, self.first], 'Y')
        send('CO', own, full.at[me], 'C')

    def relay(self):
        links, full, block = self.links, self.full, self.place.block
        links.wait('Xa')
        links.send('Da', full.at[block['X'], self.first], full.at[block['X'], self.first], 'Y')
        links.wait('Yb')
        links.send('Db', full.at[block['Y'], self.second], full.at[block['Y'], self.second], 'X')

    def forward(self, key):
        first, second = ('Xb', None) if key == 'X' else ('Ya', None) if key == 'Y' else ('Da', 'Db')
        self.links.wait(first)
        if second:
            self.links.wait(second)
        slot = self.full.at[self.place.block[key]]
        self.links.send('C' + key, slot, slot, 'C')


class Scatter:
    COPIES = 10

    def __init__(self, place, part, crecv, diag_recv, last_recv, send_sem, recv_sem):
        self.place, self.part, self.crecv = place, part, crecv
        self.diag_recv, self.last_recv = diag_recv, last_recv
        self.links = Links(place, send_sem, recv_sem)
        half = part.shape[1] // 2
        self.half = {'a': pl.ds(0, half), 'b': pl.ds(half, half)}

    def add_rows(self, slot, start, count, other, other_start):
        step = 64

        def body(i, carry):
            here = pl.ds(pl.multiple_of(start + i * step, step), step)
            there = pl.ds(pl.multiple_of(other_start + i * step, step), step)
            total = self.part[slot, here, :].astype(F32) + other[there, :].astype(F32)
            self.part[slot, here, :] = total.astype(BF16)
            return carry

        lax.fori_loop(0, count // step, body, 0)

    def swap(self, key):
        at = 'OXYD'.index(key)
        self.links.send('C' + key, self.part.at[self.place.block[key] + self.place.dc], self.crecv.at[at], 'C')

    def add_pair(self, key):
        self.links.wait('C' + key)
        at = 'OXYD'.index(key)
        self.add_rows(self.place.block[key], 0, self.part.shape[1], self.crecv.at[at], 0)

    def send_half(self, key, half):
        at = self.half[half]
        src = self.part.at[self.place.block[key], at]
        self.links.send(key + half, src, self.last_recv.at['XY'.index(key), at], key)

    def send_diag(self):
        for i, (key, half) in enumerate((('X', 'a'), ('Y', 'b'))):
            src = self.part.at[self.place.block['D'], self.half[half]]
            self.links.send('D' + half, src, self.diag_recv.at[i], key)

    def add_diag(self):
        rows = self.part.shape[1] // 2
        self.links.wait('Da')
        self.add_rows(self.place.block['Y'], 0, rows, self.diag_recv.at[0], 0)
        self.links.wait('Db')
        self.add_rows(self.place.block['X'], rows, rows, self.diag_recv.at[1], 0)
        self.send_half('Y', 'a')
        self.send_half('X', 'b')

    def wait_last(self):
        self.links.wait('Xa', 'Xb', 'Ya', 'Yb', 'CO')

    def run(self, first_half, second_half, early=None, late=None):
        second_half('D')
        self.swap('D')
        first_half('X')
        self.add_pair('D')
        self.send_diag()
        second_half('X')
        self.swap('X')
        first_half('Y')
        self.add_pair('X')
        self.send_half('X', 'a')
        second_half('Y')
        self.swap('Y')
        first_half('O')
        self.add_pair('Y')
        self.send_half('Y', 'b')
        second_half('O')
        self.swap('O')
        if early:
            early()
        self.add_diag()
        if late:
            late()
        self.wait_last()

    def total(self, at):
        me = self.place.me
        return (self.part[me, at, :].astype(F32) + self.crecv[0, at, :].astype(F32)
                + self.last_recv[0, at, :].astype(F32) + self.last_recv[1, at, :].astype(F32))


def gelu_slope(pre_act):
    tanh_val = jnp.tanh(GELU_SCALE * (pre_act + GELU_COEF * pre_act * pre_act * pre_act))
    return 0.5 * (1.0 + tanh_val) + 0.5 * pre_act * (1.0 - tanh_val * tanh_val) * GELU_SCALE * (1.0 + 3.0 * GELU_COEF * pre_act * pre_act)


def layer_norm_hat(rows_f32):
    centered = rows_f32 - jnp.mean(rows_f32, axis=-1, keepdims=True)
    inv_std = lax.rsqrt(jnp.mean(centered * centered, axis=-1, keepdims=True) + LN_EPS)
    return centered * inv_std, inv_std


LN_ROWS = 32
TILE = 1280
VMEM = pl.BlockSpec(memory_space=pltpu.VMEM)
HBM = pl.BlockSpec(memory_space=pl.ANY)
DMA = pltpu.SemaphoreType.DMA
shape = jax.ShapeDtypeStruct


def tile_at(i, size):
    return pl.ds(pl.multiple_of(i * size, size), size)


def loop(count, body, start=0):
    def step(i, carry):
        body(i)
        return carry

    lax.fori_loop(start, count, step, 0)


def comm_call(kernel, name, ident, flops, args, in_specs, out_shape, out_specs, scratch):
    return pl.pallas_call(
        kernel, in_specs=in_specs, out_specs=out_specs, out_shape=out_shape, scratch_shapes=scratch, name=name,
        compiler_params=pltpu.CompilerParams(collective_id=ident, has_side_effects=True, vmem_limit_bytes=66_000_000),
        cost_estimate=pl.CostEstimate(flops=flops, bytes_accessed=40_000_000, transcendentals=3_000_000),
    )(*args)


class Tiles:
    def __init__(self, buf, out, sem, rows=False):
        self.buf, self.out, self.sem, self.rows = buf, out, sem, rows

    def copy(self, n):
        size = self.buf.shape[1 if self.rows else 2]
        at = tile_at(n, size)
        dst = self.out.at[at] if self.rows else self.out.at[:, at]
        return pltpu.make_async_copy(self.buf.at[n % 2], dst, self.sem.at[n % 2])

    def put(self, n, value):
        @pl.when(n >= 2)
        def _():
            self.copy(n - 2).wait()

        self.buf[n % 2] = value()
        self.copy(n).start()

    def finish(self, count):
        self.copy(count - 2).wait()
        self.copy(count - 1).wait()


OUT_TILE = 512


def flat_cols(ref, cols):
    return ref[:, :, cols].reshape(ref.shape[0] * ref.shape[1], OUT_TILE)


def fwd_kernel(dout_ref, q_ref, k_ref, v_ref, dfull, ctx_ref, wide_ref, max_ref, inv_ref, k_rows, strip, own_sem, *comm_sems):
    place = Place()
    place.barrier()
    gather = Gather(place, dout_ref, dfull, *comm_sems)
    gather.start()
    own_copy = pltpu.make_async_copy(dout_ref, dfull.at[place.me], own_sem)
    own_copy.start()
    heads, dim, seq = q_ref.shape
    exp_scale = dim ** -0.5 * LOG2E

    def head(h):
        k_rows[...] = k_ref[h].T

        def query_block(qi):
            q_at = tile_at(qi, BLK)
            q_blk = q_ref[h, :, q_at]

            def score_step(ki, run_max):
                at = tile_at(ki, BLK)
                blk = dot(k_rows[at, :], q_blk)
                strip[at, :] = blk
                return jnp.maximum(run_max, jnp.max(blk, axis=0, keepdims=True))

            diag = causal_fill(dot(k_rows[q_at, :], q_blk), -1e30)
            strip[q_at, :] = diag
            row_max = lax.fori_loop(0, qi, score_step, jnp.max(diag, axis=0, keepdims=True))

            def exp_step(ki, run_sum):
                at = tile_at(ki, BLK)
                probs = jnp.exp2((strip[at, :] - row_max) * exp_scale)
                strip[at, :] = probs
                return run_sum + jnp.sum(probs, axis=0, keepdims=True)

            row_inv = 1.0 / lax.fori_loop(0, qi + 1, exp_step, jnp.zeros_like(row_max))

            def ctx_step(ki, carry):
                high, low = carry
                at = tile_at(ki, BLK)
                probs = strip[at, :] * row_inv
                probs_low = probs.astype(BF16)
                rest = (probs - probs_low.astype(F32)).astype(BF16)
                v_blk = v_ref[h, :, at]
                return high + dot(v_blk, probs_low), low + dot(v_blk, rest)

            zero = jnp.zeros((dim, BLK), F32)
            high, low = lax.fori_loop(0, qi + 1, ctx_step, (zero, zero))
            ctx_ref[h, :, q_at] = high.astype(BF16)
            wide_ref[h, :, q_at] = high + low
            max_ref[h, :, q_at] = row_max
            inv_ref[h, :, q_at] = row_inv

        loop(seq // BLK, query_block)

    for h in range(heads):
        head(h)
        if h == 1:
            gather.relay()
        if h == 2:
            gather.forward('X')
            gather.forward('Y')
    gather.forward('D')
    gather.links.wait('CO', 'CX', 'CY', 'CD')
    own_copy.wait()
    gather.links.finish()


def fwd_call(d_out, q_t, k_t, v_t):
    heads, dim, seq = q_t.shape
    rows, model = d_out.shape
    return comm_call(
        fwd_kernel, "attn_fwd", 0, 40_000_000_000, (d_out, q_t, k_t, v_t), [VMEM] * 4,
        [shape((seq // rows, rows, model), BF16), shape((heads, dim, seq), BF16), shape((heads, dim, seq), F32),
         shape((heads, 1, seq), F32), shape((heads, 1, seq), F32)],
        [HBM] + [VMEM] * 4,
        [pltpu.VMEM((seq, dim), BF16), pltpu.VMEM((seq, BLK), F32), DMA(())] + [DMA((10,))] * 2)


def dot_t(a, b):
    return lax.dot_general(a, b, (((1,), (1,)), ((), ())), preferred_element_type=F32)


def mlp_kernel(dfull, dout_ref, mid_ref, gain_ref, z_ref, w2_ref, w1_ref,
               dx1_ref, dz_ref, gb1_ref, vec_ref,
               w2v, w1v, zv, dzv, ybuf, part, crecv, diag_recv, last_recv,
               load_sem, y_sem, dz_sem, *comm_sems):
    place = Place()
    place.barrier()
    rows, model = dout_ref.shape
    hidden = w2v.shape[0]
    scatter = Scatter(place, part, crecv, diag_recv, last_recv, *comm_sems)

    def load_pair(key):
        copy = pltpu.make_async_copy(dfull.at[pl.ds(2 * place.pair[key], 2)], ybuf.at['DXYO'.index(key) % 2],
                                     y_sem.at['DXYO'.index(key)])
        copy.start()
        return copy

    pairs = {'D': load_pair('D')}
    loads = [pltpu.make_async_copy(src, dst, load_sem.at[i])
             for i, (src, dst) in enumerate(((w2_ref, w2v), (z_ref, zv), (w1_ref, w1v)))]
    for copy in loads:
        copy.start()
    pairs['X'] = load_pair('X')
    gb1_ref[...] = jnp.zeros_like(gb1_ref)
    vec_ref[...] = jnp.zeros_like(vec_ref)
    dz_copies = []

    def grad_act(key):
        slot = 'DXYO'.index(key) % 2
        at = tile_at(place.pair[key], 2 * rows)
        pairs[key].wait()

        def body(n):
            cols = tile_at(n, TILE)
            acc = dot_t(ybuf[slot].reshape(2 * rows, model), w2v[cols, :])
            grad = (acc * gelu_slope(zv[at, cols].astype(F32))).astype(BF16)
            dzv[at, cols] = grad
            gb1_ref[:, cols] += jnp.sum(grad.astype(F32), axis=0, keepdims=True)

        loop(hidden // TILE, body)
        following = {'D': 'Y', 'X': 'O'}.get(key)
        if following:
            pairs[following] = load_pair(following)
        copy = pltpu.make_async_copy(dzv.at[at], dz_ref.at[at], dz_sem.at['DXYO'.index(key)])
        copy.start()
        dz_copies.append(copy)

    def grad_norm(key):
        at = tile_at(place.pair[key], 2 * rows)
        slot = 2 * place.pair[key]

        def body(n):
            cols = tile_at(n, TILE)
            acc = dot_t(dzv[at, :], w1v[cols, :]).astype(BF16)
            part[slot, :, cols] = acc[:rows]
            part[slot + 1, :, cols] = acc[rows:]

        loop(model // TILE, body)

    loads[0].wait()
    loads[1].wait()
    grad_act('D')
    loads[2].wait()
    scatter.run(grad_act, grad_norm)

    gain = gain_ref[...]

    def norm_rows(i):
        at = tile_at(i, LN_ROWS)
        grad = scatter.total(at)
        x_hat, inv_std = layer_norm_hat(mid_ref[at, :].astype(F32))
        dout_rows = dout_ref[at, :].astype(F32)
        mid = (dout_rows + layer_norm_bwd(grad, x_hat, inv_std, gain)).astype(BF16)
        dx1_ref[at, :] = mid
        for row, val in enumerate((grad * x_hat, grad, mid.astype(F32), dout_rows)):
            vec_ref[row:row + 1, :] += jnp.sum(val, axis=0, keepdims=True)

    loop(rows // LN_ROWS, norm_rows)
    for copy in dz_copies:
        copy.wait()
    scatter.links.finish()


def scatter_scratch(rows, model):
    return [pltpu.VMEM((8, rows, model), BF16), pltpu.VMEM((4, rows, model), BF16),
            pltpu.VMEM((2, rows // 2, model), BF16), pltpu.VMEM((2, rows, model), BF16)]


def mlp_call(dfull, d_out, x_mid, ln2_gain, z_saved, w2, w1):
    rows, model = d_out.shape
    seq, hidden = z_saved.shape
    return comm_call(
        mlp_kernel, "mlp_grads", 1, 60_000_000_000, (dfull, d_out, x_mid, ln2_gain[None], z_saved, w2, w1),
        [HBM] + [VMEM] * 3 + [HBM] * 3,
        [shape((rows, model), BF16), shape((seq, hidden), BF16), shape((1, hidden), F32), shape((8, model), F32)],
        [VMEM, HBM, VMEM, VMEM],
        [pltpu.VMEM((hidden, model), BF16), pltpu.VMEM((model, hidden), BF16),
         pltpu.VMEM((seq, hidden), BF16), pltpu.VMEM((seq, hidden), BF16), pltpu.VMEM((2, 2, rows, model), BF16)]
        + scatter_scratch(rows, model) + [DMA((3,)), DMA((4,)), DMA((4,))] + [DMA((10,))] * 2)


def gelu(pre_act):
    return 0.5 * pre_act * (1.0 + jnp.tanh(GELU_SCALE * (pre_act + GELU_COEF * pre_act * pre_act * pre_act)))


def ctx_kernel(dx1_ref, wo_ref, z_ref, dfull, mfull, do_ref, dw2_ref,
               mbuf, zv, ut, yv, obuf, own_sem, m_sem, load_sem, out_sem, *comm_sems):
    place = Place()
    place.barrier()
    rows, model = dx1_ref.shape
    gather = Gather(place, dx1_ref, mfull, *comm_sems)
    gather.start()
    own_copy = pltpu.make_async_copy(dx1_ref, mfull.at[place.me], own_sem)
    own_copy.start()

    def grad_ctx(key):
        copy = pltpu.make_async_copy(mfull.at[pl.ds(2 * place.pair[key], 2)], mbuf, m_sem.at['OXYD'.index(key)])
        copy.start()
        copy.wait()
        do_ref[:, tile_at(place.pair[key], 2 * rows)] = dot_t(wo_ref[...], mbuf[...].reshape(2 * rows, model)).astype(BF16)

    loads = [pltpu.make_async_copy(z_ref, zv, load_sem.at[0]), pltpu.make_async_copy(dfull, yv, load_sem.at[1])]
    for copy in loads:
        copy.start()
    tiles = Tiles(obuf, dw2_ref, out_sem)
    count = model // OUT_TILE

    def turn(n):
        cols = tile_at(n, 256)
        ut[cols, :] = gelu(zv[:, cols].astype(F32)).astype(BF16).T

    def weight_tile(n):
        cols = tile_at(n, OUT_TILE)
        tiles.put(n, lambda: dot(ut[...], flat_cols(yv, cols)))

    loads[0].wait()
    loop(ut.shape[0] // 256, turn)
    gather.links.wait('CO')
    own_copy.wait()
    grad_ctx('O')
    gather.relay()
    loads[1].wait()
    loop(count - 1, weight_tile)
    gather.forward('X')
    gather.forward('Y')
    loop(count, weight_tile, count - 1)
    gather.links.wait('CX')
    grad_ctx('X')
    gather.links.wait('CY')
    grad_ctx('Y')
    gather.forward('D')
    gather.links.wait('CD')
    grad_ctx('D')
    tiles.finish(count)
    gather.links.finish()


def ctx_call(dx1, w_rows, z_saved, dfull):
    rows, model = dx1.shape
    feats = w_rows.shape[0]
    seq, hidden = z_saved.shape
    return comm_call(
        ctx_kernel, "ctx_grads", 2, 30_000_000_000, (dx1, w_rows, z_saved, dfull), [VMEM] * 2 + [HBM] * 2,
        [shape((seq // rows, rows, model), BF16), shape((feats, seq), BF16), shape((hidden, model), F32)], [HBM, VMEM, HBM],
        [pltpu.VMEM((2, rows, model), BF16), pltpu.VMEM((seq, hidden), BF16), pltpu.VMEM((hidden, seq), BF16),
         pltpu.VMEM((seq // rows, rows, model), BF16), pltpu.VMEM((2, hidden, OUT_TILE), F32),
         DMA(()), DMA((4,)), DMA((2,)), DMA((2,))] + [DMA((10,))] * 2)


def bwd_kernel(h1_ref, h2_ref, q_ref, k_ref, v_ref, do_ref, wide_ref, max_ref, inv_ref, ctx_ref, mfull, dz_ref,
               h1full, h2full, out_ref, dwo_ref, dw1_ref,
               k_rows, v_rows, q_rows, do_rows, delta, dq_acc, dk_acc, dv_acc, tok, dzv, obuf, wbuf,
               own_sem, load_sem, out_sem, *comm_sems):
    place = Place()
    place.barrier()
    gather1 = Gather(place, h1_ref, h1full, *comm_sems[0:2])
    gather2 = Gather(place, h2_ref, h2full, *comm_sems[2:4])
    gather2.start()
    own_copies = [pltpu.make_async_copy(src, dst.at[place.me], own_sem.at[i])
                  for i, (src, dst) in enumerate(((h1_ref, h1full), (h2_ref, h2full)))]
    for copy in own_copies:
        copy.start()
    heads, dim, seq = q_ref.shape
    blocks = seq // BLK
    scale = dim ** -0.5
    exp_scale = scale * LOG2E

    def head(h):
        k_rows[...] = k_ref[h].T
        v_rows[...] = v_ref[h].T
        q_rows[...] = q_ref[h].T
        do_rows[...] = do_ref[h].T
        delta[...] = jnp.sum(do_ref[h].astype(F32) * wide_ref[h], axis=0, keepdims=True)
        dq_acc[...] = jnp.zeros_like(dq_acc)
        dk_acc[...] = jnp.zeros_like(dk_acc)
        dv_acc[...] = jnp.zeros_like(dv_acc)

        def block(qi, ki, on_diag):
            q_at, k_at = tile_at(qi, BLK), tile_at(ki, BLK)
            scores = dot(k_rows[k_at, :], q_ref[h, :, q_at])
            if on_diag:
                scores = causal_fill(scores, -1e30)
            probs = jnp.exp2((scores - max_ref[h, :, q_at]) * exp_scale) * inv_ref[h, :, q_at]
            grad_probs = dot(v_rows[k_at, :], do_ref[h, :, q_at])
            dv_acc[k_at, :] += dot(probs.astype(BF16), do_rows[q_at, :])
            grad_scores = (probs * (grad_probs - delta[:, q_at]) * scale).astype(BF16)
            dk_acc[k_at, :] += dot(grad_scores, q_rows[q_at, :])
            dq_acc[:, q_at] += dot(k_ref[h, :, k_at], grad_scores)

        loop(blocks, lambda i: block(i, i, True))
        loop(blocks, lambda ki: loop(blocks, lambda qi: block(qi, ki, False), ki + 1))
        out_ref[0, h] = dq_acc[...].astype(BF16)
        out_ref[1, h] = dk_acc[...].T.astype(BF16)
        out_ref[2, h] = dv_acc[...].T.astype(BF16)

    loads = [pltpu.make_async_copy(mfull, tok, load_sem.at[0]), pltpu.make_async_copy(dz_ref, dzv, load_sem.at[1])]
    for copy in loads:
        copy.start()
    count = tok.shape[2] // OUT_TILE
    tiles_o = Tiles(obuf, dwo_ref, out_sem.at[0])
    tiles_1 = Tiles(wbuf, dw1_ref, out_sem.at[1], rows=True)

    def proj_tile(n):
        cols = tile_at(n, OUT_TILE)
        tiles_o.put(n, lambda: dot(ctx_ref[...], flat_cols(tok, cols)))

    def fc1_tile(n):
        cols = tile_at(n, OUT_TILE)
        tiles_1.put(n, lambda: dot(flat_cols(tok, cols).T, dzv[...]))

    head(0)
    loads[0].wait()
    loop(count, proj_tile)
    gather2.relay()
    gather1.start()
    head(1)
    head(2)
    gather2.forward('X')
    gather2.forward('Y')
    head(3)
    gather2.forward('D')
    own_copies[1].wait()
    gather2.links.wait('CO', 'CX', 'CY', 'CD')
    load = pltpu.make_async_copy(h2full, tok, load_sem.at[2])
    load.start()
    loads[1].wait()
    load.wait()
    loop(count - 2, fc1_tile)
    gather1.relay()
    loop(count, fc1_tile, count - 2)
    gather1.forward('X')
    gather1.forward('Y')
    gather1.forward('D')
    gather1.links.wait('CO', 'CX', 'CY', 'CD')
    own_copies[0].wait()
    tiles_o.finish(count)
    tiles_1.finish(count)
    gather1.links.finish()
    gather2.links.finish()


def bwd_call(h1, h2, q_t, k_t, v_t, do_t, wide, row_max, row_inv, ctx_rows, mfull, dz):
    heads, dim, seq = q_t.shape
    rows, model = h1.shape
    full = shape((seq // rows, rows, model), BF16)
    turned = pltpu.VMEM((seq, dim), BF16)
    hidden = dz.shape[1]
    feats = ctx_rows.shape[0]
    return comm_call(
        bwd_kernel, "attn_bwd", 3, 80_000_000_000,
        (h1, h2, q_t, k_t, v_t, do_t, wide, row_max, row_inv, ctx_rows, mfull, dz), [VMEM] * 10 + [HBM] * 2,
        [full, full, shape((3, heads, dim, seq), BF16), shape((feats, model), F32), shape((model, hidden), F32)],
        [HBM, HBM, VMEM, HBM, HBM],
        [turned] * 4 + [pltpu.VMEM((1, seq), F32), pltpu.VMEM((dim, seq), F32), pltpu.VMEM((seq, dim), F32),
                        pltpu.VMEM((seq, dim), F32), pltpu.VMEM((seq // rows, rows, model), BF16),
                        pltpu.VMEM((seq, hidden), BF16), pltpu.VMEM((2, feats, OUT_TILE), F32),
                        pltpu.VMEM((2, OUT_TILE, hidden), F32), DMA((2,)), DMA((3,)), DMA((2, 2))] + [DMA((10,))] * 4)


def qkv_kernel(qkv_ref, w_ref, dx1_ref, x_ref, gain_ref, vec_ref, h1full, dx_ref, vsum_ref, dw_ref,
               turned, part, crecv, diag_recv, last_recv, vsend, vrecv, tok, obuf, vsem, load_sem, out_sem, *comm_sems):
    place = Place()
    place.barrier()
    rows, model = dx1_ref.shape
    scatter = Scatter(place, part, crecv, diag_recv, last_recv, *comm_sems)

    def turn(key):
        turned[...] = qkv_ref[:, tile_at(place.pair[key], 2 * rows)].T

    def grad_norm(key):
        slot = 2 * place.pair[key]

        def body(n):
            cols = tile_at(n, TILE)
            acc = dot(turned[...], w_ref[:, cols]).astype(BF16)
            part[slot, :, cols] = acc[:rows]
            part[slot + 1, :, cols] = acc[rows:]

        loop(model // TILE, body)

    load = pltpu.make_async_copy(h1full, tok, load_sem)
    load.start()
    tiles = Tiles(obuf, dw_ref, out_sem)
    count = model // OUT_TILE

    def weight_tile(n):
        cols = tile_at(n, OUT_TILE)
        tiles.put(n, lambda: dot(qkv_ref[...], flat_cols(tok, cols)))

    def early_tiles():
        load.wait()
        loop(count - 2, weight_tile)

    def late_tiles():
        loop(count, weight_tile, count - 2)

    turn('D')
    scatter.run(turn, grad_norm, early_tiles, late_tiles)
    tiles.finish(count)
    gain = gain_ref[...]
    vsum_ref[...] = vec_ref[...]

    def norm_rows(i):
        at = tile_at(i, LN_ROWS)
        grad = scatter.total(at)
        x_hat, inv_std = layer_norm_hat(x_ref[at, :].astype(F32))
        dx_ref[at, :] = (dx1_ref[at, :].astype(F32) + layer_norm_bwd(grad, x_hat, inv_std, gain)).astype(BF16)
        vsum_ref[4:5, :] += jnp.sum(grad * x_hat, axis=0, keepdims=True)
        vsum_ref[5:6, :] += jnp.sum(grad, axis=0, keepdims=True)

    loop(rows // LN_ROWS, norm_rows)
    for i, key in enumerate('CXY'):
        vsend[i] = vsum_ref[...]
        copy = pltpu.make_async_remote_copy(
            src_ref=vsend.at[i], dst_ref=vrecv.at[i], send_sem=vsem.at[i], recv_sem=vsem.at[3 + i],
            device_id=(place.group, place.peer[key]), device_id_type=pl.DeviceIdType.MESH)
        copy.start()
        copy.wait()
        vsum_ref[...] += vrecv[i]
    scatter.links.finish()


def qkv_call(qkv_rows, w_rows, dx1, x_in, ln1_gain, vec, h1full):
    rows, model = dx1.shape
    feats = qkv_rows.shape[0]
    return comm_call(
        qkv_kernel, "qkv_grads", 4, 30_000_000_000, (qkv_rows, w_rows, dx1, x_in, ln1_gain[None], vec, h1full), [VMEM] * 6 + [HBM],
        [shape((rows, model), BF16), shape((8, model), F32), shape((feats, model), F32)], [VMEM, VMEM, HBM],
        [pltpu.VMEM((2 * rows, feats), BF16)] + scatter_scratch(rows, model)
        + [pltpu.VMEM((3, 8, model), F32), pltpu.VMEM((3, 8, model), F32), pltpu.VMEM((8, rows, model), BF16),
           pltpu.VMEM((2, feats, OUT_TILE), F32), DMA((6,)), DMA(()), DMA((2,))] + [DMA((10,))] * 2)


def solution(mesh):
    def local_backward(x_in, x_mid, d_out, q_saved, k_saved, v_saved, z_saved, ln1_gain, ln1_bias, ln2_gain, ln2_bias, w_qkv, w_proj, w_fc1, w_fc2):
        x_in, x_mid, d_out, z_saved = x_in[0], x_mid[0], d_out[0], z_saved[0]
        heads, dim = q_saved.shape[2:]
        seq, model = z_saved.shape[0], x_in.shape[1]
        q_t, k_t, v_t = (v[0].transpose(1, 2, 0) for v in (q_saved, k_saved, v_saved))
        _, _, h2_local = layer_norm_fwd(x_mid, ln2_gain, ln2_bias)
        _, _, h1_local = layer_norm_fwd(x_in, ln1_gain, ln1_bias)
        dfull, ctx_t, wide_t, row_max, row_inv = fwd_call(d_out, q_t, k_t, v_t)
        dx1, grad_pre, grad_bfc1, vec = mlp_call(dfull, d_out, x_mid, ln2_gain, z_saved, w_fc2, w_fc1)
        mfull, do_t, grad_wfc2 = ctx_call(dx1, w_proj.reshape(heads * dim, model), z_saved, dfull)
        h1_full, _, qkv_t, grad_wproj, grad_wfc1 = bwd_call(
            h1_local, h2_local, q_t, k_t, v_t, do_t.reshape(heads, dim, seq), wide_t, row_max, row_inv,
            ctx_t.reshape(heads * dim, seq), mfull, grad_pre)
        qkv_rows = qkv_t.reshape(3 * heads * dim, seq)
        w_rows = w_qkv.transpose(0, 2, 3, 1).reshape(3 * heads * dim, model)
        grad_x, vec_sum, grad_wqkv = qkv_call(qkv_rows, w_rows, dx1, x_in, ln1_gain, vec, h1_full)
        grad_wproj = grad_wproj.reshape(heads, dim, model)
        grad_wqkv = grad_wqkv.reshape(3, heads, dim, model).transpose(0, 3, 1, 2)
        grad_bqkv = jnp.sum(qkv_t, axis=3, dtype=F32)
        grad_vecs = jnp.concatenate([vec_sum[4:6], vec_sum[:4]])
        return grad_x[None], grad_wqkv, grad_bqkv, grad_wproj, grad_wfc1, grad_bfc1[0], grad_wfc2, grad_vecs

    tok_spec = P('dp', 'tp', None)
    head_spec = P('dp', None, 'tp', None)
    in_specs = (tok_spec, tok_spec, tok_spec, head_spec, head_spec, head_spec, P('dp', None, 'tp'),
                P(None), P(None), P(None), P(None),
                P(None, None, 'tp', None), P('tp', None, None), P(None, 'tp'), P('tp', None))
    out_specs = (tok_spec, P('dp', None, 'tp', None), P('dp', 'tp', None), P(('dp', 'tp'), None, None),
                 P('dp', 'tp'), P(('dp', 'tp')), P(('dp', 'tp'), None), P('dp', None))
    return jax.shard_map(local_backward, mesh=mesh, in_specs=in_specs, out_specs=out_specs, check_vma=False)
```

```python
import jax
import jax.numpy as jnp
from jax import lax
from jax.experimental import pallas as pl
from jax.experimental.pallas import tpu as pltpu
from jax.sharding import PartitionSpec as P

LN_EPS = 1e-5
GELU_COEF = 0.044715
GELU_SCALE = 0.7978845608028654
LOG2E = 1.4426950408889634
BLK = 512
F32 = jnp.float32
BF16 = jnp.bfloat16


def layer_norm_bwd(grad_norm, x_hat, inv_std, norm_gain):
    grad_hat = grad_norm * norm_gain
    centered_grad = grad_hat - jnp.mean(grad_hat, axis=-1, keepdims=True)
    return inv_std * (centered_grad - x_hat * jnp.mean(grad_hat * x_hat, axis=-1, keepdims=True))


def dot(a, b):
    return jnp.dot(a, b, preferred_element_type=F32)


def causal_fill(scores, fill):
    key_ids = lax.broadcasted_iota(jnp.int32, scores.shape, 0)
    query_ids = lax.broadcasted_iota(jnp.int32, scores.shape, 1)
    return jnp.where(query_ids >= key_ids, scores, fill)


class Place:
    def __init__(self):
        self.group = lax.axis_index('dp')
        self.me = lax.axis_index('tp')
        self.core = self.me % 2
        self.dx = 2 - 4 * ((self.me // 2) % 2)
        self.dy = 4 - 8 * (self.me // 4)
        self.dc = 1 - 2 * self.core
        self.peer = {'X': self.me + self.dx, 'Y': self.me + self.dy, 'C': self.me + self.dc}
        self.block = {'O': self.me, 'X': self.me + self.dx, 'Y': self.me + self.dy, 'D': self.me + self.dx + self.dy}
        self.other = {key: val + self.dc for key, val in self.block.items()}
        self.x, self.y = (self.me // 2) % 2, self.me // 4

    def pair_at(self, i):
        flip_x, flip_y = 1 - i // 2, 1 - i % 2
        return 2 * (self.y + flip_y * (1 - 2 * self.y)) + self.x + flip_x * (1 - 2 * self.x)

    def barrier(self):
        sem = pltpu.get_barrier_semaphore()
        for key in 'XYC':
            pl.semaphore_signal(sem, inc=1, device_id=(self.group, self.peer[key]), device_id_type=pl.DeviceIdType.MESH)
        pl.semaphore_wait(sem, 3)


class Links:
    def __init__(self, place, send_sem, recv_sem):
        self.place, self.send_sem, self.recv_sem = place, send_sem, recv_sem
        self.copies = {}

    def define(self, name, to, src, dst, *index):
        at = len(self.copies)

        def place_of(ref):
            ref, where = ref if isinstance(ref, tuple) else (ref, index)
            return ref.at[where] if where else ref

        def copy():
            return pltpu.make_async_remote_copy(
                src_ref=place_of(src), dst_ref=place_of(dst), send_sem=self.send_sem.at[at], recv_sem=self.recv_sem.at[at],
                device_id=(self.place.group, self.place.peer[to]), device_id_type=pl.DeviceIdType.MESH)

        self.copies[name] = copy

    def start(self, name):
        self.copies[name]().start()

    def send(self, name, *rest):
        self.define(name, *rest)
        self.start(name)

    def wait(self, *names):
        for name in names:
            self.copies[name]().wait_recv()

    def finish(self):
        for copy in self.copies.values():
            copy().wait_send()


class Gather:
    COPIES = 10

    def __init__(self, place, own, full, send_sem, recv_sem):
        self.place, self.own, self.full = place, own, full
        self.links = Links(place, send_sem, recv_sem)
        half = own.shape[0] // 2
        self.first, self.second = pl.ds(0, half), pl.ds(half, half)

    def start(self):
        me, full, own, send = self.place.me, self.full, self.own, self.links.send
        for name, half in (('Xa', self.first), ('Yb', self.second), ('Xb', self.second), ('Ya', self.first)):
            send(name, name[0], (own, (half,)), (full, (me, half)))
        send('CO', 'C', (own, ()), (full, (me,)))

    def relay(self):
        links, full, block = self.links, self.full, self.place.block
        links.wait('Xa')
        links.send('Da', 'Y', full, full, block['X'], self.first)
        links.wait('Yb')
        links.send('Db', 'X', full, full, block['Y'], self.second)

    def forward(self, key):
        first, second = ('Xb', None) if key == 'X' else ('Ya', None) if key == 'Y' else ('Da', 'Db')
        self.links.wait(first)
        if second:
            self.links.wait(second)
        self.links.send('C' + key, 'C', self.full, self.full, self.place.block[key])


class ThirdGather:
    COPIES = 5

    def __init__(self, place, full, send_sem, recv_sem):
        self.place, self.full = place, full
        self.links = Links(place, send_sem, recv_sem)
        half = full.shape[1] // 2
        self.first, self.second = pl.ds(0, half), pl.ds(half, half)

    def start(self, third, own):
        me, full = self.place.me, self.full
        near = {'X': self.first, 'Y': self.second} if third == 0 else {'X': self.second, 'Y': self.first}
        if third == 2:
            block = self.place.block
            near = {'Y': (block['X'], self.first), 'X': (block['Y'], self.second)}
        for key in 'XY':
            if third == 2:
                self.links.send('N' + key, key, full, full, *near[key])
            else:
                src = (full, (me, near[key])) if own is None else (own, (near[key],))
                self.links.send('N' + key, key, src, (full, (me, near[key])))
        if third == 0:
            self.links.send('CO', 'C', (own, ()), (full, (me,)))

    def forward(self, third):
        block = self.place.block
        for key in 'XY':
            self.links.wait('N' + key)
            half = self.first if (third == 0) == (key == 'X') else self.second
            slot = block[key]
            if third == 2:
                slot, half = block['D'], (self.second if key == 'X' else self.first)
            self.links.send('C' + key, 'C', self.full, self.full, slot, half)

    def wait_pair(self, third):
        self.links.wait('CX', 'CY', *(('CO',) if third == 0 else ()))


class Scatter:
    COPIES = 10

    def __init__(self, place, part, crecv, diag_recv, last_recv, send_sem, recv_sem):
        self.place, self.part, self.crecv = place, part, crecv
        self.diag_recv, self.last_recv = diag_recv, last_recv
        self.links = Links(place, send_sem, recv_sem)
        half = part.shape[1] // 2
        self.half = {'a': pl.ds(0, half), 'b': pl.ds(half, half)}
        for at, key in enumerate('OXYD'):
            self.links.define('C' + key, 'C', (part, (place.other[key],)), (crecv, (at,)))

    def add_rows(self, slot, start, count, other, other_start):
        step = 64

        def body(i, carry):
            here = pl.ds(pl.multiple_of(start + i * step, step), step)
            there = pl.ds(pl.multiple_of(other_start + i * step, step), step)
            total = self.part[slot, here, :].astype(F32) + other[there, :].astype(F32)
            self.part[slot, here, :] = total.astype(BF16)
            return carry

        lax.fori_loop(0, count // step, body, 0)

    def swap(self, key):
        self.links.start('C' + key)

    def add_pair(self, key):
        self.links.wait('C' + key)
        at = 'OXYD'.index(key)
        self.add_rows(self.place.block[key], 0, self.part.shape[1], self.crecv.at[at], 0)

    def send_half(self, key, half):
        at = self.half[half]
        self.links.send(key + half, key, (self.part, (self.place.block[key], at)), (self.last_recv, ('XY'.index(key), at)))

    def send_diag(self):
        for i, (key, half) in enumerate((('X', 'a'), ('Y', 'b'))):
            self.links.send('D' + half, key, (self.part, (self.place.block['D'], self.half[half])), (self.diag_recv, (i,)))

    def add_diag(self):
        rows = self.part.shape[1] // 2
        self.links.wait('Da')
        self.add_rows(self.place.block['Y'], 0, rows, self.diag_recv.at[0], 0)
        self.links.wait('Db')
        self.add_rows(self.place.block['X'], rows, rows, self.diag_recv.at[1], 0)
        self.send_half('Y', 'a')
        self.send_half('X', 'b')

    def wait_last(self):
        self.links.wait('Xa', 'Xb', 'Ya', 'Yb', 'CO')

    def between(self, i):
        @pl.when(i == 1)
        def _():
            self.add_pair('D')
            self.send_diag()

        @pl.when(i == 2)
        def _():
            self.add_pair('X')
            self.send_half('X', 'a')

        @pl.when(i == 3)
        def _():
            self.add_pair('Y')
            self.send_half('Y', 'b')

    def after(self, i):
        for at, key in enumerate('DXYO'):
            @pl.when(i == at)
            def _():
                self.swap(key)

    def total(self, at):
        me = self.place.me
        return (self.part[me, at, :].astype(F32) + self.crecv[0, at, :].astype(F32)
                + self.last_recv[0, at, :].astype(F32) + self.last_recv[1, at, :].astype(F32))


def gelu_slope(pre_act):
    tanh_val = jnp.tanh(GELU_SCALE * (pre_act + GELU_COEF * pre_act * pre_act * pre_act))
    return 0.5 * (1.0 + tanh_val) + 0.5 * pre_act * (1.0 - tanh_val * tanh_val) * GELU_SCALE * (1.0 + 3.0 * GELU_COEF * pre_act * pre_act)


def layer_norm_hat(rows_f32):
    centered = rows_f32 - jnp.mean(rows_f32, axis=-1, keepdims=True)
    inv_std = lax.rsqrt(jnp.mean(centered * centered, axis=-1, keepdims=True) + LN_EPS)
    return centered * inv_std, inv_std


LN_ROWS = 32
TILE = 1280
VMEM = pl.BlockSpec(memory_space=pltpu.VMEM)
HBM = pl.BlockSpec(memory_space=pl.ANY)
DMA = pltpu.SemaphoreType.DMA
shape = jax.ShapeDtypeStruct


def tile_at(i, size):
    return pl.ds(pl.multiple_of(i * size, size), size)


def loop(count, body, start=0):
    def step(i, carry):
        body(i)
        return carry

    lax.fori_loop(start, count, step, 0)


def comm_call(kernel, name, ident, flops, args, in_specs, out_shape, out_specs, scratch, aliases={}):
    return pl.pallas_call(
        kernel, in_specs=in_specs, out_specs=out_specs, out_shape=out_shape, scratch_shapes=scratch, name=name,
        input_output_aliases=aliases,
        compiler_params=pltpu.CompilerParams(collective_id=ident, has_side_effects=True, vmem_limit_bytes=66_000_000),
        cost_estimate=pl.CostEstimate(flops=flops, bytes_accessed=40_000_000, transcendentals=3_000_000),
    )(*args)


class Tiles:
    def __init__(self, buf, out, sem, rows=False):
        self.buf, self.out, self.sem, self.rows = buf, out, sem, rows

    def copy(self, n):
        size = self.buf.shape[1 if self.rows else 2]
        at = tile_at(n, size)
        dst = self.out.at[at] if self.rows else self.out.at[:, at]
        return pltpu.make_async_copy(self.buf.at[n % 2], dst, self.sem.at[n % 2])

    def put(self, n, value):
        @pl.when(n >= 2)
        def _():
            self.copy(n - 2).wait()

        self.buf[n % 2] = value()
        self.copy(n).start()

    def finish(self, count):
        self.copy(count - 2).wait()
        self.copy(count - 1).wait()


OUT_TILE = 512


def flat_cols(ref, cols):
    return ref[:, :, cols].reshape(ref.shape[0] * ref.shape[1], OUT_TILE)


def fwd_kernel(dout_ref, q_ref, k_ref, v_ref, x_ref, mid_ref, affine_ref,
               dfull, ctx_ref, wide_ref, max_ref, inv_ref, h1_ref, h2_ref, k_rows, strip, own_sem, *comm_sems):
    place = Place()
    place.barrier()
    gather = Gather(place, dout_ref, dfull, *comm_sems)
    gather.start()
    own_copy = pltpu.make_async_copy(dout_ref, dfull.at[place.me], own_sem)
    own_copy.start()
    heads, dim, seq = q_ref.shape
    exp_scale = dim ** -0.5 * LOG2E
    affine = affine_ref[...]

    def norm_rows(i):
        at = tile_at(i, LN_ROWS)
        for row, (src, dst) in enumerate(((x_ref, h1_ref), (mid_ref, h2_ref))):
            x_hat, _ = layer_norm_hat(src[at, :].astype(F32))
            dst[at, :] = (x_hat * affine[2 * row:2 * row + 1] + affine[2 * row + 1:2 * row + 2]).astype(BF16)

    loop(x_ref.shape[0] // LN_ROWS, norm_rows)

    def head(h):
        k_rows[...] = k_ref[h].T

        def query_block(qi):
            q_at = tile_at(qi, BLK)
            q_blk = q_ref[h, :, q_at]

            def score_step(ki, run_max):
                at = tile_at(ki, BLK)
                blk = dot(k_rows[at, :], q_blk)
                strip[at, :] = blk
                return jnp.maximum(run_max, jnp.max(blk, axis=0, keepdims=True))

            diag = causal_fill(dot(k_rows[q_at, :], q_blk), -1e30)
            strip[q_at, :] = diag
            row_max = lax.fori_loop(0, qi, score_step, jnp.max(diag, axis=0, keepdims=True))

            def exp_step(ki, run_sum):
                at = tile_at(ki, BLK)
                probs = jnp.exp2((strip[at, :] - row_max) * exp_scale)
                strip[at, :] = probs
                return run_sum + jnp.sum(probs, axis=0, keepdims=True)

            row_inv = 1.0 / lax.fori_loop(0, qi + 1, exp_step, jnp.zeros_like(row_max))

            def ctx_step(ki, carry):
                high, low = carry
                at = tile_at(ki, BLK)
                probs = strip[at, :] * row_inv
                probs_low = probs.astype(BF16)
                rest = (probs - probs_low.astype(F32)).astype(BF16)
                v_blk = v_ref[h, :, at]
                return high + dot(v_blk, probs_low), low + dot(v_blk, rest)

            zero = jnp.zeros((dim, BLK), F32)
            high, low = lax.fori_loop(0, qi + 1, ctx_step, (zero, zero))
            ctx_ref[h, :, q_at] = high.astype(BF16)
            wide_ref[h, :, q_at] = high + low
            max_ref[h, :, q_at] = row_max
            inv_ref[h, :, q_at] = row_inv

        loop(seq // BLK, query_block)

    def head_step(h):
        head(h)

        @pl.when(h == 1)
        def _():
            gather.relay()

        @pl.when(h == 2)
        def _():
            gather.forward('X')
            gather.forward('Y')

    loop(heads, head_step)
    gather.forward('D')
    gather.links.wait('CO', 'CX', 'CY', 'CD')
    own_copy.wait()
    gather.links.finish()


def fwd_call(d_out, q_t, k_t, v_t, x_in, x_mid, affine):
    heads, dim, seq = q_t.shape
    rows, model = d_out.shape
    return comm_call(
        fwd_kernel, "attn_fwd", 0, 40_000_000_000, (d_out, q_t, k_t, v_t, x_in, x_mid, affine), [VMEM] * 7,
        [shape((seq // rows, rows, model), BF16), shape((heads, dim, seq), BF16), shape((heads, dim, seq), F32),
         shape((heads, 1, seq), F32), shape((heads, 1, seq), F32), shape((rows, model), BF16), shape((rows, model), BF16)],
        [HBM] + [VMEM] * 6,
        [pltpu.VMEM((seq, dim), BF16), pltpu.VMEM((seq, BLK), F32), DMA(())] + [DMA((10,))] * 2)


def dot_t(a, b):
    return lax.dot_general(a, b, (((1,), (1,)), ((), ())), preferred_element_type=F32)


def mlp_kernel(dfull, dout_ref, mid_ref, affine_ref, h1_ref, z_ref, w2_ref, w1_ref,
               dx1_ref, dz_ref, gb1_ref, vec_ref, h1full,
               w2v, w1v, zv, dzv, ybuf, part, crecv, diag_recv, last_recv,
               load_sem, y_sem, dz_sem, own_sem, *comm_sems):
    place = Place()
    place.barrier()
    rows, model = dout_ref.shape
    hidden = w2v.shape[0]
    scatter = Scatter(place, part, crecv, diag_recv, last_recv, *comm_sems[0:2])
    gather = ThirdGather(place, h1full, *comm_sems[2:4])
    gather.start(0, h1_ref)
    own_copy = pltpu.make_async_copy(h1_ref, h1full.at[place.me], own_sem)

    def load_pair(i):
        return pltpu.make_async_copy(dfull.at[pl.ds(2 * place.pair_at(i), 2)], ybuf.at[i % 2], y_sem.at[i])

    def store_grad(i):
        at = tile_at(place.pair_at(i), 2 * rows)
        return pltpu.make_async_copy(dzv.at[at], dz_ref.at[at], dz_sem.at[i])

    load_pair(0).start()
    loads = [pltpu.make_async_copy(src, dst, load_sem.at[i])
             for i, (src, dst) in enumerate(((w2_ref, w2v), (z_ref, zv), (w1_ref, w1v)))]
    for copy in loads:
        copy.start()
    load_pair(1).start()
    own_copy.start()
    gb1_ref[...] = jnp.zeros_like(gb1_ref)
    vec_ref[...] = jnp.zeros_like(vec_ref)
    loads[0].wait()
    loads[1].wait()

    def pair_step(i):
        slot = i % 2
        pair = place.pair_at(i)
        at = tile_at(pair, 2 * rows)
        load_pair(i).wait()

        def grad_act(n):
            cols = tile_at(n, TILE)
            acc = dot_t(ybuf[slot].reshape(2 * rows, model), w2v[cols, :])
            grad = (acc * gelu_slope(zv[at, cols].astype(F32))).astype(BF16)
            dzv[at, cols] = grad
            gb1_ref[:, cols] += jnp.sum(grad.astype(F32), axis=0, keepdims=True)

        loop(hidden // TILE, grad_act)
        store_grad(i).start()

        @pl.when(i < 2)
        def _():
            load_pair(i + 2).start()

        @pl.when(i == 0)
        def _():
            loads[2].wait()

        @pl.when(i == 2)
        def _():
            gather.forward(0)

        scatter.between(i)

        def grad_norm(n):
            cols = tile_at(n, TILE)
            acc = dot_t(dzv[at, :], w1v[cols, :]).astype(BF16)
            part[2 * pair, :, cols] = acc[:rows]
            part[2 * pair + 1, :, cols] = acc[rows:]

        loop(model // TILE, grad_norm)
        scatter.after(i)

    loop(4, pair_step)
    scatter.add_diag()
    scatter.wait_last()

    gain = affine_ref[2:3, :]

    def norm_rows(i):
        at = tile_at(i, LN_ROWS)
        grad = scatter.total(at)
        x_hat, inv_std = layer_norm_hat(mid_ref[at, :].astype(F32))
        dout_rows = dout_ref[at, :].astype(F32)
        mid = (dout_rows + layer_norm_bwd(grad, x_hat, inv_std, gain)).astype(BF16)
        dx1_ref[at, :] = mid
        for row, val in enumerate((grad * x_hat, grad, mid.astype(F32), dout_rows)):
            vec_ref[row + 2:row + 3, :] += jnp.sum(val, axis=0, keepdims=True)

    loop(rows // LN_ROWS, norm_rows)
    for i in range(4):
        store_grad(i).wait()
    own_copy.wait()
    gather.wait_pair(0)
    gather.links.finish()
    scatter.links.finish()


def scatter_scratch(rows, model):
    return [pltpu.VMEM((8, rows, model), BF16), pltpu.VMEM((4, rows, model), BF16),
            pltpu.VMEM((2, rows // 2, model), BF16), pltpu.VMEM((2, rows, model), BF16)]


def mlp_call(dfull, d_out, x_mid, affine, h1, z_saved, w2, w1):
    rows, model = d_out.shape
    seq, hidden = z_saved.shape
    return comm_call(
        mlp_kernel, "mlp_grads", 1, 60_000_000_000, (dfull, d_out, x_mid, affine, h1, z_saved, w2, w1),
        [HBM] + [VMEM] * 3 + [HBM] * 4,
        [shape((rows, model), BF16), shape((seq, hidden), BF16), shape((1, hidden), F32), shape((8, model), F32),
         shape(dfull.shape, BF16)],
        [VMEM, HBM, VMEM, VMEM, HBM],
        [pltpu.VMEM((hidden, model), BF16), pltpu.VMEM((model, hidden), BF16),
         pltpu.VMEM((seq, hidden), BF16), pltpu.VMEM((seq, hidden), BF16), pltpu.VMEM((2, 2, rows, model), BF16)]
        + scatter_scratch(rows, model) + [DMA((3,)), DMA((4,)), DMA((4,)), DMA(())] + [DMA((10,))] * 2 + [DMA((5,))] * 2)


def gelu(pre_act):
    return 0.5 * pre_act * (1.0 + jnp.tanh(GELU_SCALE * (pre_act + GELU_COEF * pre_act * pre_act * pre_act)))


def ctx_kernel(dx1_ref, wo_ref, z_ref, dfull, mfull, do_ref, dw2_ref,
               mbuf, zv, ut, yv, obuf, own_sem, m_sem, load_sem, out_sem, *comm_sems):
    place = Place()
    place.barrier()
    rows, model = dx1_ref.shape
    gather = Gather(place, dx1_ref, mfull, *comm_sems)
    gather.start()
    own_copy = pltpu.make_async_copy(dx1_ref, mfull.at[place.me], own_sem)
    own_copy.start()

    loads = [pltpu.make_async_copy(z_ref, zv, load_sem.at[0]), pltpu.make_async_copy(dfull, yv, load_sem.at[1])]
    for copy in loads:
        copy.start()
    tiles = Tiles(obuf, dw2_ref, out_sem)
    count = model // OUT_TILE

    def turn(n):
        cols = tile_at(n, 256)
        ut[cols, :] = gelu(zv[:, cols].astype(F32)).astype(BF16).T

    def weight_tile(n):
        cols = tile_at(n, OUT_TILE)
        tiles.put(n, lambda: dot(ut[...], flat_cols(yv, cols)))

    loads[0].wait()
    loop(ut.shape[0] // 256, turn)
    gather.relay()
    loads[1].wait()
    loop(count, weight_tile)
    gather.forward('X')
    gather.forward('Y')
    own_copy.wait()
    gather.links.wait('CO')

    def grad_ctx(i):
        @pl.when(i == 1)
        def _():
            gather.links.wait('CY')

        @pl.when(i == 2)
        def _():
            gather.links.wait('CX')

        @pl.when(i == 3)
        def _():
            gather.forward('D')
            gather.links.wait('CD')

        pair = place.pair_at(3 - i)
        copy = pltpu.make_async_copy(mfull.at[pl.ds(2 * pair, 2)], mbuf, m_sem)
        copy.start()
        copy.wait()
        do_ref[:, tile_at(pair, 2 * rows)] = dot_t(wo_ref[...], mbuf[...].reshape(2 * rows, model)).astype(BF16)

    loop(4, grad_ctx)
    tiles.finish(count)
    gather.links.finish()


def ctx_call(dx1, w_rows, z_saved, dfull):
    rows, model = dx1.shape
    feats = w_rows.shape[0]
    seq, hidden = z_saved.shape
    return comm_call(
        ctx_kernel, "ctx_grads", 2, 30_000_000_000, (dx1, w_rows, z_saved, dfull), [VMEM] * 2 + [HBM] * 2,
        [shape((seq // rows, rows, model), BF16), shape((feats, seq), BF16), shape((hidden, model), F32)], [HBM, VMEM, HBM],
        [pltpu.VMEM((2, rows, model), BF16), pltpu.VMEM((seq, hidden), BF16), pltpu.VMEM((hidden, seq), BF16),
         pltpu.VMEM((seq // rows, rows, model), BF16), pltpu.VMEM((2, hidden, OUT_TILE), F32),
         DMA(()), DMA(()), DMA((2,)), DMA((2,))] + [DMA((10,))] * 2)


def bwd_kernel(h2_ref, q_ref, k_ref, v_ref, do_ref, wide_ref, max_ref, inv_ref, dz_ref, h1_in,
               h1full, h2full, out_ref, dw1_ref,
               k_rows, v_rows, q_rows, do_rows, delta, dq_acc, dk_acc, dv_acc, tok, dzv, wbuf,
               own_sem, load_sem, out_sem, *comm_sems):
    place = Place()
    place.barrier()
    gather1 = ThirdGather(place, h1full, *comm_sems[0:2])
    gather2 = Gather(place, h2_ref, h2full, *comm_sems[2:4])
    gather2.start()
    own_copy = pltpu.make_async_copy(h2_ref, h2full.at[place.me], own_sem)
    own_copy.start()
    heads, dim, seq = q_ref.shape
    blocks = seq // BLK
    scale = dim ** -0.5
    exp_scale = scale * LOG2E

    def head(h):
        k_rows[...] = k_ref[h].T
        v_rows[...] = v_ref[h].T
        q_rows[...] = q_ref[h].T
        do_rows[...] = do_ref[h].T
        delta[...] = jnp.sum(do_ref[h].astype(F32) * wide_ref[h], axis=0, keepdims=True)
        dq_acc[...] = jnp.zeros_like(dq_acc)
        dk_acc[...] = jnp.zeros_like(dk_acc)
        dv_acc[...] = jnp.zeros_like(dv_acc)

        def block(qi, ki, on_diag):
            q_at, k_at = tile_at(qi, BLK), tile_at(ki, BLK)
            scores = dot(k_rows[k_at, :], q_ref[h, :, q_at])
            if on_diag:
                scores = causal_fill(scores, -1e30)
            probs = jnp.exp2((scores - max_ref[h, :, q_at]) * exp_scale) * inv_ref[h, :, q_at]
            grad_probs = dot(v_rows[k_at, :], do_ref[h, :, q_at])
            dv_acc[k_at, :] += dot(probs.astype(BF16), do_rows[q_at, :])
            grad_scores = (probs * (grad_probs - delta[:, q_at]) * scale).astype(BF16)
            dk_acc[k_at, :] += dot(grad_scores, q_rows[q_at, :])
            dq_acc[:, q_at] += dot(k_ref[h, :, k_at], grad_scores)

        loop(blocks, lambda i: block(i, i, True))
        loop(blocks, lambda ki: loop(blocks, lambda qi: block(qi, ki, False), ki + 1))
        out_ref[0, h] = dq_acc[...].astype(BF16)
        out_ref[1, h] = dk_acc[...].T.astype(BF16)
        out_ref[2, h] = dv_acc[...].T.astype(BF16)

    load_grad = pltpu.make_async_copy(dz_ref, dzv, load_sem.at[0])
    load_grad.start()
    count = tok.shape[2] // OUT_TILE
    tiles = Tiles(wbuf, dw1_ref, out_sem, rows=True)

    def fc1_tile(n):
        cols = tile_at(n, OUT_TILE)
        tiles.put(n, lambda: dot(flat_cols(tok, cols).T, dzv[...]))

    def head_step(h):
        head(h)

        @pl.when(h == 1)
        def _():
            gather2.relay()
            gather1.start(1, None)

        @pl.when(h == 2)
        def _():
            gather2.forward('X')
            gather2.forward('Y')

    loop(heads, head_step)
    gather2.forward('D')
    own_copy.wait()
    gather2.links.wait('CO', 'CX', 'CY', 'CD')
    load = pltpu.make_async_copy(h2full, tok, load_sem.at[1])
    load.start()
    load_grad.wait()
    load.wait()
    loop(count, fc1_tile)
    gather1.forward(1)
    gather1.wait_pair(1)
    tiles.finish(count)
    gather1.links.finish()
    gather2.links.finish()


def bwd_call(h2, q_t, k_t, v_t, do_t, wide, row_max, row_inv, dz, h1full):
    heads, dim, seq = q_t.shape
    rows, model = h2.shape
    full = shape((seq // rows, rows, model), BF16)
    turned = pltpu.VMEM((seq, dim), BF16)
    hidden = dz.shape[1]
    return comm_call(
        bwd_kernel, "attn_bwd", 3, 80_000_000_000,
        (h2, q_t, k_t, v_t, do_t, wide, row_max, row_inv, dz, h1full), [VMEM] * 8 + [HBM] * 2,
        [full, full, shape((3, heads, dim, seq), BF16), shape((model, hidden), F32)], [HBM, HBM, VMEM, HBM],
        [turned] * 4 + [pltpu.VMEM((1, seq), F32), pltpu.VMEM((dim, seq), F32), pltpu.VMEM((seq, dim), F32),
                        pltpu.VMEM((seq, dim), F32), pltpu.VMEM((seq // rows, rows, model), BF16),
                        pltpu.VMEM((seq, hidden), BF16), pltpu.VMEM((2, OUT_TILE, hidden), F32),
                        DMA(()), DMA((2,)), DMA((2,))] + [DMA((5,))] * 2 + [DMA((10,))] * 2,
        aliases={9: 0})


def qkv_kernel(qkv_ref, w_ref, dx1_ref, x_ref, affine_ref, vec_ref, ctx_ref, mfull, h1_in,
               dx_ref, vsum_ref, bias_ref, dwo_ref, dw_ref, h1full,
               turned, part, crecv, diag_recv, last_recv, vacc, vsend, vrecv, last_send, last_got, tok, obuf, wbuf,
               vsem, load_sem, out_sem, *comm_sems):
    place = Place()
    place.barrier()
    rows, model = dx1_ref.shape
    scatter = Scatter(place, part, crecv, diag_recv, last_recv, *comm_sems[0:2])
    gather = ThirdGather(place, h1full, *comm_sems[2:4])
    gather.start(2, None)
    loads = [pltpu.make_async_copy(src, tok, load_sem.at[i]) for i, src in enumerate((mfull, h1full))]
    loads[0].start()
    tiles_o = Tiles(obuf, dwo_ref, out_sem.at[0])
    tiles = Tiles(wbuf, dw_ref, out_sem.at[1])
    count = model // OUT_TILE
    swaps = Links(place, vsem.at[0], vsem.at[1])

    def vec_step(i):
        if i > 0:
            swaps.wait('CXY'[i - 1])
            vacc[...] += vrecv[i - 1]
        if i < 3:
            vsend[i] = vacc[...]

    def vec_send(i):
        swaps.send('CXY'[i], 'CXY'[i], vsend, vrecv, i)

    vacc[...] = vec_ref[...]
    vec_step(0)

    def pair_step(i):
        pair = place.pair_at(i)
        turned[...] = qkv_ref[:, tile_at(pair, 2 * rows)].T

        @pl.when(i == 3)
        def _():
            gather.forward(2)

        for at in range(3):
            @pl.when(i == at)
            def _():
                vec_send(at)

        scatter.between(i)

        def grad_norm(n):
            cols = tile_at(n, TILE)
            acc = dot(turned[...], w_ref[:, cols]).astype(BF16)
            part[2 * pair, :, cols] = acc[:rows]
            part[2 * pair + 1, :, cols] = acc[rows:]

        loop(model // TILE, grad_norm)
        scatter.after(i)

        for at in range(3):
            @pl.when(i == at)
            def _():
                vec_step(at + 1)

    loop(4, pair_step)
    loads[0].wait()

    def proj_tile(n):
        cols = tile_at(n, OUT_TILE)
        tiles_o.put(n, lambda: dot(ctx_ref[...], flat_cols(tok, cols)))

    def qkv_tile(n):
        cols = tile_at(n, OUT_TILE)
        tiles.put(n, lambda: dot(qkv_ref[...], flat_cols(tok, cols)))

    loop(count, proj_tile)
    scatter.add_diag()
    gather.wait_pair(2)
    loads[1].start()
    ones = jnp.ones((8, qkv_ref.shape[1]), BF16)
    bias_ref[...] = dot_t(ones, qkv_ref[...])
    loads[1].wait()
    loop(count, qkv_tile)
    scatter.wait_last()
    gain = affine_ref[0:1, :]

    def norm_rows(i):
        at = tile_at(i, LN_ROWS)
        grad = scatter.total(at)
        x_hat, inv_std = layer_norm_hat(x_ref[at, :].astype(F32))
        dx_ref[at, :] = (dx1_ref[at, :].astype(F32) + layer_norm_bwd(grad, x_hat, inv_std, gain)).astype(BF16)
        vacc[0:1, :] += jnp.sum(grad * x_hat, axis=0, keepdims=True)
        vacc[1:2, :] += jnp.sum(grad, axis=0, keepdims=True)

    loop(rows // LN_ROWS, norm_rows)
    finals = Links(place, vsem.at[2], vsem.at[3])
    total = vacc[0:2, :]
    for i, key in enumerate('CXY'):
        last_send[i] = total
        finals.send(key, key, last_send, last_got, i)
        if i == 0:
            tiles_o.finish(count)
            tiles.finish(count)
        finals.wait(key)
        total = total + last_got[i]
    vsum_ref[0:2, :] = total
    vsum_ref[2:6, :] = vacc[2:6, :]
    for links in (swaps, finals, scatter.links, gather.links):
        links.finish()


def qkv_call(qkv_rows, w_rows, dx1, x_in, affine, vec, ctx_rows, mfull, h1full):
    rows, model = dx1.shape
    feats, seq = qkv_rows.shape
    proj = ctx_rows.shape[0]
    return comm_call(
        qkv_kernel, "qkv_grads", 4, 30_000_000_000,
        (qkv_rows, w_rows, dx1, x_in, affine, vec, ctx_rows, mfull, h1full), [VMEM] * 7 + [HBM] * 2,
        [shape((rows, model), BF16), shape((6, model), F32), shape((8, feats), F32), shape((proj, model), F32),
         shape((feats, model), F32), shape(h1full.shape, BF16)],
        [VMEM] * 3 + [HBM] * 3,
        [pltpu.VMEM((2 * rows, feats), BF16)] + scatter_scratch(rows, model)
        + [pltpu.VMEM((8, model), F32), pltpu.VMEM((3, 8, model), F32), pltpu.VMEM((3, 8, model), F32),
           pltpu.VMEM((3, 2, model), F32), pltpu.VMEM((3, 2, model), F32), pltpu.VMEM((8, rows, model), BF16),
           pltpu.VMEM((2, proj, OUT_TILE), F32), pltpu.VMEM((2, feats, OUT_TILE), F32),
           DMA((4, 3)), DMA((2,)), DMA((2, 2))] + [DMA((10,))] * 2 + [DMA((5,))] * 2,
        aliases={8: 5})


def solution(mesh):
    def local_backward(x_in, x_mid, d_out, q_saved, k_saved, v_saved, z_saved, ln1_gain, ln1_bias, ln2_gain, ln2_bias, w_qkv, w_proj, w_fc1, w_fc2):
        x_in, x_mid, d_out, z_saved = x_in[0], x_mid[0], d_out[0], z_saved[0]
        heads, dim = q_saved.shape[2:]
        seq, model = z_saved.shape[0], x_in.shape[1]
        q_t, k_t, v_t = (v[0].transpose(1, 2, 0) for v in (q_saved, k_saved, v_saved))
        affine = jnp.stack([ln1_gain, ln1_bias, ln2_gain, ln2_bias])
        dfull, ctx_t, wide_t, row_max, row_inv, h1_local, h2_local = fwd_call(d_out, q_t, k_t, v_t, x_in, x_mid, affine)
        dx1, grad_pre, grad_bfc1, vec, h1_full = mlp_call(dfull, d_out, x_mid, affine, h1_local, z_saved, w_fc2, w_fc1)
        mfull, do_t, grad_wfc2 = ctx_call(dx1, w_proj.reshape(heads * dim, model), z_saved, dfull)
        h1_full, _, qkv_t, grad_wfc1 = bwd_call(
            h2_local, q_t, k_t, v_t, do_t.reshape(heads, dim, seq), wide_t, row_max, row_inv, grad_pre, h1_full)
        qkv_rows = qkv_t.reshape(3 * heads * dim, seq)
        w_rows = w_qkv.transpose(0, 2, 3, 1).reshape(3 * heads * dim, model)
        grad_x, grad_vecs, bias_rows, grad_wproj, grad_wqkv, _ = qkv_call(
            qkv_rows, w_rows, dx1, x_in, affine, vec, ctx_t.reshape(heads * dim, seq), mfull, h1_full)
        grad_wproj = grad_wproj.reshape(heads, dim, model)
        grad_wqkv = grad_wqkv.reshape(3, heads, dim, model).transpose(0, 3, 1, 2)
        grad_bqkv = bias_rows[0].reshape(3, heads, dim)
        return grad_x[None], grad_wqkv, grad_bqkv, grad_wproj, grad_wfc1, grad_bfc1[0], grad_wfc2, grad_vecs

    tok_spec = P('dp', 'tp', None)
    head_spec = P('dp', None, 'tp', None)
    in_specs = (tok_spec, tok_spec, tok_spec, head_spec, head_spec, head_spec, P('dp', None, 'tp'),
                P(None), P(None), P(None), P(None),
                P(None, None, 'tp', None), P('tp', None, None), P(None, 'tp'), P('tp', None))
    out_specs = (tok_spec, P('dp', None, 'tp', None), P('dp', 'tp', None), P(('dp', 'tp'), None, None),
                 P('dp', 'tp'), P(('dp', 'tp')), P(('dp', 'tp'), None), P('dp', None))
    return jax.shard_map(local_backward, mesh=mesh, in_specs=in_specs, out_specs=out_specs, check_vma=False)
```

```python
import jax
import jax.numpy as jnp
from jax import lax
from jax.experimental import pallas as pl
from jax.experimental.pallas import tpu as pltpu
from jax.sharding import PartitionSpec as P

LN_EPS = 1e-5
GELU_COEF = 0.044715
GELU_SCALE = 0.7978845608028654
LOG2E = 1.4426950408889634
BLK = 512
F32 = jnp.float32
BF16 = jnp.bfloat16


def layer_norm_bwd(grad_norm, x_hat, inv_std, norm_gain):
    grad_hat = grad_norm * norm_gain
    centered_grad = grad_hat - jnp.mean(grad_hat, axis=-1, keepdims=True)
    return inv_std * (centered_grad - x_hat * jnp.mean(grad_hat * x_hat, axis=-1, keepdims=True))


def dot(a, b):
    return jnp.dot(a, b, preferred_element_type=F32)


def causal_fill(scores, fill):
    key_ids = lax.broadcasted_iota(jnp.int32, scores.shape, 0)
    query_ids = lax.broadcasted_iota(jnp.int32, scores.shape, 1)
    return jnp.where(query_ids >= key_ids, scores, fill)


class Place:
    def __init__(self):
        self.group = lax.axis_index('dp')
        self.me = lax.axis_index('tp')
        self.core = self.me % 2
        self.dx = 2 - 4 * ((self.me // 2) % 2)
        self.dy = 4 - 8 * (self.me // 4)
        self.dc = 1 - 2 * self.core
        self.peer = {'X': self.me + self.dx, 'Y': self.me + self.dy, 'C': self.me + self.dc}
        self.peer.update({k: (self.me + k) % 8 for k in range(1, 8)})
        self.block = {'O': self.me, 'X': self.me + self.dx, 'Y': self.me + self.dy, 'D': self.me + self.dx + self.dy}
        self.other = {key: val + self.dc for key, val in self.block.items()}
        self.x, self.y = (self.me // 2) % 2, self.me // 4

    def pair_at(self, i):
        flip_x, flip_y = 1 - i // 2, 1 - i % 2
        return 2 * (self.y + flip_y * (1 - 2 * self.y)) + self.x + flip_x * (1 - 2 * self.x)

    def barrier(self, everyone=False):
        sem = pltpu.get_barrier_semaphore()
        keys = range(1, 8) if everyone else 'XYC'
        for key in keys:
            pl.semaphore_signal(sem, inc=1, device_id=(self.group, self.peer[key]), device_id_type=pl.DeviceIdType.MESH)
        pl.semaphore_wait(sem, len(keys))


class Links:
    def __init__(self, place, send_sem, recv_sem):
        self.place, self.send_sem, self.recv_sem = place, send_sem, recv_sem
        self.copies = {}

    def define(self, name, to, src, dst, *index):
        at = len(self.copies)

        def place_of(ref):
            ref, where = ref if isinstance(ref, tuple) else (ref, index)
            return ref.at[where] if where else ref

        def copy():
            return pltpu.make_async_remote_copy(
                src_ref=place_of(src), dst_ref=place_of(dst), send_sem=self.send_sem.at[at], recv_sem=self.recv_sem.at[at],
                device_id=(self.place.group, self.place.peer[to]), device_id_type=pl.DeviceIdType.MESH)

        self.copies[name] = copy

    def start(self, name):
        self.copies[name]().start()

    def send(self, name, *rest):
        self.define(name, *rest)
        self.start(name)

    def wait(self, *names):
        for name in names:
            self.copies[name]().wait_recv()

    def finish(self):
        for copy in self.copies.values():
            copy().wait_send()


class Gather:
    COPIES = 10

    def __init__(self, place, own, full, send_sem, recv_sem):
        self.place, self.own, self.full = place, own, full
        self.links = Links(place, send_sem, recv_sem)
        half = own.shape[0] // 2
        self.first, self.second = pl.ds(0, half), pl.ds(half, half)

    def start(self):
        me, full, own, send = self.place.me, self.full, self.own, self.links.send
        for name, half in (('Xa', self.first), ('Yb', self.second), ('Xb', self.second), ('Ya', self.first)):
            send(name, name[0], (own, (half,)), (full, (me, half)))
        send('CO', 'C', (own, ()), (full, (me,)))

    def relay(self):
        links, full, block = self.links, self.full, self.place.block
        links.wait('Xa')
        links.send('Da', 'Y', full, full, block['X'], self.first)
        links.wait('Yb')
        links.send('Db', 'X', full, full, block['Y'], self.second)

    def forward(self, key):
        first, second = ('Xb', None) if key == 'X' else ('Ya', None) if key == 'Y' else ('Da', 'Db')
        self.links.wait(first)
        if second:
            self.links.wait(second)
        self.links.send('C' + key, 'C', self.full, self.full, self.place.block[key])


class ThirdGather:
    COPIES = 5

    def __init__(self, place, full, send_sem, recv_sem):
        self.place, self.full = place, full
        self.links = Links(place, send_sem, recv_sem)
        half = full.shape[1] // 2
        self.first, self.second = pl.ds(0, half), pl.ds(half, half)

    def start(self, third, own):
        me, full = self.place.me, self.full
        near = {'X': self.first, 'Y': self.second} if third == 0 else {'X': self.second, 'Y': self.first}
        if third == 2:
            block = self.place.block
            near = {'Y': (block['X'], self.first), 'X': (block['Y'], self.second)}
        for key in 'XY':
            if third == 2:
                self.links.send('N' + key, key, full, full, *near[key])
            else:
                src = (full, (me, near[key])) if own is None else (own, (near[key],))
                self.links.send('N' + key, key, src, (full, (me, near[key])))
        if third == 0:
            self.links.send('CO', 'C', (own, ()), (full, (me,)))

    def forward(self, third):
        block = self.place.block
        for key in 'XY':
            self.links.wait('N' + key)
            half = self.first if (third == 0) == (key == 'X') else self.second
            slot = block[key]
            if third == 2:
                slot, half = block['D'], (self.second if key == 'X' else self.first)
            self.links.send('C' + key, 'C', self.full, self.full, slot, half)

    def wait_pair(self, third):
        self.links.wait('CX', 'CY', *(('CO',) if third == 0 else ()))


class Scatter:
    COPIES = 10

    def __init__(self, place, part, crecv, diag_recv, last_recv, send_sem, recv_sem):
        self.place, self.part, self.crecv = place, part, crecv
        self.diag_recv, self.last_recv = diag_recv, last_recv
        self.links = Links(place, send_sem, recv_sem)
        half = part.shape[1] // 2
        self.half = {'a': pl.ds(0, half), 'b': pl.ds(half, half)}
        for at, key in enumerate('OXYD'):
            self.links.define('C' + key, 'C', (part, (place.other[key],)), (crecv, (at,)))

    def add_rows(self, slot, start, count, other, other_start):
        step = 64

        def body(i, carry):
            here = pl.ds(pl.multiple_of(start + i * step, step), step)
            there = pl.ds(pl.multiple_of(other_start + i * step, step), step)
            total = self.part[slot, here, :].astype(F32) + other[there, :].astype(F32)
            self.part[slot, here, :] = total.astype(BF16)
            return carry

        lax.fori_loop(0, count // step, body, 0)

    def swap(self, key):
        self.links.start('C' + key)

    def add_pair(self, key):
        self.links.wait('C' + key)
        at = 'OXYD'.index(key)
        self.add_rows(self.place.block[key], 0, self.part.shape[1], self.crecv.at[at], 0)

    def send_half(self, key, half):
        at = self.half[half]
        self.links.send(key + half, key, (self.part, (self.place.block[key], at)), (self.last_recv, ('XY'.index(key), at)))

    def send_diag(self):
        for i, (key, half) in enumerate((('X', 'a'), ('Y', 'b'))):
            self.links.send('D' + half, key, (self.part, (self.place.block['D'], self.half[half])), (self.diag_recv, (i,)))

    def add_diag(self):
        rows = self.part.shape[1] // 4
        for i, (half, key, start) in enumerate((('a', 'Y', 0), ('b', 'X', 2 * rows))):
            self.links.wait('D' + half)
            for quarter in range(2):
                off = quarter * rows
                self.add_rows(self.place.block[key], start + off, rows, self.diag_recv.at[i], off)
                at = pl.ds(start + off, rows)
                self.links.send(key + half + str(quarter), key, (self.part, (self.place.block[key], at)),
                                (self.last_recv, ('XY'.index(key), at)))

    def wait_last(self, quarter):
        if quarter == 0:
            self.links.wait('Xa', 'Yb', 'CO')
        self.links.wait('Ya' + str(quarter), 'Xb' + str(quarter))

    def norm_loop(self, body):
        rows = self.part.shape[1]
        chunks = rows // LN_ROWS
        quarter = chunks // 4

        def step(i):
            for part in range(2):
                @pl.when(i == part * (chunks // 2))
                def _():
                    self.wait_last(part)

            part, j = i // (2 * quarter), i % (2 * quarter)
            body(tile_at((j // quarter) * 2 * quarter + part * quarter + j % quarter, LN_ROWS))

        loop(chunks, step)

    def between(self, i):
        @pl.when(i == 1)
        def _():
            self.add_pair('D')
            self.send_diag()

        @pl.when(i == 2)
        def _():
            self.add_pair('X')
            self.send_half('X', 'a')

        @pl.when(i == 3)
        def _():
            self.add_pair('Y')
            self.send_half('Y', 'b')

    def after(self, i):
        for at, key in enumerate('DXYO'):
            @pl.when(i == at)
            def _():
                self.swap(key)

    def total(self, at):
        me = self.place.me
        return (self.part[me, at, :].astype(F32) + self.crecv[0, at, :].astype(F32)
                + self.last_recv[0, at, :].astype(F32) + self.last_recv[1, at, :].astype(F32))


def gelu_slope(pre_act):
    tanh_val = jnp.tanh(GELU_SCALE * (pre_act + GELU_COEF * pre_act * pre_act * pre_act))
    return 0.5 * (1.0 + tanh_val) + 0.5 * pre_act * (1.0 - tanh_val * tanh_val) * GELU_SCALE * (1.0 + 3.0 * GELU_COEF * pre_act * pre_act)


def layer_norm_hat(rows_f32):
    centered = rows_f32 - jnp.mean(rows_f32, axis=-1, keepdims=True)
    inv_std = lax.rsqrt(jnp.mean(centered * centered, axis=-1, keepdims=True) + LN_EPS)
    return centered * inv_std, inv_std


LN_ROWS = 32
TILE = 1280
VMEM = pl.BlockSpec(memory_space=pltpu.VMEM)
HBM = pl.BlockSpec(memory_space=pl.ANY)
DMA = pltpu.SemaphoreType.DMA
shape = jax.ShapeDtypeStruct


def tile_at(i, size):
    return pl.ds(pl.multiple_of(i * size, size), size)


def start_copies(sem, *pairs):
    copies = [pltpu.make_async_copy(src, dst, sem.at[i]) for i, (src, dst) in enumerate(pairs)]
    for copy in copies:
        copy.start()
    return copies


def loop(count, body, start=0):
    def step(i, carry):
        body(i)
        return carry

    lax.fori_loop(start, count, step, 0)


def comm_call(kernel, name, ident, flops, args, in_specs, out_shape, out_specs, scratch, aliases={}):
    return pl.pallas_call(
        kernel, in_specs=in_specs, out_specs=out_specs, out_shape=out_shape, scratch_shapes=scratch, name=name,
        input_output_aliases=aliases,
        compiler_params=pltpu.CompilerParams(collective_id=ident, has_side_effects=True, vmem_limit_bytes=66_000_000),
        cost_estimate=pl.CostEstimate(flops=flops, bytes_accessed=40_000_000, transcendentals=3_000_000),
    )(*args)


class Tiles:
    def __init__(self, buf, out, sem, rows=False):
        self.buf, self.out, self.sem, self.rows = buf, out, sem, rows

    def copy(self, n):
        size = self.buf.shape[1 if self.rows else 2]
        at = tile_at(n, size)
        dst = self.out.at[at] if self.rows else self.out.at[:, at]
        return pltpu.make_async_copy(self.buf.at[n % 2], dst, self.sem.at[n % 2])

    def put(self, n, value):
        @pl.when(n >= 2)
        def _():
            self.copy(n - 2).wait()

        self.buf[n % 2] = value()
        self.copy(n).start()

    def finish(self, count):
        self.copy(count - 2).wait()
        self.copy(count - 1).wait()


OUT_TILE = 512


def flat_cols(ref, cols):
    return ref[:, :, cols].reshape(ref.shape[0] * ref.shape[1], OUT_TILE)


def fwd_kernel(dout_ref, q_hbm, k_hbm, v_hbm, x_hbm, mid_hbm, gain1_ref, bias1_ref, gain2_ref, bias2_ref,
               dfull, ctx_ref, wide_ref, max_ref, inv_ref, h1_ref, h2_ref,
               k_rows, strip, q_ref, k_ref, v_ref, x_ref, mid_ref, own_sem, load_sem, *comm_sems):
    place = Place()
    place.barrier()
    gather = Gather(place, dout_ref, dfull, *comm_sems)
    gather.start()
    loads = start_copies(load_sem, (x_hbm, x_ref), (mid_hbm, mid_ref), (k_hbm, k_ref), (q_hbm, q_ref), (v_hbm, v_ref))
    own_copy = pltpu.make_async_copy(dout_ref, dfull.at[place.me], own_sem)
    own_copy.start()
    heads, dim, seq = q_ref.shape
    exp_scale = dim ** -0.5 * LOG2E
    loads[0].wait()
    loads[1].wait()
    affine = [ref[...].reshape(1, ref.shape[0]) for ref in (gain1_ref, bias1_ref, gain2_ref, bias2_ref)]

    def norm_rows(i):
        at = tile_at(i, LN_ROWS)
        for row, (src, dst) in enumerate(((x_ref, h1_ref), (mid_ref, h2_ref))):
            x_hat, _ = layer_norm_hat(src[at, :].astype(F32))
            dst[at, :] = (x_hat * affine[2 * row] + affine[2 * row + 1]).astype(BF16)

    loop(x_ref.shape[0] // LN_ROWS, norm_rows)
    for copy in loads[2:]:
        copy.wait()

    def head(h):
        k_rows[...] = k_ref[h].T

        def query_block(qi):
            q_at = tile_at(qi, BLK)
            q_blk = q_ref[h, :, q_at]

            def score_step(ki, run_max):
                at = tile_at(ki, BLK)
                blk = dot(k_rows[at, :], q_blk)
                strip[at, :] = blk
                return jnp.maximum(run_max, jnp.max(blk, axis=0, keepdims=True))

            diag = causal_fill(dot(k_rows[q_at, :], q_blk), -1e30)
            strip[q_at, :] = diag
            row_max = lax.fori_loop(0, qi, score_step, jnp.max(diag, axis=0, keepdims=True))

            def exp_step(ki, run_sum):
                at = tile_at(ki, BLK)
                probs = jnp.exp2((strip[at, :] - row_max) * exp_scale)
                strip[at, :] = probs
                return run_sum + jnp.sum(probs, axis=0, keepdims=True)

            row_inv = 1.0 / lax.fori_loop(0, qi + 1, exp_step, jnp.zeros_like(row_max))

            def ctx_step(ki, carry):
                high, low = carry
                at = tile_at(ki, BLK)
                probs = strip[at, :] * row_inv
                probs_low = probs.astype(BF16)
                rest = (probs - probs_low.astype(F32)).astype(BF16)
                v_blk = v_ref[h, :, at]
                return high + dot(v_blk, probs_low), low + dot(v_blk, rest)

            zero = jnp.zeros((dim, BLK), F32)
            high, low = lax.fori_loop(0, qi + 1, ctx_step, (zero, zero))
            ctx_ref[h, :, q_at] = high.astype(BF16)
            wide_ref[h, :, q_at] = high + low
            max_ref[h, :, q_at] = row_max
            inv_ref[h, :, q_at] = row_inv

        loop(seq // BLK, query_block)

    def head_step(h):
        head(h)

        @pl.when(h == 1)
        def _():
            gather.relay()

        @pl.when(h == 2)
        def _():
            gather.forward('X')
            gather.forward('Y')

    loop(heads, head_step)
    gather.forward('D')
    gather.links.wait('CO', 'CX', 'CY', 'CD')
    own_copy.wait()
    gather.links.finish()


def fwd_call(d_out, q_t, k_t, v_t, x_in, x_mid, affine):
    heads, dim, seq = q_t.shape
    rows, model = d_out.shape
    return comm_call(
        fwd_kernel, "attn_fwd", 0, 40_000_000_000, (d_out, q_t, k_t, v_t, x_in, x_mid, *affine),
        [VMEM] + [HBM] * 5 + [VMEM] * 4,
        [shape((seq // rows, rows, model), BF16), shape((heads, dim, seq), BF16), shape((heads, dim, seq), F32),
         shape((heads, 1, seq), F32), shape((heads, 1, seq), F32), shape((rows, model), BF16), shape((rows, model), BF16)],
        [HBM] + [VMEM] * 6,
        [pltpu.VMEM((seq, dim), BF16), pltpu.VMEM((seq, BLK), F32)] + [pltpu.VMEM(q_t.shape, BF16)] * 3
        + [pltpu.VMEM((rows, model), BF16)] * 2 + [DMA(()), DMA((5,))] + [DMA((10,))] * 2)


def dot_t(a, b):
    return lax.dot_general(a, b, (((1,), (1,)), ((), ())), preferred_element_type=F32)


def mlp_kernel(dfull, dout_hbm, mid_hbm, gain_ref, h1_ref, z_ref, w2_ref, w1_ref,
               dx1_ref, dz_ref, gb1_ref, vec_ref, h1full,
               w2v, w1v, dzv, ybuf, part, crecv, diag_recv, last_recv, dout_ref, mid_ref,
               load_sem, y_sem, z_sem, dz_sem, own_sem, *comm_sems):
    place = Place()
    place.barrier()
    rows, model = dout_hbm.shape
    hidden = w2v.shape[0]
    scatter = Scatter(place, part, crecv, diag_recv, last_recv, *comm_sems[0:2])
    gather = ThirdGather(place, h1full, *comm_sems[2:4])
    gather.start(0, h1_ref)
    own_copy = pltpu.make_async_copy(h1_ref, h1full.at[place.me], own_sem)

    def load_pair(i):
        return pltpu.make_async_copy(dfull.at[pl.ds(2 * place.pair_at(i), 2)], ybuf.at[i % 2], y_sem.at[i])

    def store_grad(i):
        at = tile_at(place.pair_at(i), 2 * rows)
        return pltpu.make_async_copy(dzv.at[at], dz_ref.at[at], dz_sem.at[i])

    def load_pre(i):
        at = tile_at(place.pair_at(i), 2 * rows)
        return pltpu.make_async_copy(z_ref.at[at], dzv.at[at], z_sem.at[i])

    load_pair(0).start()
    load_pre(0).start()
    loads = start_copies(load_sem, (w2_ref, w2v), (w1_ref, w1v), (dout_hbm, dout_ref), (mid_hbm, mid_ref))
    for i in range(1, 4):
        load_pre(i).start()
    load_pair(1).start()
    own_copy.start()
    gb1_ref[...] = jnp.zeros_like(gb1_ref)
    vec_ref[...] = jnp.zeros_like(vec_ref)
    loads[0].wait()

    def pair_step(i):
        slot = i % 2
        pair = place.pair_at(i)
        at = tile_at(pair, 2 * rows)
        load_pair(i).wait()
        load_pre(i).wait()

        def grad_act(n):
            cols = tile_at(n, TILE)
            acc = dot_t(ybuf[slot].reshape(2 * rows, model), w2v[cols, :])
            grad = (acc * gelu_slope(dzv[at, cols].astype(F32))).astype(BF16)
            dzv[at, cols] = grad
            gb1_ref[:, cols] += jnp.sum(grad.astype(F32), axis=0, keepdims=True)

        loop(hidden // TILE, grad_act)
        store_grad(i).start()

        @pl.when(i < 2)
        def _():
            load_pair(i + 2).start()

        @pl.when(i == 0)
        def _():
            loads[1].wait()

        @pl.when(i == 2)
        def _():
            gather.forward(0)

        scatter.between(i)

        def grad_norm(n):
            cols = tile_at(n, TILE)
            acc = dot_t(dzv[at, :], w1v[cols, :]).astype(BF16)
            part[2 * pair, :, cols] = acc[:rows]
            part[2 * pair + 1, :, cols] = acc[rows:]

        loop(model // TILE, grad_norm)
        scatter.after(i)

    loop(4, pair_step)
    scatter.add_diag()

    gain = gain_ref[...].reshape(1, model)
    loads[2].wait()
    loads[3].wait()

    def norm_rows(at):
        grad = scatter.total(at)
        x_hat, inv_std = layer_norm_hat(mid_ref[at, :].astype(F32))
        dout_rows = dout_ref[at, :].astype(F32)
        mid = (dout_rows + layer_norm_bwd(grad, x_hat, inv_std, gain)).astype(BF16)
        dx1_ref[at, :] = mid
        for row, val in enumerate((grad * x_hat, grad, mid.astype(F32), dout_rows)):
            vec_ref[row + 2:row + 3, :] += jnp.sum(val, axis=0, keepdims=True)

    scatter.norm_loop(norm_rows)
    for i in range(4):
        store_grad(i).wait()
    own_copy.wait()
    gather.wait_pair(0)
    gather.links.finish()
    scatter.links.finish()


def scatter_scratch(rows, model):
    return [pltpu.VMEM((8, rows, model), BF16), pltpu.VMEM((4, rows, model), BF16),
            pltpu.VMEM((2, rows // 2, model), BF16), pltpu.VMEM((2, rows, model), BF16)]


def mlp_call(dfull, d_out, x_mid, gain, h1, z_saved, w2, w1):
    rows, model = d_out.shape
    seq, hidden = z_saved.shape
    return comm_call(
        mlp_kernel, "mlp_grads", 1, 60_000_000_000, (dfull, d_out, x_mid, gain, h1, z_saved, w2, w1),
        [HBM] * 3 + [VMEM] + [HBM] * 4,
        [shape((rows, model), BF16), shape((seq, hidden), BF16), shape((1, hidden), F32), shape((8, model), F32),
         shape(dfull.shape, BF16)],
        [VMEM, HBM, VMEM, VMEM, HBM],
        [pltpu.VMEM((hidden, model), BF16), pltpu.VMEM((model, hidden), BF16),
         pltpu.VMEM((seq, hidden), BF16), pltpu.VMEM((2, 2, rows, model), BF16)]
        + scatter_scratch(rows, model) + [pltpu.VMEM((rows, model), BF16)] * 2
        + [DMA((4,))] * 4 + [DMA(())] + [DMA((12,))] * 2 + [DMA((5,))] * 2)


def gelu(pre_act):
    return 0.5 * pre_act * (1.0 + jnp.tanh(GELU_SCALE * (pre_act + GELU_COEF * pre_act * pre_act * pre_act)))


def ctx_kernel(dx1_ref, wo_ref, z_ref, dfull, mfull, do_ref, dw2_ref,
               mbuf, zv, ut, yv, obuf, own_sem, m_sem, load_sem, out_sem, *comm_sems):
    place = Place()
    place.barrier()
    rows, model = dx1_ref.shape
    gather = Gather(place, dx1_ref, mfull, *comm_sems)
    gather.start()
    own_copy = pltpu.make_async_copy(dx1_ref, mfull.at[place.me], own_sem)
    own_copy.start()

    loads = [pltpu.make_async_copy(z_ref, zv, load_sem.at[0]), pltpu.make_async_copy(dfull, yv, load_sem.at[1])]
    for copy in loads:
        copy.start()
    tiles = Tiles(obuf, dw2_ref, out_sem)
    count = model // OUT_TILE

    def turn(n):
        cols = tile_at(n, 256)
        ut[cols, :] = gelu(zv[:, cols].astype(F32)).astype(BF16).T

    def weight_tile(n):
        cols = tile_at(n, OUT_TILE)
        tiles.put(n, lambda: dot(ut[...], flat_cols(yv, cols)))

    loads[0].wait()
    loop(ut.shape[0] // 256, turn)
    gather.relay()
    loads[1].wait()
    loop(count, weight_tile)
    gather.forward('X')
    gather.forward('Y')
    own_copy.wait()
    gather.links.wait('CO')

    def grad_ctx(i):
        @pl.when(i == 1)
        def _():
            gather.links.wait('CY')

        @pl.when(i == 2)
        def _():
            gather.links.wait('CX')

        @pl.when(i == 3)
        def _():
            gather.forward('D')
            gather.links.wait('CD')

        pair = place.pair_at(3 - i)
        copy = pltpu.make_async_copy(mfull.at[pl.ds(2 * pair, 2)], mbuf, m_sem)
        copy.start()
        copy.wait()
        do_ref[:, tile_at(pair, 2 * rows)] = dot_t(wo_ref[...], mbuf[...].reshape(2 * rows, model)).astype(BF16)

    loop(4, grad_ctx)
    tiles.finish(count)
    gather.links.finish()


def ctx_call(dx1, w_rows, z_saved, dfull):
    rows, model = dx1.shape
    feats = w_rows.shape[0]
    seq, hidden = z_saved.shape
    return comm_call(
        ctx_kernel, "ctx_grads", 2, 30_000_000_000, (dx1, w_rows, z_saved, dfull), [VMEM] * 2 + [HBM] * 2,
        [shape((seq // rows, rows, model), BF16), shape((feats, seq), BF16), shape((hidden, model), F32)], [HBM, VMEM, HBM],
        [pltpu.VMEM((2, rows, model), BF16), pltpu.VMEM((seq, hidden), BF16), pltpu.VMEM((hidden, seq), BF16),
         pltpu.VMEM((seq // rows, rows, model), BF16), pltpu.VMEM((2, hidden, OUT_TILE), F32),
         DMA(()), DMA(()), DMA((2,)), DMA((2,))] + [DMA((10,))] * 2)


def bwd_kernel(h2_ref, q_hbm, k_hbm, v_hbm, do_hbm, wide_hbm, max_ref, inv_ref, dz_ref, h1_in,
               h1full, h2full, out_ref, dw1_ref,
               k_rows, v_rows, q_rows, do_rows, delta, dq_acc, dk_acc, dv_acc, tok, dzv, wbuf,
               q_ref, k_ref, v_ref, do_ref, wide_ref, own_sem, head_sem, load_sem, out_sem, *comm_sems):
    place = Place()
    place.barrier()
    gather1 = ThirdGather(place, h1full, *comm_sems[0:2])
    gather2 = Gather(place, h2_ref, h2full, *comm_sems[2:4])
    gather2.start()
    loads = start_copies(head_sem, (k_hbm, k_ref), (v_hbm, v_ref), (q_hbm, q_ref), (do_hbm, do_ref), (wide_hbm, wide_ref))
    own_copy = pltpu.make_async_copy(h2_ref, h2full.at[place.me], own_sem)
    own_copy.start()
    heads, dim, seq = q_ref.shape
    blocks = seq // BLK
    scale = dim ** -0.5
    exp_scale = scale * LOG2E

    def head(h):
        k_rows[...] = k_ref[h].T
        v_rows[...] = v_ref[h].T
        q_rows[...] = q_ref[h].T
        do_rows[...] = do_ref[h].T
        delta[...] = jnp.sum(do_ref[h].astype(F32) * wide_ref[h], axis=0, keepdims=True)
        dq_acc[...] = jnp.zeros_like(dq_acc)
        dk_acc[...] = jnp.zeros_like(dk_acc)
        dv_acc[...] = jnp.zeros_like(dv_acc)

        def block(qi, ki, on_diag):
            q_at, k_at = tile_at(qi, BLK), tile_at(ki, BLK)
            scores = dot(k_rows[k_at, :], q_ref[h, :, q_at])
            if on_diag:
                scores = causal_fill(scores, -1e30)
            probs = jnp.exp2((scores - max_ref[h, :, q_at]) * exp_scale) * inv_ref[h, :, q_at]
            grad_probs = dot(v_rows[k_at, :], do_ref[h, :, q_at])
            dv_acc[k_at, :] += dot(probs.astype(BF16), do_rows[q_at, :])
            grad_scores = (probs * (grad_probs - delta[:, q_at]) * scale).astype(BF16)
            dk_acc[k_at, :] += dot(grad_scores, q_rows[q_at, :])
            dq_acc[:, q_at] += dot(k_ref[h, :, k_at], grad_scores)

        loop(blocks, lambda i: block(i, i, True))
        loop(blocks, lambda ki: loop(blocks, lambda qi: block(qi, ki, False), ki + 1))
        out_ref[0, h] = dq_acc[...].astype(BF16)
        out_ref[1, h] = dk_acc[...].astype(BF16).T
        out_ref[2, h] = dv_acc[...].astype(BF16).T

    load_grad = pltpu.make_async_copy(dz_ref, dzv, load_sem.at[4])

    def load_tok(i):
        at = pl.ds(2 * place.pair_at(i), 2)
        return pltpu.make_async_copy(h2full.at[at], tok.at[at], load_sem.at[i])

    for copy in loads:
        copy.wait()
    count = tok.shape[2] // OUT_TILE
    tiles = Tiles(wbuf, dw1_ref, out_sem, rows=True)

    def fc1_tile(n):
        cols = tile_at(n, OUT_TILE)
        tiles.put(n, lambda: dot(flat_cols(tok, cols).T, dzv[...]))

    def head_step(h):
        head(h)

        @pl.when(h == 1)
        def _():
            gather2.relay()
            gather1.start(1, None)

        @pl.when(h == 2)
        def _():
            load_grad.start()
            gather2.forward('X')
            gather2.forward('Y')
            own_copy.wait()
            gather2.links.wait('CO')
            load_tok(3).start()

    loop(heads, head_step)
    gather2.forward('D')
    gather2.links.wait('CX', 'CY')
    load_tok(1).start()
    load_tok(2).start()
    load_grad.wait()
    gather2.links.wait('CD')
    load_tok(0).start()
    for i in range(4):
        load_tok(i).wait()
    loop(count, fc1_tile)
    gather1.forward(1)
    gather1.wait_pair(1)
    tiles.finish(count)
    gather1.links.finish()
    gather2.links.finish()


def bwd_call(h2, q_t, k_t, v_t, do_t, wide, row_max, row_inv, dz, h1full):
    heads, dim, seq = q_t.shape
    rows, model = h2.shape
    full = shape((seq // rows, rows, model), BF16)
    turned = pltpu.VMEM((seq, dim), BF16)
    hidden = dz.shape[1]
    return comm_call(
        bwd_kernel, "attn_bwd", 3, 80_000_000_000,
        (h2, q_t, k_t, v_t, do_t, wide, row_max, row_inv, dz, h1full), [VMEM] + [HBM] * 5 + [VMEM] * 2 + [HBM] * 2,
        [full, full, shape((3, heads, dim, seq), BF16), shape((model, hidden), F32)], [HBM, HBM, VMEM, HBM],
        [turned] * 4 + [pltpu.VMEM((1, seq), F32), pltpu.VMEM((dim, seq), F32), pltpu.VMEM((seq, dim), F32),
                        pltpu.VMEM((seq, dim), F32), pltpu.VMEM((seq // rows, rows, model), BF16),
                        pltpu.VMEM((seq, hidden), BF16), pltpu.VMEM((2, OUT_TILE, hidden), F32),
                        *[pltpu.VMEM(q_t.shape, BF16)] * 4, pltpu.VMEM(wide.shape, F32),
                        DMA(()), DMA((5,)), DMA((5,)), DMA((2,))] + [DMA((5,))] * 2 + [DMA((10,))] * 2,
        aliases={9: 0})


def qkv_kernel(qkv_hbm, w_hbm, dx1_hbm, x_hbm, gain_ref, vec_ref, ctx_hbm, mfull, h1_in,
               dx_ref, vsum_ref, bias_ref, dwo_ref, dw_ref, h1full,
               turned, part, crecv, diag_recv, last_recv, vacc, vsend, vrecv, last_got, tok, obuf, wbuf,
               qkv_ref, w_ref, dx1_ref, x_ref, ctx_ref, vsem, last_sem, load_sem, in_sem, out_sem, *comm_sems):
    place = Place()
    place.barrier(everyone=True)
    rows, model = dx1_ref.shape
    scatter = Scatter(place, part, crecv, diag_recv, last_recv, *comm_sems[0:2])
    gather = ThirdGather(place, h1full, *comm_sems[2:4])
    gather.start(2, None)
    inputs = start_copies(in_sem, (qkv_hbm, qkv_ref), (w_hbm, w_ref), (ctx_hbm, ctx_ref), (dx1_hbm, dx1_ref), (x_hbm, x_ref))
    loads = [pltpu.make_async_copy(src, tok, load_sem.at[i]) for i, src in enumerate((mfull, h1full))]
    tiles_o = Tiles(obuf, dwo_ref, out_sem.at[0])
    tiles = Tiles(wbuf, dw_ref, out_sem.at[1])
    count = model // OUT_TILE
    swaps = Links(place, vsem.at[0], vsem.at[1])
    inputs[0].wait()

    def vec_step(i):
        if i > 0:
            swaps.wait('CXY'[i - 1])
            vacc[...] += vrecv[i - 1]
        if i < 3:
            vsend[i] = vacc[...]

    def vec_send(i):
        swaps.send('CXY'[i], 'CXY'[i], vsend, vrecv, i)

    vacc[...] = vec_ref[...]
    vec_step(0)
    vec_send(0)

    def pair_step(i):
        pair = place.pair_at(i)
        turned[...] = qkv_ref[:, tile_at(pair, 2 * rows)].T

        @pl.when(i == 0)
        def _():
            inputs[1].wait()

        @pl.when(i == 1)
        def _():
            loads[0].start()

        @pl.when(i == 3)
        def _():
            gather.forward(2)

        for at in range(1, 3):
            @pl.when(i == at)
            def _():
                vec_step(at)
                vec_send(at)

        scatter.between(i)

        def grad_norm(n):
            cols = tile_at(n, TILE)
            acc = dot(turned[...], w_ref[:, cols]).astype(BF16)
            part[2 * pair, :, cols] = acc[:rows]
            part[2 * pair + 1, :, cols] = acc[rows:]

        loop(model // TILE, grad_norm)
        scatter.after(i)

    loop(4, pair_step)
    loads[0].wait()
    for copy in inputs[2:]:
        copy.wait()

    def proj_tile(n):
        cols = tile_at(n, OUT_TILE)
        tiles_o.put(n, lambda: dot(ctx_ref[...], flat_cols(tok, cols)))

    def qkv_tile(n):
        cols = tile_at(n, OUT_TILE)
        tiles.put(n, lambda: dot(qkv_ref[...], flat_cols(tok, cols)))

    loop(count, proj_tile)
    scatter.add_diag()
    gather.wait_pair(2)
    loads[1].start()
    ones = jnp.ones((8, qkv_ref.shape[1]), BF16)
    bias_ref[...] = dot_t(ones, qkv_ref[...])
    loads[1].wait()
    loop(count, qkv_tile)
    vec_step(3)
    tiles_o.finish(count)
    gain = gain_ref[...].reshape(1, model)

    def norm_rows(at):
        grad = scatter.total(at)
        x_hat, inv_std = layer_norm_hat(x_ref[at, :].astype(F32))
        dx_ref[at, :] = (dx1_ref[at, :].astype(F32) + layer_norm_bwd(grad, x_hat, inv_std, gain)).astype(BF16)
        vacc[0:1, :] += jnp.sum(grad * x_hat, axis=0, keepdims=True)
        vacc[1:2, :] += jnp.sum(grad, axis=0, keepdims=True)

    scatter.norm_loop(norm_rows)
    finals = Links(place, last_sem.at[0], last_sem.at[1])
    last_got[0] = vacc[0:2, :]
    vsum_ref[2:6, :] = vacc[2:6, :]
    for k in range(1, 8):
        finals.send(k, k, (last_got, (0,)), (last_got, (k,)))
    tiles.finish(count)
    finals.wait(*range(1, 8))
    total = last_got[place.me]
    for source in range(1, 8):
        total += last_got[(place.me + 8 - source) % 8]
    vsum_ref[0:2, :] = total
    for links in (swaps, finals, scatter.links, gather.links):
        links.finish()


def qkv_call(qkv_rows, w_rows, dx1, x_in, gain, vec, ctx_rows, mfull, h1full):
    rows, model = dx1.shape
    feats, seq = qkv_rows.shape
    proj = ctx_rows.shape[0]
    return comm_call(
        qkv_kernel, "qkv_grads", 4, 30_000_000_000,
        (qkv_rows, w_rows, dx1, x_in, gain, vec, ctx_rows, mfull, h1full), [HBM] * 4 + [VMEM] * 2 + [HBM] * 3,
        [shape((rows, model), BF16), shape((6, model), F32), shape((8, feats), F32), shape((proj, model), F32),
         shape((feats, model), F32), shape(h1full.shape, BF16)],
        [VMEM] * 3 + [HBM] * 3,
        [pltpu.VMEM((2 * rows, feats), BF16)] + scatter_scratch(rows, model)
        + [pltpu.VMEM((8, model), F32), pltpu.VMEM((3, 8, model), F32), pltpu.VMEM((3, 8, model), F32),
           pltpu.VMEM((8, 2, model), F32), pltpu.VMEM((8, rows, model), BF16),
           pltpu.VMEM((2, proj, OUT_TILE), F32), pltpu.VMEM((2, feats, OUT_TILE), F32),
           pltpu.VMEM((feats, seq), BF16), pltpu.VMEM((feats, model), BF16), pltpu.VMEM((rows, model), BF16),
           pltpu.VMEM((rows, model), BF16), pltpu.VMEM((proj, seq), BF16),
           DMA((2, 3)), DMA((2, 7)), DMA((2,)), DMA((5,)), DMA((2, 2))] + [DMA((12,))] * 2 + [DMA((5,))] * 2,
        aliases={8: 5})


def finish_kernel(*refs):
    count = (len(refs) - 8) // 2
    rings, single, (small_sem, in_sem, out_sem) = refs[2 * count:2 * count + 2], refs[-6:-3], refs[-3:]
    chunks, used = [], [0, 0]
    small = [(src, buf, dst) for src, buf, dst in zip(refs[4:count], single, refs[count + 4:2 * count])]
    for i, (src, buf, _) in enumerate(small):
        pltpu.make_async_copy(src, buf, small_sem.at[0, i]).start()
    for src, dst in zip(refs[:4], refs[count:count + 4]):
        kind = 0 if src.shape[1] == rings[0].shape[2] else 1
        rows = rings[kind].shape[1]
        for row in range(0, src.shape[0], rows):
            chunks.append((src.at[pl.ds(row, rows)], dst.at[pl.ds(row, rows)], kind, used[kind]))
            used[kind] += 1

    def copy_in(src, dst, kind, at):
        slot = at % RING
        return pltpu.make_async_copy(src, rings[kind].at[slot], in_sem.at[kind, slot])

    def copy_out(src, dst, kind, at):
        slot = at % RING
        return pltpu.make_async_copy(rings[kind].at[slot], dst, out_sem.at[kind, slot])

    waiting = {}

    def start(chunk):
        key = (chunk[2], chunk[3] % RING)
        if key in waiting:
            copy_out(*waiting.pop(key)).wait()
        copy_in(*chunk).start()

    for chunk in chunks[:AHEAD]:
        start(chunk)
    for i, (src, buf, dst) in enumerate(small):
        pltpu.make_async_copy(src, buf, small_sem.at[0, i]).wait()
        pltpu.make_async_copy(buf, dst, small_sem.at[1, i]).start()
    for i, chunk in enumerate(chunks):
        copy_in(*chunk).wait()
        copy_out(*chunk).start()
        waiting[(chunk[2], chunk[3] % RING)] = chunk
        if i + AHEAD < len(chunks):
            start(chunks[i + AHEAD])
    for chunk in waiting.values():
        copy_out(*chunk).wait()
    for i, (_, buf, dst) in enumerate(small):
        pltpu.make_async_copy(buf, dst, small_sem.at[1, i]).wait()


RING = 32
AHEAD = 20


def finish_call(*arrays):
    wide = max(a.shape[1] for a in arrays[:4])
    narrow = min(a.shape[1] for a in arrays[:4])
    small = [pltpu.VMEM(a.shape, a.dtype) for a in arrays[4:]]
    return pl.pallas_call(
        finish_kernel, name="finish", in_specs=[HBM] * len(arrays), out_specs=[HBM] * len(arrays),
        out_shape=[shape(a.shape, a.dtype) for a in arrays],
        scratch_shapes=[pltpu.VMEM((RING, 64, wide), F32), pltpu.VMEM((RING, 128, narrow), F32), *small,
                        DMA((2, len(small))), DMA((2, RING)), DMA((2, RING))],
        compiler_params=pltpu.CompilerParams(vmem_limit_bytes=66_000_000),
        cost_estimate=pl.CostEstimate(flops=1_000_000, bytes_accessed=72_000_000, transcendentals=0),
    )(*arrays)


def solution(mesh):
    def local_backward(x_in, x_mid, d_out, q_saved, k_saved, v_saved, z_saved, ln1_gain, ln1_bias, ln2_gain, ln2_bias, w_qkv, w_proj, w_fc1, w_fc2):
        x_in, x_mid, d_out, z_saved = x_in[0], x_mid[0], d_out[0], z_saved[0]
        heads, dim = q_saved.shape[2:]
        seq, model = z_saved.shape[0], x_in.shape[1]
        q_t, k_t, v_t = (v[0].transpose(1, 2, 0) for v in (q_saved, k_saved, v_saved))
        affine = (ln1_gain, ln1_bias, ln2_gain, ln2_bias)
        dfull, ctx_t, wide_t, row_max, row_inv, h1_local, h2_local = fwd_call(d_out, q_t, k_t, v_t, x_in, x_mid, affine)
        dx1, grad_pre, grad_bfc1, vec, h1_full = mlp_call(dfull, d_out, x_mid, ln2_gain, h1_local, z_saved, w_fc2, w_fc1)
        mfull, do_t, grad_wfc2 = ctx_call(dx1, w_proj.reshape(heads * dim, model), z_saved, dfull)
        h1_full, _, qkv_t, grad_wfc1 = bwd_call(
            h2_local, q_t, k_t, v_t, do_t.reshape(heads, dim, seq), wide_t, row_max, row_inv, grad_pre, h1_full)
        qkv_rows = qkv_t.reshape(3 * heads * dim, seq)
        w_rows = w_qkv.transpose(0, 2, 3, 1).reshape(3 * heads * dim, model)
        grad_x, grad_vecs, bias_rows, grad_wproj, grad_wqkv, _ = qkv_call(
            qkv_rows, w_rows, dx1, x_in, ln1_gain, vec, ctx_t.reshape(heads * dim, seq), mfull, h1_full)
        grad_wfc2, grad_wfc1, grad_wqkv, grad_wproj, grad_x, grad_vecs, grad_bfc1 = finish_call(
            grad_wfc2, grad_wfc1, grad_wqkv, grad_wproj, grad_x, grad_vecs, grad_bfc1)
        grad_wproj = grad_wproj.reshape(heads, dim, model)
        grad_wqkv = grad_wqkv.reshape(3, heads, dim, model).transpose(0, 3, 1, 2)
        grad_bqkv = bias_rows[0].reshape(3, heads, dim)
        return grad_x[None], grad_wqkv, grad_bqkv, grad_wproj, grad_wfc1, grad_bfc1[0], grad_wfc2, grad_vecs

    tok_spec = P('dp', 'tp', None)
    head_spec = P('dp', None, 'tp', None)
    in_specs = (tok_spec, tok_spec, tok_spec, head_spec, head_spec, head_spec, P('dp', None, 'tp'),
                P(None), P(None), P(None), P(None),
                P(None, None, 'tp', None), P('tp', None, None), P(None, 'tp'), P('tp', None))
    out_specs = (tok_spec, P('dp', None, 'tp', None), P('dp', 'tp', None), P(('dp', 'tp'), None, None),
                 P('dp', 'tp'), P(('dp', 'tp')), P(('dp', 'tp'), None), P('dp', None))
    return jax.shard_map(local_backward, mesh=mesh, in_specs=in_specs, out_specs=out_specs, check_vma=False)
```

```python
import jax
import jax.numpy as jnp
from jax import lax
from jax.experimental import pallas as pl
from jax.experimental.pallas import tpu as pltpu
from jax.sharding import PartitionSpec as P

LN_EPS = 1e-5
GELU_COEF = 0.044715
GELU_SCALE = 0.7978845608028654
LOG2E = 1.4426950408889634
BLK = 512
F32 = jnp.float32
BF16 = jnp.bfloat16
COLS = dict(axis=0, keepdims=True)
ROWS = dict(axis=-1, keepdims=True)


def layer_norm_bwd(grad_norm, x_hat, inv_std, norm_gain):
    grad_hat = grad_norm * norm_gain
    centered_grad = grad_hat - jnp.mean(grad_hat, **ROWS)
    return inv_std * (centered_grad - x_hat * jnp.mean(grad_hat * x_hat, **ROWS))


def dot(a, b):
    return jnp.dot(a, b, preferred_element_type=F32)


def causal_fill(scores, fill):
    key_ids = lax.broadcasted_iota(jnp.int32, scores.shape, 0)
    query_ids = lax.broadcasted_iota(jnp.int32, scores.shape, 1)
    return jnp.where(query_ids >= key_ids, scores, fill)


class Place:
    def __init__(self):
        self.group = lax.axis_index('dp')
        self.me = lax.axis_index('tp')
        self.core = self.me % 2
        self.dx = 2 - 4 * ((self.me // 2) % 2)
        self.dy = 4 - 8 * (self.me // 4)
        self.dc = 1 - 2 * self.core
        self.peer = {'X': self.me + self.dx, 'Y': self.me + self.dy, 'C': self.me + self.dc}
        self.peer.update({k: (self.me + k) % 8 for k in range(1, 8)})
        self.block = {'O': self.me, 'X': self.me + self.dx, 'Y': self.me + self.dy, 'D': self.me + self.dx + self.dy}
        self.other = {key: val + self.dc for key, val in self.block.items()}
        self.x, self.y = (self.me // 2) % 2, self.me // 4

    def pair_at(self, i):
        flip_x, flip_y = 1 - i // 2, 1 - i % 2
        return 2 * (self.y + flip_y * (1 - 2 * self.y)) + self.x + flip_x * (1 - 2 * self.x)

    def barrier(self, everyone=False):
        sem = pltpu.get_barrier_semaphore()
        keys = range(1, 8) if everyone else 'XYC'
        for key in keys:
            pl.semaphore_signal(sem, inc=1, device_id=(self.group, self.peer[key]), device_id_type=pl.DeviceIdType.MESH)
        pl.semaphore_wait(sem, len(keys))


class Links:
    def __init__(self, place, send_sem, recv_sem):
        self.place, self.send_sem, self.recv_sem = place, send_sem, recv_sem
        self.copies = {}

    def define(self, name, to, src, dst, *index):
        at = len(self.copies)

        def place_of(ref):
            ref, where = ref if isinstance(ref, tuple) else (ref, index)
            return ref.at[where] if where else ref

        def copy():
            return pltpu.make_async_remote_copy(
                src_ref=place_of(src), dst_ref=place_of(dst), send_sem=self.send_sem.at[at], recv_sem=self.recv_sem.at[at],
                device_id=(self.place.group, self.place.peer[to]), device_id_type=pl.DeviceIdType.MESH)

        self.copies[name] = copy

    def start(self, name):
        self.copies[name]().start()

    def send(self, name, *rest):
        self.define(name, *rest)
        self.start(name)

    def wait(self, *names):
        for name in names:
            self.copies[name]().wait_recv()

    def finish(self):
        for copy in self.copies.values():
            copy().wait_send()


class Gather:
    COPIES = 10

    def __init__(self, place, own, full, send_sem, recv_sem):
        self.place, self.own, self.full = place, own, full
        self.links = Links(place, send_sem, recv_sem)
        half = own.shape[0] // 2
        self.first, self.second = pl.ds(0, half), pl.ds(half, half)

    def start(self):
        me, full, own, send = self.place.me, self.full, self.own, self.links.send
        for name, half in (('Xa', self.first), ('Yb', self.second), ('Xb', self.second), ('Ya', self.first)):
            send(name, name[0], (own, (half,)), (full, (me, half)))
        send('CO', 'C', (own, ()), (full, (me,)))

    def relay(self):
        links, full, block = self.links, self.full, self.place.block
        links.wait('Xa')
        links.send('Da', 'Y', full, full, block['X'], self.first)
        links.wait('Yb')
        links.send('Db', 'X', full, full, block['Y'], self.second)

    def forward(self, key):
        first, second = ('Xb', None) if key == 'X' else ('Ya', None) if key == 'Y' else ('Da', 'Db')
        self.links.wait(first)
        if second:
            self.links.wait(second)
        self.links.send('C' + key, 'C', self.full, self.full, self.place.block[key])


class ThirdGather:
    def __init__(self, place, full, send_sem, recv_sem):
        self.place, self.full = place, full
        self.links = Links(place, send_sem, recv_sem)
        half = full.shape[1] // 2
        self.first, self.second = pl.ds(0, half), pl.ds(half, half)

    def start(self, third, own):
        me, full, block = self.place.me, self.full, self.place.block
        near = {'near': {'X': self.first, 'Y': self.second}, 'rest': {'X': self.second, 'Y': self.first}}.get(third)
        for key in 'XY':
            if near is None:
                slot, half = (block['Y'], self.second) if key == 'X' else (block['X'], self.first)
                self.links.send(third + key, key, full, full, slot, half)
            else:
                src = (full, (me, near[key])) if own is None else (own, (near[key],))
                self.links.send(third + key, key, src, (full, (me, near[key])))
        if third == 'near':
            self.links.send('CO', 'C', (own, ()), (full, (me,)))

    def forward(self, third):
        block = self.place.block
        for key in 'XY':
            self.links.wait(third + key)
            half = self.first if (third == 'near') == (key == 'X') else self.second
            slot = block[key]
            if third == 'diag':
                slot, half = block['D'], (self.second if key == 'X' else self.first)
            self.links.send('C' + third + key, 'C', self.full, self.full, slot, half)

    def wait_pair(self, third):
        self.links.wait('C' + third + 'X', 'C' + third + 'Y', *(('CO',) if third == 'near' else ()))


class Scatter:
    COPIES = 10

    def __init__(self, place, part, crecv, diag_recv, last_recv, send_sem, recv_sem):
        self.place, self.part, self.crecv = place, part, crecv
        self.diag_recv, self.last_recv = diag_recv, last_recv
        self.links = Links(place, send_sem, recv_sem)
        half = part.shape[1] // 2
        self.half = {'a': pl.ds(0, half), 'b': pl.ds(half, half)}
        for at, key in enumerate('OXYD'):
            self.links.define('C' + key, 'C', (part, (place.other[key],)), (crecv, (at,)))

    def add_rows(self, slot, start, count, other, other_start):
        step = 64

        def body(i, carry):
            here = pl.ds(pl.multiple_of(start + i * step, step), step)
            there = pl.ds(pl.multiple_of(other_start + i * step, step), step)
            total = self.part[slot, here, :].astype(F32) + other[there, :].astype(F32)
            self.part[slot, here, :] = total.astype(BF16)
            return carry

        lax.fori_loop(0, count // step, body, 0)

    def swap(self, key):
        self.links.start('C' + key)

    def add_pair(self, key):
        self.links.wait('C' + key)
        at = 'OXYD'.index(key)
        self.add_rows(self.place.block[key], 0, self.part.shape[1], self.crecv.at[at], 0)

    def send_half(self, key, half):
        at = self.half[half]
        self.links.send(key + half, key, (self.part, (self.place.block[key], at)), (self.last_recv, ('XY'.index(key), at)))

    def send_diag(self):
        for i, (key, half) in enumerate((('X', 'a'), ('Y', 'b'))):
            self.links.send('D' + half, key, (self.part, (self.place.block['D'], self.half[half])), (self.diag_recv, (i,)))

    def add_diag(self):
        rows = self.part.shape[1] // 4
        for i, (half, key, start) in enumerate((('a', 'Y', 0), ('b', 'X', 2 * rows))):
            self.links.wait('D' + half)
            for quarter in range(2):
                off = quarter * rows
                self.add_rows(self.place.block[key], start + off, rows, self.diag_recv.at[i], off)
                at = pl.ds(start + off, rows)
                self.links.send(key + half + str(quarter), key, (self.part, (self.place.block[key], at)),
                                (self.last_recv, ('XY'.index(key), at)))

    def wait_last(self, quarter):
        if quarter == 0:
            self.links.wait('Xa', 'Yb', 'CO')
        self.links.wait('Ya' + str(quarter), 'Xb' + str(quarter))

    def norm_loop(self, body):
        rows = self.part.shape[1]
        chunks = rows // LN_ROWS
        quarter = chunks // 4

        def step(i):
            for part in range(2):
                @pl.when(i == part * (chunks // 2))
                def _():
                    self.wait_last(part)

            part, j = i // (2 * quarter), i % (2 * quarter)
            body(tile_at((j // quarter) * 2 * quarter + part * quarter + j % quarter, LN_ROWS))

        loop(chunks, step)

    def between(self, i):
        @pl.when(i == 1)
        def _():
            self.add_pair('D')
            self.send_diag()

        @pl.when(i == 2)
        def _():
            self.add_pair('X')
            self.send_half('X', 'a')

        @pl.when(i == 3)
        def _():
            self.add_pair('Y')
            self.send_half('Y', 'b')

    def after(self, i):
        for at, key in enumerate('DXYO'):
            @pl.when(i == at)
            def _():
                self.swap(key)

    def total(self, at):
        me = self.place.me
        return (self.part[me, at, :].astype(F32) + self.crecv[0, at, :].astype(F32)
                + self.last_recv[0, at, :].astype(F32) + self.last_recv[1, at, :].astype(F32))


def gelu_slope(pre_act):
    tanh_val = jnp.tanh(GELU_SCALE * (pre_act + GELU_COEF * pre_act * pre_act * pre_act))
    return 0.5 * (1.0 + tanh_val) + 0.5 * pre_act * (1.0 - tanh_val * tanh_val) * GELU_SCALE * (1.0 + 3.0 * GELU_COEF * pre_act * pre_act)


def layer_norm_hat(rows_f32):
    centered = rows_f32 - jnp.mean(rows_f32, **ROWS)
    inv_std = lax.rsqrt(jnp.mean(centered * centered, **ROWS) + LN_EPS)
    return centered * inv_std, inv_std


LN_ROWS = 32
TILE = 1280
VMEM = pl.BlockSpec(memory_space=pltpu.VMEM)
HBM = pl.BlockSpec(memory_space=pl.ANY)
DMA = pltpu.SemaphoreType.DMA
COMM = DMA((12,))
PAIR = DMA((2,))
shape = jax.ShapeDtypeStruct


def tile_at(i, size):
    return pl.ds(pl.multiple_of(i * size, size), size)


def start_copies(sem, *pairs):
    copies = [pltpu.make_async_copy(src, dst, sem.at[i]) for i, (src, dst) in enumerate(pairs)]
    for copy in copies:
        copy.start()
    return copies


def loop(count, body, start=0):
    def step(i, carry):
        body(i)
        return carry

    lax.fori_loop(start, count, step, 0)


def comm_call(kernel, name, ident, flops, args, in_specs, out_shape, out_specs, scratch, aliases={}):
    return pl.pallas_call(
        kernel, in_specs=in_specs, out_specs=out_specs, out_shape=out_shape, scratch_shapes=scratch, name=name,
        input_output_aliases=aliases,
        compiler_params=pltpu.CompilerParams(collective_id=ident, has_side_effects=True, vmem_limit_bytes=66_000_000),
        cost_estimate=pl.CostEstimate(flops=flops, bytes_accessed=flops // 1000, transcendentals=flops // 1000),
    )(*args)


class Tiles:
    def __init__(self, buf, out, sem, rows=False):
        self.buf, self.out, self.sem, self.rows = buf, out, sem, rows

    def copy(self, n):
        size = self.buf.shape[1 if self.rows else 2]
        at = tile_at(n, size)
        dst = self.out.at[at] if self.rows else self.out.at[:, at]
        return pltpu.make_async_copy(self.buf.at[n % 2], dst, self.sem.at[n % 2])

    def put(self, n, value):
        @pl.when(n >= 2)
        def _():
            self.copy(n - 2).wait()

        self.buf[n % 2] = value()
        self.copy(n).start()

    def finish(self, count):
        self.copy(count - 2).wait()
        self.copy(count - 1).wait()


OUT_TILE = 512


def flat_cols(ref, cols):
    return ref[:, :, cols].reshape(ref.shape[0] * ref.shape[1], OUT_TILE)


def fwd_kernel(dout_ref, q_hbm, k_hbm, v_hbm, x_hbm, mid_hbm, gain1_ref, bias1_ref, gain2_ref, bias2_ref,
               dfull, ctx_ref, wide_ref, max_ref, inv_ref, h1_ref, h2_ref,
               k_rows, strip, q_ref, k_ref, v_ref, x_ref, mid_ref, own_sem, load_sem, *comm_sems):
    place = Place()
    place.barrier()
    gather = Gather(place, dout_ref, dfull, *comm_sems)
    gather.start()
    loads = start_copies(load_sem, (x_hbm, x_ref), (mid_hbm, mid_ref), (k_hbm, k_ref), (q_hbm, q_ref), (v_hbm, v_ref))
    own_copy = pltpu.make_async_copy(dout_ref, dfull.at[place.me], own_sem)
    own_copy.start()
    heads, dim, seq = q_ref.shape
    exp_scale = dim ** -0.5 * LOG2E
    loads[0].wait()
    loads[1].wait()
    affine = [ref[...].reshape(1, ref.shape[0]) for ref in (gain1_ref, bias1_ref, gain2_ref, bias2_ref)]

    def norm_rows(i):
        at = tile_at(i, LN_ROWS)
        for row, (src, dst) in enumerate(((x_ref, h1_ref), (mid_ref, h2_ref))):
            x_hat, _ = layer_norm_hat(src[at, :].astype(F32))
            dst[at, :] = (x_hat * affine[2 * row] + affine[2 * row + 1]).astype(BF16)

    loop(x_ref.shape[0] // LN_ROWS, norm_rows)
    for copy in loads[2:]:
        copy.wait()

    def head(h):
        k_rows[...] = k_ref[h].T

        def query_block(qi):
            q_at = tile_at(qi, BLK)
            q_blk = q_ref[h, :, q_at]

            def score_step(ki, run_max):
                at = tile_at(ki, BLK)
                blk = dot(k_rows[at, :], q_blk)
                strip[at, :] = blk
                return jnp.maximum(run_max, jnp.max(blk, **COLS))

            diag = causal_fill(dot(k_rows[q_at, :], q_blk), -1e30)
            strip[q_at, :] = diag
            row_max = lax.fori_loop(0, qi, score_step, jnp.max(diag, **COLS))

            def exp_step(ki, run_sum):
                at = tile_at(ki, BLK)
                probs = jnp.exp2((strip[at, :] - row_max) * exp_scale)
                strip[at, :] = probs
                return run_sum + jnp.sum(probs, **COLS)

            row_inv = 1.0 / lax.fori_loop(0, qi + 1, exp_step, jnp.zeros_like(row_max))

            def ctx_step(ki, carry):
                high, low = carry
                at = tile_at(ki, BLK)
                probs = strip[at, :] * row_inv
                probs_low = probs.astype(BF16)
                rest = (probs - probs_low.astype(F32)).astype(BF16)
                v_blk = v_ref[h, :, at]
                return high + dot(v_blk, probs_low), low + dot(v_blk, rest)

            zero = jnp.zeros((dim, BLK), F32)
            high, low = lax.fori_loop(0, qi + 1, ctx_step, (zero, zero))
            ctx_ref[h, :, q_at] = high.astype(BF16)
            wide_ref[h, :, q_at] = high + low
            max_ref[h, :, q_at] = row_max
            inv_ref[h, :, q_at] = row_inv

        loop(seq // BLK, query_block)

    def head_step(h):
        head(h)

        @pl.when(h == 1)
        def _():
            gather.relay()

        @pl.when(h == 2)
        def _():
            gather.forward('X')
            gather.forward('Y')

    loop(heads, head_step)
    gather.forward('D')
    gather.links.wait('CO', 'CX', 'CY', 'CD')
    own_copy.wait()
    gather.links.finish()


def fwd_call(d_out, q_t, k_t, v_t, x_in, x_mid, affine):
    heads, dim, seq = q_t.shape
    rows, model = d_out.shape
    return comm_call(
        fwd_kernel, "attn_fwd", 0, 40_000_000_000, (d_out, q_t, k_t, v_t, x_in, x_mid, *affine),
        [VMEM] + [HBM] * 5 + [VMEM] * 4,
        [shape((seq // rows, rows, model), BF16), shape((heads, dim, seq), BF16), shape((heads, dim, seq), F32),
         shape((heads, 1, seq), F32), shape((heads, 1, seq), F32), shape((rows, model), BF16), shape((rows, model), BF16)],
        [HBM] + [VMEM] * 6,
        [pltpu.VMEM((seq, dim), BF16), pltpu.VMEM((seq, BLK), F32)] + [pltpu.VMEM(q_t.shape, BF16)] * 3
        + [pltpu.VMEM((rows, model), BF16)] * 2 + [DMA(()), DMA((5,))] + [COMM] * 2)


def dot_t(a, b):
    return lax.dot_general(a, b, (((1,), (1,)), ((), ())), preferred_element_type=F32)


def mlp_kernel(dfull, dout_hbm, mid_hbm, gain_ref, h2_ref, z_ref, w2_ref, w1_ref,
               dx1_ref, dz_ref, gb1_ref, vec_ref, h2full,
               w2v, w1v, dzv, ybuf, part, crecv, diag_recv, last_recv, dout_ref, mid_ref,
               load_sem, y_sem, z_sem, dz_sem, own_sem, *comm_sems):
    place = Place()
    place.barrier()
    rows, model = dout_hbm.shape
    hidden = w2v.shape[0]
    scatter = Scatter(place, part, crecv, diag_recv, last_recv, *comm_sems[0:2])
    gather = ThirdGather(place, h2full, *comm_sems[2:4])
    gather.start('near', h2_ref)
    own_copy = pltpu.make_async_copy(h2_ref, h2full.at[place.me], own_sem)

    def load_pair(i):
        return pltpu.make_async_copy(dfull.at[pl.ds(2 * place.pair_at(i), 2)], ybuf.at[i % 2], y_sem.at[i])

    def store_grad(i):
        at = tile_at(place.pair_at(i), 2 * rows)
        return pltpu.make_async_copy(dzv.at[at], dz_ref.at[at], dz_sem.at[i])

    def load_pre(i):
        at = tile_at(place.pair_at(i), 2 * rows)
        return pltpu.make_async_copy(z_ref.at[at], dzv.at[at], z_sem.at[i])

    load_pair(0).start()
    load_pre(0).start()
    loads = start_copies(load_sem, (w2_ref, w2v), (w1_ref, w1v), (dout_hbm, dout_ref), (mid_hbm, mid_ref))
    for i in range(1, 4):
        load_pre(i).start()
    load_pair(1).start()
    own_copy.start()
    gb1_ref[...] = jnp.zeros_like(gb1_ref)
    vec_ref[...] = jnp.zeros_like(vec_ref)
    loads[0].wait()

    def pair_step(i):
        slot = i % 2
        pair = place.pair_at(i)
        at = tile_at(pair, 2 * rows)
        load_pair(i).wait()
        load_pre(i).wait()

        def grad_act(n):
            cols = tile_at(n, TILE)
            acc = dot_t(ybuf[slot].reshape(2 * rows, model), w2v[cols, :])
            grad = (acc * gelu_slope(dzv[at, cols].astype(F32))).astype(BF16)
            dzv[at, cols] = grad
            gb1_ref[:, cols] += jnp.sum(grad.astype(F32), **COLS)

        loop(hidden // TILE, grad_act)
        store_grad(i).start()

        @pl.when(i < 2)
        def _():
            load_pair(i + 2).start()

        @pl.when(i == 0)
        def _():
            loads[1].wait()

        @pl.when(i == 2)
        def _():
            gather.forward('near')

        scatter.between(i)

        def grad_norm(n):
            cols = tile_at(n, TILE)
            acc = dot_t(dzv[at, :], w1v[cols, :]).astype(BF16)
            part[2 * pair, :, cols] = acc[:rows]
            part[2 * pair + 1, :, cols] = acc[rows:]

        loop(model // TILE, grad_norm)
        scatter.after(i)

    loop(4, pair_step)
    scatter.add_diag()

    gain = gain_ref[...].reshape(1, model)
    loads[2].wait()
    loads[3].wait()

    def norm_rows(at):
        grad = scatter.total(at)
        x_hat, inv_std = layer_norm_hat(mid_ref[at, :].astype(F32))
        dout_rows = dout_ref[at, :].astype(F32)
        mid = (dout_rows + layer_norm_bwd(grad, x_hat, inv_std, gain)).astype(BF16)
        dx1_ref[at, :] = mid
        for row, val in enumerate((grad * x_hat, grad, mid.astype(F32), dout_rows)):
            vec_ref[row + 2:row + 3, :] += jnp.sum(val, **COLS)

    scatter.norm_loop(norm_rows)
    for i in range(4):
        store_grad(i).wait()
    own_copy.wait()
    gather.wait_pair('near')
    gather.links.finish()
    scatter.links.finish()


def scatter_scratch(rows, model):
    return [pltpu.VMEM((8, rows, model), BF16), pltpu.VMEM((4, rows, model), BF16),
            pltpu.VMEM((2, rows // 2, model), BF16), pltpu.VMEM((2, rows, model), BF16)]


def mlp_call(dfull, d_out, x_mid, gain, h1, z_saved, w2, w1):
    rows, model = d_out.shape
    seq, hidden = z_saved.shape
    return comm_call(
        mlp_kernel, "mlp_grads", 1, 60_000_000_000, (dfull, d_out, x_mid, gain, h1, z_saved, w2, w1),
        [HBM] * 3 + [VMEM] + [HBM] * 4,
        [shape((rows, model), BF16), shape((seq, hidden), BF16), shape((1, hidden), F32), shape((8, model), F32),
         shape(dfull.shape, BF16)],
        [VMEM, HBM, VMEM, VMEM, HBM],
        [pltpu.VMEM((hidden, model), BF16), pltpu.VMEM((model, hidden), BF16),
         pltpu.VMEM((seq, hidden), BF16), pltpu.VMEM((2, 2, rows, model), BF16)]
        + scatter_scratch(rows, model) + [pltpu.VMEM((rows, model), BF16)] * 2
        + [DMA((4,))] * 4 + [DMA(())] + [COMM] * 4)


def gelu(pre_act):
    return 0.5 * pre_act * (1.0 + jnp.tanh(GELU_SCALE * (pre_act + GELU_COEF * pre_act * pre_act * pre_act)))


def ctx_kernel(dx1_ref, wo_ref, z_ref, dfull, mfull, do_ref, dw2_ref,
               mbuf, zv, ut, yv, obuf, own_sem, m_sem, load_sem, out_sem, *comm_sems):
    place = Place()
    place.barrier()
    rows, model = dx1_ref.shape
    gather = Gather(place, dx1_ref, mfull, *comm_sems)
    gather.start()
    own_copy = pltpu.make_async_copy(dx1_ref, mfull.at[place.me], own_sem)
    own_copy.start()

    loads = [pltpu.make_async_copy(z_ref, zv, load_sem.at[0]), pltpu.make_async_copy(dfull, yv, load_sem.at[1])]
    for copy in loads:
        copy.start()
    tiles = Tiles(obuf, dw2_ref, out_sem)
    count = model // OUT_TILE

    def turn(n):
        cols = tile_at(n, 256)
        ut[cols, :] = gelu(zv[:, cols].astype(F32)).astype(BF16).T

    def weight_tile(n):
        cols = tile_at(n, OUT_TILE)
        tiles.put(n, lambda: dot(ut[...], flat_cols(yv, cols)))

    loads[0].wait()
    loop(ut.shape[0] // 256, turn)
    gather.relay()
    loads[1].wait()
    loop(count, weight_tile)
    gather.forward('X')
    gather.forward('Y')
    own_copy.wait()
    gather.links.wait('CO')

    def grad_ctx(i):
        @pl.when(i == 1)
        def _():
            gather.links.wait('CY')

        @pl.when(i == 2)
        def _():
            gather.links.wait('CX')

        @pl.when(i == 3)
        def _():
            gather.forward('D')
            gather.links.wait('CD')

        pair = place.pair_at(3 - i)
        copy = pltpu.make_async_copy(mfull.at[pl.ds(2 * pair, 2)], mbuf, m_sem)
        copy.start()
        copy.wait()
        do_ref[:, tile_at(pair, 2 * rows)] = dot_t(wo_ref[...], mbuf[...].reshape(2 * rows, model)).astype(BF16)

    loop(4, grad_ctx)
    tiles.finish(count)
    gather.links.finish()


def ctx_call(dx1, w_rows, z_saved, dfull):
    rows, model = dx1.shape
    feats = w_rows.shape[0]
    seq, hidden = z_saved.shape
    return comm_call(
        ctx_kernel, "ctx_grads", 2, 30_000_000_000, (dx1, w_rows, z_saved, dfull), [VMEM] * 2 + [HBM] * 2,
        [shape((seq // rows, rows, model), BF16), shape((feats, seq), BF16), shape((hidden, model), F32)], [HBM, VMEM, HBM],
        [pltpu.VMEM((2, rows, model), BF16), pltpu.VMEM((seq, hidden), BF16), pltpu.VMEM((hidden, seq), BF16),
         pltpu.VMEM((seq // rows, rows, model), BF16), pltpu.VMEM((2, hidden, OUT_TILE), F32),
         DMA(()), DMA(()), PAIR, PAIR] + [COMM] * 2)


def bwd_kernel(h1_ref, q_hbm, k_hbm, v_hbm, do_hbm, wide_hbm, max_ref, inv_ref, dz_ref, h2_in,
               h2full, h1full, out_ref, dw1_ref,
               k_rows, v_rows, q_rows, do_rows, delta, dq_acc, dk_acc, dv_acc, tok, dzv, wbuf,
               q_ref, k_ref, v_ref, do_ref, wide_ref, own_sem, head_sem, load_sem, out_sem, *comm_sems):
    place = Place()
    place.barrier()
    gather1 = ThirdGather(place, h1full, *comm_sems[0:2])
    gather2 = ThirdGather(place, h2full, *comm_sems[2:4])
    gather2.start('rest', None)
    gather2.start('diag', None)
    gather1.start('near', h1_ref)
    gather1.start('rest', h1_ref)
    loads = start_copies(head_sem, (k_hbm, k_ref), (v_hbm, v_ref), (q_hbm, q_ref), (do_hbm, do_ref), (wide_hbm, wide_ref))
    own_copy = pltpu.make_async_copy(h1_ref, h1full.at[place.me], own_sem)
    own_copy.start()
    heads, dim, seq = q_ref.shape
    blocks = seq // BLK
    scale = dim ** -0.5
    exp_scale = scale * LOG2E

    def head(h):
        k_rows[...] = k_ref[h].T
        v_rows[...] = v_ref[h].T
        q_rows[...] = q_ref[h].T
        do_rows[...] = do_ref[h].T
        delta[...] = jnp.sum(do_ref[h].astype(F32) * wide_ref[h], **COLS)
        dq_acc[...] = jnp.zeros_like(dq_acc)
        dk_acc[...] = jnp.zeros_like(dk_acc)
        dv_acc[...] = jnp.zeros_like(dv_acc)

        def block(qi, ki, on_diag):
            q_at, k_at = tile_at(qi, BLK), tile_at(ki, BLK)
            scores = dot(k_rows[k_at, :], q_ref[h, :, q_at])
            if on_diag:
                scores = causal_fill(scores, -1e30)
            probs = jnp.exp2((scores - max_ref[h, :, q_at]) * exp_scale) * inv_ref[h, :, q_at]
            grad_probs = dot(v_rows[k_at, :], do_ref[h, :, q_at])
            dv_acc[k_at, :] += dot(probs.astype(BF16), do_rows[q_at, :])
            grad_scores = (probs * (grad_probs - delta[:, q_at]) * scale).astype(BF16)
            dk_acc[k_at, :] += dot(grad_scores, q_rows[q_at, :])
            dq_acc[:, q_at] += dot(k_ref[h, :, k_at], grad_scores)

        loop(blocks, lambda i: block(i, i, True))
        loop(blocks, lambda ki: loop(blocks, lambda qi: block(qi, ki, False), ki + 1))
        out_ref[0, h] = dq_acc[...].astype(BF16)
        out_ref[1, h] = dk_acc[...].astype(BF16).T
        out_ref[2, h] = dv_acc[...].astype(BF16).T

    load_grad, load_tok = [pltpu.make_async_copy(src, dst, load_sem.at[i])
                           for i, (src, dst) in enumerate(((dz_ref, dzv), (h2full, tok)))]
    for copy in loads:
        copy.wait()
    count = tok.shape[2] // OUT_TILE
    tiles = Tiles(wbuf, dw1_ref, out_sem, rows=True)

    def fc1_tile(n):
        cols = tile_at(n, OUT_TILE)
        tiles.put(n, lambda: dot(flat_cols(tok, cols).T, dzv[...]))

    def head_step(h):
        head(h)

        @pl.when(h == 1)
        def _():
            load_grad.start()
            gather2.forward('rest')

        @pl.when(h == heads - 2)
        def _():
            gather2.forward('diag')
            gather2.wait_pair('rest')

    loop(heads - 1, head_step)
    gather2.wait_pair('diag')
    load_tok.start()
    head(heads - 1)
    load_grad.wait()
    load_tok.wait()
    loop(count, fc1_tile)
    for third in ('near', 'rest'):
        gather1.forward(third)
    for third in ('near', 'rest'):
        gather1.wait_pair(third)
    own_copy.wait()
    tiles.finish(count)
    gather1.links.finish()
    gather2.links.finish()


def bwd_call(h1, q_t, k_t, v_t, do_t, wide, row_max, row_inv, dz, h2full):
    heads, dim, seq = q_t.shape
    rows, model = h1.shape
    full = shape((seq // rows, rows, model), BF16)
    turned = pltpu.VMEM((seq, dim), BF16)
    hidden = dz.shape[1]
    return comm_call(
        bwd_kernel, "attn_bwd", 3, 80_000_000_000,
        (h1, q_t, k_t, v_t, do_t, wide, row_max, row_inv, dz, h2full), [VMEM] + [HBM] * 5 + [VMEM] * 2 + [HBM] * 2,
        [full, full, shape((3, heads, dim, seq), BF16), shape((model, hidden), F32)], [HBM, HBM, VMEM, HBM],
        [turned] * 4 + [pltpu.VMEM((1, seq), F32), pltpu.VMEM((dim, seq), F32), pltpu.VMEM((seq, dim), F32),
                        pltpu.VMEM((seq, dim), F32), pltpu.VMEM((seq // rows, rows, model), BF16),
                        pltpu.VMEM((seq, hidden), BF16), pltpu.VMEM((2, OUT_TILE, hidden), F32),
                        *[pltpu.VMEM(q_t.shape, BF16)] * 4, pltpu.VMEM(wide.shape, F32),
                        DMA(()), DMA((5,)), PAIR, PAIR] + [COMM] * 4,
        aliases={9: 0})


def qkv_kernel(qkv_hbm, w_hbm, dx1_hbm, x_hbm, gain_ref, vec_ref, ctx_hbm, mfull, h1_in,
               dx_ref, vsum_ref, bias_ref, dwo_ref, dw_ref, h1full,
               turned, part, crecv, diag_recv, last_recv, vacc, vsend, vrecv, last_got, tok, obuf, wbuf,
               qkv_ref, w_ref, dx1_ref, x_ref, ctx_ref, vsem, last_sem, load_sem, in_sem, out_sem, *comm_sems):
    place = Place()
    place.barrier(everyone=True)
    rows, model = dx1_ref.shape
    scatter = Scatter(place, part, crecv, diag_recv, last_recv, *comm_sems[0:2])
    gather = ThirdGather(place, h1full, *comm_sems[2:4])
    gather.start('diag', None)
    inputs = start_copies(in_sem, (qkv_hbm, qkv_ref), (w_hbm, w_ref), (ctx_hbm, ctx_ref), (dx1_hbm, dx1_ref), (x_hbm, x_ref))
    loads = [pltpu.make_async_copy(src, tok, load_sem.at[i]) for i, src in enumerate((mfull, h1full))]
    tiles_o = Tiles(obuf, dwo_ref, out_sem.at[0])
    tiles = Tiles(wbuf, dw_ref, out_sem.at[1])
    count = model // OUT_TILE
    swaps = Links(place, vsem.at[0], vsem.at[1])
    inputs[0].wait()

    def vec_step(i):
        if i > 0:
            swaps.wait('CXY'[i - 1])
            vacc[...] += vrecv[i - 1]
        if i < 3:
            vsend[i] = vacc[...]

    def vec_send(i):
        swaps.send('CXY'[i], 'CXY'[i], vsend, vrecv, i)

    vacc[...] = vec_ref[...]
    vec_step(0)
    vec_send(0)

    def pair_step(i):
        pair = place.pair_at(i)
        turned[...] = qkv_ref[:, tile_at(pair, 2 * rows)].T

        @pl.when(i == 0)
        def _():
            inputs[1].wait()

        @pl.when(i == 1)
        def _():
            loads[0].start()

        @pl.when(i == 3)
        def _():
            gather.forward('diag')

        for at in range(1, 3):
            @pl.when(i == at)
            def _():
                vec_step(at)
                vec_send(at)

        scatter.between(i)

        def grad_norm(n):
            cols = tile_at(n, TILE)
            acc = dot(turned[...], w_ref[:, cols]).astype(BF16)
            part[2 * pair, :, cols] = acc[:rows]
            part[2 * pair + 1, :, cols] = acc[rows:]

        loop(model // TILE, grad_norm)
        scatter.after(i)

    loop(4, pair_step)
    loads[0].wait()
    for copy in inputs[2:]:
        copy.wait()

    def proj_tile(n):
        cols = tile_at(n, OUT_TILE)
        tiles_o.put(n, lambda: dot(ctx_ref[...], flat_cols(tok, cols)))

    def qkv_tile(n):
        cols = tile_at(n, OUT_TILE)
        tiles.put(n, lambda: dot(qkv_ref[...], flat_cols(tok, cols)))

    loop(count, proj_tile)
    scatter.add_diag()
    gather.wait_pair('diag')
    loads[1].start()
    ones = jnp.ones((8, qkv_ref.shape[1]), BF16)
    bias_ref[...] = dot_t(ones, qkv_ref[...])
    loads[1].wait()
    loop(count, qkv_tile)
    vec_step(3)
    tiles_o.finish(count)
    gain = gain_ref[...].reshape(1, model)

    def norm_rows(at):
        grad = scatter.total(at)
        x_hat, inv_std = layer_norm_hat(x_ref[at, :].astype(F32))
        dx_ref[at, :] = (dx1_ref[at, :].astype(F32) + layer_norm_bwd(grad, x_hat, inv_std, gain)).astype(BF16)
        vacc[0:1, :] += jnp.sum(grad * x_hat, **COLS)
        vacc[1:2, :] += jnp.sum(grad, **COLS)

    scatter.norm_loop(norm_rows)
    finals = Links(place, last_sem.at[0], last_sem.at[1])
    last_got[0] = vacc[0:2, :]
    vsum_ref[2:6, :] = vacc[2:6, :]
    for k in range(1, 8):
        finals.send(k, k, (last_got, (0,)), (last_got, (k,)))
    tiles.finish(count)
    finals.wait(*range(1, 8))
    total = last_got[place.me]
    for source in range(1, 8):
        total += last_got[(place.me + 8 - source) % 8]
    vsum_ref[0:2, :] = total
    for links in (swaps, finals, scatter.links, gather.links):
        links.finish()


def qkv_call(qkv_rows, w_rows, dx1, x_in, gain, vec, ctx_rows, mfull, h1full):
    rows, model = dx1.shape
    feats, seq = qkv_rows.shape
    proj = ctx_rows.shape[0]
    return comm_call(
        qkv_kernel, "qkv_grads", 4, 30_000_000_000,
        (qkv_rows, w_rows, dx1, x_in, gain, vec, ctx_rows, mfull, h1full), [HBM] * 4 + [VMEM] * 2 + [HBM] * 3,
        [shape((rows, model), BF16), shape((6, model), F32), shape((8, feats), F32), shape((proj, model), F32),
         shape((feats, model), F32), shape(h1full.shape, BF16)],
        [VMEM] * 3 + [HBM] * 3,
        [pltpu.VMEM((2 * rows, feats), BF16)] + scatter_scratch(rows, model)
        + [pltpu.VMEM((8, model), F32), pltpu.VMEM((3, 8, model), F32), pltpu.VMEM((3, 8, model), F32),
           pltpu.VMEM((8, 2, model), F32), pltpu.VMEM((8, rows, model), BF16),
           pltpu.VMEM((2, proj, OUT_TILE), F32), pltpu.VMEM((2, feats, OUT_TILE), F32),
           pltpu.VMEM((feats, seq), BF16), pltpu.VMEM((feats, model), BF16), pltpu.VMEM((rows, model), BF16),
           pltpu.VMEM((rows, model), BF16), pltpu.VMEM((proj, seq), BF16),
           DMA((2, 3)), DMA((2, 7)), PAIR, DMA((5,)), DMA((2, 2))] + [COMM] * 4,
        aliases={8: 5})


def finish_kernel(*refs):
    count = (len(refs) - 8) // 2
    rings, single, (small_sem, in_sem, out_sem) = refs[2 * count:2 * count + 2], refs[-6:-3], refs[-3:]
    chunks, used = [], [0, 0]
    small = [(src, buf, dst) for src, buf, dst in zip(refs[4:count], single, refs[count + 4:2 * count])]
    for i, (src, buf, _) in enumerate(small):
        pltpu.make_async_copy(src, buf, small_sem.at[0, i]).start()
    for src, dst in zip(refs[:4], refs[count:count + 4]):
        kind = 0 if src.shape[1] == rings[0].shape[2] else 1
        rows = rings[kind].shape[1]
        for row in range(0, src.shape[0], rows):
            chunks.append((src.at[pl.ds(row, rows)], dst.at[pl.ds(row, rows)], kind, used[kind]))
            used[kind] += 1

    def copy_in(src, dst, kind, at):
        slot = at % RING
        return pltpu.make_async_copy(src, rings[kind].at[slot], in_sem.at[kind, slot])

    def copy_out(src, dst, kind, at):
        slot = at % RING
        return pltpu.make_async_copy(rings[kind].at[slot], dst, out_sem.at[kind, slot])

    waiting = {}

    def start(chunk):
        key = (chunk[2], chunk[3] % RING)
        if key in waiting:
            copy_out(*waiting.pop(key)).wait()
        copy_in(*chunk).start()

    for chunk in chunks[:AHEAD]:
        start(chunk)
    for i, (src, buf, dst) in enumerate(small):
        pltpu.make_async_copy(src, buf, small_sem.at[0, i]).wait()
        pltpu.make_async_copy(buf, dst, small_sem.at[1, i]).start()
    for i, chunk in enumerate(chunks):
        copy_in(*chunk).wait()
        copy_out(*chunk).start()
        waiting[(chunk[2], chunk[3] % RING)] = chunk
        if i + AHEAD < len(chunks):
            start(chunks[i + AHEAD])
    for chunk in waiting.values():
        copy_out(*chunk).wait()
    for i, (_, buf, dst) in enumerate(small):
        pltpu.make_async_copy(buf, dst, small_sem.at[1, i]).wait()


RING = 32
AHEAD = 20


def finish_call(*arrays):
    wide = max(a.shape[1] for a in arrays[:4])
    narrow = min(a.shape[1] for a in arrays[:4])
    small = [pltpu.VMEM(a.shape, a.dtype) for a in arrays[4:]]
    return pl.pallas_call(
        finish_kernel, name="finish", in_specs=[HBM] * len(arrays), out_specs=[HBM] * len(arrays),
        out_shape=[shape(a.shape, a.dtype) for a in arrays],
        scratch_shapes=[pltpu.VMEM((RING, 64, wide), F32), pltpu.VMEM((RING, 128, narrow), F32), *small,
                        DMA((2, len(small))), DMA((2, RING)), DMA((2, RING))],
        compiler_params=pltpu.CompilerParams(vmem_limit_bytes=66_000_000),
        cost_estimate=pl.CostEstimate(flops=1_000_000, bytes_accessed=72_000_000, transcendentals=0),
    )(*arrays)


def solution(mesh):
    def local_backward(x_in, x_mid, d_out, q_saved, k_saved, v_saved, z_saved, ln1_gain, ln1_bias, ln2_gain, ln2_bias, w_qkv, w_proj, w_fc1, w_fc2):
        x_in, x_mid, d_out, z_saved = x_in[0], x_mid[0], d_out[0], z_saved[0]
        heads, dim = q_saved.shape[2:]
        seq, model = z_saved.shape[0], x_in.shape[1]
        q_t, k_t, v_t = (v[0].transpose(1, 2, 0) for v in (q_saved, k_saved, v_saved))
        affine = (ln1_gain, ln1_bias, ln2_gain, ln2_bias)
        dfull, ctx_t, wide_t, row_max, row_inv, h1_local, h2_local = fwd_call(d_out, q_t, k_t, v_t, x_in, x_mid, affine)
        dx1, grad_pre, grad_bfc1, vec, h2_full = mlp_call(dfull, d_out, x_mid, ln2_gain, h2_local, z_saved, w_fc2, w_fc1)
        mfull, do_t, grad_wfc2 = ctx_call(dx1, w_proj.reshape(heads * dim, model), z_saved, dfull)
        _, h1_full, qkv_t, grad_wfc1 = bwd_call(
            h1_local, q_t, k_t, v_t, do_t.reshape(heads, dim, seq), wide_t, row_max, row_inv, grad_pre, h2_full)
        qkv_rows = qkv_t.reshape(3 * heads * dim, seq)
        w_rows = w_qkv.transpose(0, 2, 3, 1).reshape(3 * heads * dim, model)
        grad_x, grad_vecs, bias_rows, grad_wproj, grad_wqkv, _ = qkv_call(
            qkv_rows, w_rows, dx1, x_in, ln1_gain, vec, ctx_t.reshape(heads * dim, seq), mfull, h1_full)
        grad_wfc2, grad_wfc1, grad_wqkv, grad_wproj, grad_x, grad_vecs, grad_bfc1 = finish_call(
            grad_wfc2, grad_wfc1, grad_wqkv, grad_wproj, grad_x, grad_vecs, grad_bfc1)
        grad_wproj = grad_wproj.reshape(heads, dim, model)
        grad_wqkv = grad_wqkv.reshape(3, heads, dim, model).transpose(0, 3, 1, 2)
        grad_bqkv = bias_rows[0].reshape(3, heads, dim)
        return grad_x[None], grad_wqkv, grad_bqkv, grad_wproj, grad_wfc1, grad_bfc1[0], grad_wfc2, grad_vecs

    tok_spec = P('dp', 'tp', None)
    head_spec = P('dp', None, 'tp', None)
    in_specs = (tok_spec, tok_spec, tok_spec, head_spec, head_spec, head_spec, P('dp', None, 'tp'),
                P(None), P(None), P(None), P(None),
                P(None, None, 'tp', None), P('tp', None, None), P(None, 'tp'), P('tp', None))
    out_specs = (tok_spec, P('dp', None, 'tp', None), P('dp', 'tp', None), P(('dp', 'tp'), None, None),
                 P('dp', 'tp'), P(('dp', 'tp')), P(('dp', 'tp'), None), P('dp', None))
    return jax.shard_map(local_backward, mesh=mesh, in_specs=in_specs, out_specs=out_specs, check_vma=False)
```

```python
import jax
import jax.numpy as jnp
from jax import lax
from jax.experimental import pallas as pl
from jax.experimental.pallas import tpu as pltpu
from jax.sharding import PartitionSpec as P

LN_EPS = 1e-5
GELU_COEF = 0.044715
GELU_SCALE = 0.7978845608028654
LOG2E = 1.4426950408889634
BLK = 512
F32 = jnp.float32
BF16 = jnp.bfloat16
DIM0, DIM1, DIM2 = range(3)
COLS = dict(axis=0, keepdims=True)
ROWS = dict(axis=-1, keepdims=True)


def layer_norm_bwd(grad_norm, x_hat, inv_std, norm_gain):
    grad_hat = grad_norm * norm_gain
    centered_grad = grad_hat - jnp.mean(grad_hat, **ROWS)
    return inv_std * (centered_grad - x_hat * jnp.mean(grad_hat * x_hat, **ROWS))


def dot(a, b):
    return jnp.dot(a, b, preferred_element_type=F32)


def causal_fill(scores, fill):
    key_ids = lax.broadcasted_iota(jnp.int32, scores.shape, 0)
    query_ids = lax.broadcasted_iota(jnp.int32, scores.shape, 1)
    return jnp.where(query_ids >= key_ids, scores, fill)


class Place:
    def __init__(self):
        self.group = lax.axis_index('dp')
        self.me = lax.axis_index('tp')
        self.core = self.me % 2
        self.dx = 2 - 4 * ((self.me // 2) % 2)
        self.dy = 4 - 8 * (self.me // 4)
        self.dc = 1 - 2 * self.core
        self.peer = {'X': self.me + self.dx, 'Y': self.me + self.dy, 'C': self.me + self.dc}
        self.peer.update({k: (self.me + k) % 8 for k in range(1, 8)})
        self.block = {'O': self.me, 'X': self.me + self.dx, 'Y': self.me + self.dy, 'D': self.me + self.dx + self.dy}
        self.pair = {key: val // 2 for key, val in self.block.items()}
        self.other = {key: val + self.dc for key, val in self.block.items()}
        self.x, self.y = (self.me // 2) % 2, self.me // 4

    def pair_at(self, i):
        flip_x, flip_y = 1 - i // 2, 1 - i % 2
        return 2 * (self.y + flip_y * (1 - 2 * self.y)) + self.x + flip_x * (1 - 2 * self.x)

    def chunk(self, i, c):
        mixed = i * (3 - i) // 2
        pair, half = (self.pair['X'], i - 1) if c < 2 else (self.pair['Y'], 2 - i)
        slot = (1 - mixed) * (2 * self.pair_at(i) + c // 2) + mixed * (2 * pair + c % 2)
        return slot, (1 - mixed) * (c % 2) + mixed * half

    def barrier(self, everyone=False):
        sem = pltpu.get_barrier_semaphore()
        keys = range(1, 8) if everyone else 'XYC'
        for key in keys:
            pl.semaphore_signal(sem, inc=1, device_id=(self.group, self.peer[key]), device_id_type=pl.DeviceIdType.MESH)
        pl.semaphore_wait(sem, len(keys))


class Links:
    def __init__(self, place, send_sem, recv_sem):
        self.place, self.send_sem, self.recv_sem = place, send_sem, recv_sem
        self.copies = {}

    def define(self, name, to, src, dst, *index):
        at = len(self.copies)

        def place_of(ref):
            ref, where = ref if isinstance(ref, tuple) else (ref, index)
            return ref.at[where] if where else ref

        def copy():
            return pltpu.make_async_remote_copy(
                src_ref=place_of(src), dst_ref=place_of(dst), send_sem=self.send_sem.at[at], recv_sem=self.recv_sem.at[at],
                device_id=(self.place.group, self.place.peer[to]), device_id_type=pl.DeviceIdType.MESH)

        self.copies[name] = copy

    def start(self, name):
        self.copies[name]().start()

    def send(self, name, *rest):
        self.define(name, *rest)
        self.start(name)

    def wait(self, *names):
        for name in names:
            self.copies[name]().wait_recv()

    def finish(self):
        for copy in self.copies.values():
            copy().wait_send()


class Gather:
    COPIES = 10

    def __init__(self, place, own, full, send_sem, recv_sem):
        self.place, self.own, self.full = place, own, full
        self.links = Links(place, send_sem, recv_sem)
        half = own.shape[DIM0] // 2
        self.first, self.second = pl.ds(0, half), pl.ds(half, half)

    def start(self):
        me, full, own, send = self.place.me, self.full, self.own, self.links.send
        for name, half in (('Xa', self.first), ('Yb', self.second), ('Xb', self.second), ('Ya', self.first)):
            send(name, name[0], (own, (half,)), (full, (me, half)))
        send('CO', 'C', (own, ()), (full, (me,)))

    def relay(self):
        links, full, block = self.links, self.full, self.place.block
        links.wait('Xa')
        links.send('Da', 'Y', full, full, block['X'], self.first)
        links.wait('Yb')
        links.send('Db', 'X', full, full, block['Y'], self.second)

    def forward(self, key):
        first, second = ('Xb', None) if key == 'X' else ('Ya', None) if key == 'Y' else ('Da', 'Db')
        self.links.wait(first)
        if second:
            self.links.wait(second)
        self.links.send('C' + key, 'C', self.full, self.full, self.place.block[key])


class ThirdGather:
    def __init__(self, place, full, send_sem, recv_sem):
        self.place, self.full = place, full
        self.links = Links(place, send_sem, recv_sem)
        half = full.shape[DIM1] // 2
        self.first, self.second = pl.ds(0, half), pl.ds(half, half)

    def start(self, third, own):
        me, full, block = self.place.me, self.full, self.place.block
        near = {'near': {'X': self.first, 'Y': self.second}, 'rest': {'X': self.second, 'Y': self.first}}.get(third)
        for key in 'XY':
            if near is None:
                slot, half = (block['Y'], self.second) if key == 'X' else (block['X'], self.first)
                self.links.send(third + key, key, full, full, slot, half)
            else:
                src = (full, (me, near[key])) if own is None else (own, (near[key],))
                self.links.send(third + key, key, src, (full, (me, near[key])))
        if third == 'near':
            self.links.send('CO', 'C', (own, ()), (full, (me,)))

    def forward(self, third):
        block = self.place.block
        for key in 'XY':
            self.links.wait(third + key)
            half = self.first if (third == 'near') == (key == 'X') else self.second
            slot = block[key]
            if third == 'diag':
                slot, half = block['D'], (self.second if key == 'X' else self.first)
            self.links.send('C' + third + key, 'C', self.full, self.full, slot, half)

    def wait_pair(self, third):
        self.links.wait('C' + third + 'X', 'C' + third + 'Y', *(('CO',) if third == 'near' else ()))


CRECV = dict(O=0, Xa=1, Xb=1, Ya=2, Yb=2, D=3)


class Scatter:
    COPIES = 10

    def __init__(self, place, part, crecv, diag_recv, last_recv, send_sem, recv_sem):
        self.place, self.part, self.crecv = place, part, crecv
        self.diag_recv, self.last_recv = diag_recv, last_recv
        self.links = Links(place, send_sem, recv_sem)
        half = part.shape[DIM1] // 2
        self.half = {'a': pl.ds(0, half), 'b': pl.ds(half, half)}
        for name, at in CRECV.items():
            index = (at,) if len(name) == 1 else (at, self.half[name[1]])
            self.links.define('C' + name, 'C', (part, (place.other[name[0]],) + index[1:]), (crecv, index))

    def add_rows(self, slot, start, count, other, other_start):
        step = 64

        def body(i, carry):
            here = pl.ds(pl.multiple_of(start + i * step, step), step)
            there = pl.ds(pl.multiple_of(other_start + i * step, step), step)
            total = self.part[slot, here, :].astype(F32) + other[there, :].astype(F32)
            self.part[slot, here, :] = total.astype(BF16)
            return carry

        lax.fori_loop(0, count // step, body, 0)

    def store(self, i, cols, rows):
        for c in range(4):
            slot, half = self.place.chunk(i, c)
            size = rows.shape[DIM0] // 4
            self.part[slot, tile_at(half, size), cols] = rows[c * size:(c + 1) * size]

    def swap(self, *names):
        for name in names:
            self.links.start('C' + name)

    def add_pair(self, name):
        self.links.wait('C' + name)
        rows = self.part.shape[DIM1]
        start, count = (0, rows) if len(name) == 1 else ((rows // 2) * 'ab'.index(name[1]), rows // 2)
        self.add_rows(self.place.block[name[0]], start, count, self.crecv.at[CRECV[name]], start)

    def send_half(self, key, half):
        at = self.half[half]
        self.links.send(key + half, key, (self.part, (self.place.block[key], at)), (self.last_recv, ('XY'.index(key), at)))

    def send_diag(self):
        for i, (key, half) in enumerate((('X', 'a'), ('Y', 'b'))):
            self.links.send('D' + half, key, (self.part, (self.place.block['D'], self.half[half])), (self.diag_recv, (i,)))

    def add_diag(self):
        self.add_pair('Xb')
        self.add_pair('Ya')
        rows = self.part.shape[DIM1] // 4
        for i, (half, key, start) in enumerate((('a', 'Y', 0), ('b', 'X', 2 * rows))):
            self.links.wait('D' + half)
            for quarter in range(2):
                off = quarter * rows
                self.add_rows(self.place.block[key], start + off, rows, self.diag_recv.at[i], off)
                at = pl.ds(start + off, rows)
                self.links.send(key + half + str(quarter), key, (self.part, (self.place.block[key], at)),
                                (self.last_recv, ('XY'.index(key), at)))

    def wait_last(self, quarter):
        if quarter == 0:
            self.links.wait('Xa', 'Yb', 'CO')
        self.links.wait('Ya' + str(quarter), 'Xb' + str(quarter))

    def norm_loop(self, body):
        rows = self.part.shape[DIM1]
        chunks = rows // LN_ROWS
        quarter = chunks // 4

        def step(i):
            for part in range(2):
                @pl.when(i == part * (chunks // 2))
                def _():
                    self.wait_last(part)

            part, j = i // (2 * quarter), i % (2 * quarter)
            body(tile_at((j // quarter) * 2 * quarter + part * quarter + j % quarter, LN_ROWS))

        loop(chunks, step)

    def between(self, i):
        @pl.when(i == 1)
        def _():
            self.add_pair('D')
            self.send_diag()

        @pl.when(i == 2)
        def _():
            for name in ('Xa', 'Yb'):
                self.add_pair(name)
                self.send_half(*name)

    def after(self, i):
        for at, names in enumerate((('D',), ('Xa', 'Yb'), ('Xb', 'Ya'), ('O',))):
            @pl.when(i == at)
            def _():
                self.swap(*names)

    def total(self, at):
        me = self.place.me
        return (self.part[me, at, :].astype(F32) + self.crecv[0, at, :].astype(F32)
                + self.last_recv[0, at, :].astype(F32) + self.last_recv[1, at, :].astype(F32))


def gelu_slope(pre_act):
    tanh_val = jnp.tanh(GELU_SCALE * (pre_act + GELU_COEF * pre_act * pre_act * pre_act))
    return 0.5 * (1.0 + tanh_val) + 0.5 * pre_act * (1.0 - tanh_val * tanh_val) * GELU_SCALE * (1.0 + 3.0 * GELU_COEF * pre_act * pre_act)


def layer_norm_hat(rows_f32):
    centered = rows_f32 - jnp.mean(rows_f32, **ROWS)
    inv_std = lax.rsqrt(jnp.mean(centered * centered, **ROWS) + LN_EPS)
    return centered * inv_std, inv_std


LN_ROWS = 32
TILE = 1280
VMEM = pl.BlockSpec(memory_space=pltpu.VMEM)
HBM = pl.BlockSpec(memory_space=pl.ANY)
DMA = pltpu.SemaphoreType.DMA
COMM = DMA((14,))
PAIR = DMA((2,))
shape = jax.ShapeDtypeStruct


def tile_at(i, size):
    return pl.ds(pl.multiple_of(i * size, size), size)


def start_all(copies):
    for copy in copies:
        copy.start()
    return copies


def wait_all(copies):
    for copy in copies:
        copy.wait()


def start_copies(sem, *pairs):
    return start_all([pltpu.make_async_copy(src, dst, sem.at[i]) for i, (src, dst) in enumerate(pairs)])


def loop(count, body, start=0):
    def step(i, carry):
        body(i)
        return carry

    lax.fori_loop(start, count, step, 0)


def comm_call(kernel, name, ident, flops, args, in_specs, out_shape, out_specs, scratch, aliases={}):
    return pl.pallas_call(
        kernel, in_specs=in_specs, out_specs=out_specs, out_shape=out_shape, scratch_shapes=scratch, name=name,
        input_output_aliases=aliases,
        compiler_params=pltpu.CompilerParams(collective_id=ident, has_side_effects=True, vmem_limit_bytes=66_000_000),
        cost_estimate=pl.CostEstimate(flops=flops, bytes_accessed=flops // 1000, transcendentals=flops // 1000),
    )(*args)


class Tiles:
    def __init__(self, buf, out, sem, rows=False):
        self.buf, self.out, self.sem, self.rows = buf, out, sem, rows

    def copy(self, n):
        size = self.buf.shape[1 if self.rows else 2]
        at = tile_at(n, size)
        dst = self.out.at[at] if self.rows else self.out.at[:, at]
        return pltpu.make_async_copy(self.buf.at[n % 2], dst, self.sem.at[n % 2])

    def put(self, n, value):
        @pl.when(n >= 2)
        def _():
            self.copy(n - 2).wait()

        self.buf[n % 2] = value()
        self.copy(n).start()

    def finish(self, count):
        self.copy(count - 2).wait()
        self.copy(count - 1).wait()


OUT_TILE = 512


def flat_cols(ref, cols):
    return ref[:, :, cols].reshape(ref.shape[DIM0] * ref.shape[DIM1], OUT_TILE)


def fwd_kernel(dout_ref, q_hbm, k_hbm, v_hbm, x_hbm, mid_hbm, gain1_ref, bias1_ref, gain2_ref, bias2_ref,
               dfull, ctx_ref, wide_ref, max_ref, inv_ref, h1_ref, h2_ref,
               k_rows, strip, q_ref, k_ref, v_ref, x_ref, mid_ref, own_sem, load_sem, *comm_sems):
    place = Place()
    place.barrier()
    gather = Gather(place, dout_ref, dfull, *comm_sems)
    gather.start()
    loads = start_copies(load_sem, (x_hbm, x_ref), (mid_hbm, mid_ref), (k_hbm, k_ref), (q_hbm, q_ref), (v_hbm, v_ref))
    own_copy = pltpu.make_async_copy(dout_ref, dfull.at[place.me], own_sem)
    own_copy.start()
    heads, dim, seq = q_ref.shape
    exp_scale = dim ** -0.5 * LOG2E
    loads[0].wait()
    loads[1].wait()
    affine = [ref[...].reshape(1, ref.shape[DIM0]) for ref in (gain1_ref, bias1_ref, gain2_ref, bias2_ref)]

    def norm_rows(i):
        at = tile_at(i, LN_ROWS)
        for row, (src, dst) in enumerate(((x_ref, h1_ref), (mid_ref, h2_ref))):
            x_hat, _ = layer_norm_hat(src[at, :].astype(F32))
            dst[at, :] = (x_hat * affine[2 * row] + affine[2 * row + 1]).astype(BF16)

    loop(x_ref.shape[DIM0] // LN_ROWS, norm_rows)
    for copy in loads[2:]:
        copy.wait()

    def head(h):
        k_rows[...] = k_ref[h].T

        def query_block(qi):
            q_at = tile_at(qi, BLK)
            q_blk = q_ref[h, :, q_at]

            def score_step(ki, run_max):
                at = tile_at(ki, BLK)
                blk = dot(k_rows[at, :], q_blk)
                strip[at, :] = blk
                return jnp.maximum(run_max, jnp.max(blk, **COLS))

            diag = causal_fill(dot(k_rows[q_at, :], q_blk), -1e30)
            strip[q_at, :] = diag
            row_max = lax.fori_loop(0, qi, score_step, jnp.max(diag, **COLS))

            def exp_step(ki, run_sum):
                at = tile_at(ki, BLK)
                probs = jnp.exp2((strip[at, :] - row_max) * exp_scale)
                strip[at, :] = probs
                return run_sum + jnp.sum(probs, **COLS)

            row_inv = 1.0 / lax.fori_loop(0, qi + 1, exp_step, jnp.zeros_like(row_max))

            def ctx_step(ki, carry):
                high, low = carry
                at = tile_at(ki, BLK)
                probs = strip[at, :] * row_inv
                probs_low = probs.astype(BF16)
                rest = (probs - probs_low.astype(F32)).astype(BF16)
                v_blk = v_ref[h, :, at]
                return high + dot(v_blk, probs_low), low + dot(v_blk, rest)

            zero = jnp.zeros((dim, BLK), F32)
            high, low = lax.fori_loop(0, qi + 1, ctx_step, (zero, zero))
            ctx_ref[h, :, q_at] = high.astype(BF16)
            wide_ref[h, :, q_at] = high + low
            max_ref[h, :, q_at] = row_max
            inv_ref[h, :, q_at] = row_inv

        loop(seq // BLK, query_block)

    def head_step(h):
        head(h)

        @pl.when(h == 1)
        def _():
            gather.relay()

        @pl.when(h == 2)
        def _():
            gather.forward('X')
            gather.forward('Y')

    loop(heads, head_step)
    gather.forward('D')
    gather.links.wait('CO', 'CX', 'CY', 'CD')
    own_copy.wait()
    gather.links.finish()


def fwd_call(d_out, q_t, k_t, v_t, x_in, x_mid, affine):
    heads, dim, seq = q_t.shape
    rows, model = d_out.shape
    return comm_call(
        fwd_kernel, "attn_fwd", 0, 40_000_000_000, (d_out, q_t, k_t, v_t, x_in, x_mid, *affine),
        [VMEM] + [HBM] * 5 + [VMEM] * 4,
        [shape((seq // rows, rows, model), BF16), shape((heads, dim, seq), BF16), shape((heads, dim, seq), F32),
         shape((heads, 1, seq), F32), shape((heads, 1, seq), F32), shape((rows, model), BF16), shape((rows, model), BF16)],
        [HBM] + [VMEM] * 6,
        [pltpu.VMEM((seq, dim), BF16), pltpu.VMEM((seq, BLK), F32)] + [pltpu.VMEM(q_t.shape, BF16)] * 3
        + [pltpu.VMEM((rows, model), BF16)] * 2 + [DMA(()), DMA((5,))] + [COMM] * 2)


def dot_t(a, b):
    return lax.dot_general(a, b, (((1,), (1,)), ((), ())), preferred_element_type=F32)


def mlp_kernel(dfull, dout_hbm, mid_hbm, gain_ref, h2_ref, z_ref, w2_ref, w1_ref,
               dx1_ref, dz_ref, gb1_ref, vec_ref, h2full,
               w2v, w1v, dzv, ybuf, part, crecv, diag_recv, last_recv, dout_ref, mid_ref,
               load_sem, y_sem, z_sem, dz_sem, own_sem, *comm_sems):
    place = Place()
    place.barrier()
    rows, model = dout_hbm.shape
    hidden = w2v.shape[DIM0]
    scatter = Scatter(place, part, crecv, diag_recv, last_recv, *comm_sems[0:2])
    gather = ThirdGather(place, h2full, *comm_sems[2:4])
    gather.start('near', h2_ref)
    own_copy = pltpu.make_async_copy(h2_ref, h2full.at[place.me], own_sem)

    half = rows // 2

    def chunk_copies(i, copy):
        return [copy(c, *place.chunk(i, c)) for c in range(4)]

    def load_pair(i):
        return chunk_copies(i, lambda c, slot, at: pltpu.make_async_copy(
            dfull.at[slot, tile_at(at, half)], ybuf.at[i % 2, c], y_sem.at[i, c]))

    def load_pre(i):
        return chunk_copies(i, lambda c, slot, at: pltpu.make_async_copy(
            z_ref.at[tile_at(2 * slot + at, half)], dzv.at[i, c], z_sem.at[i, c]))

    def store_grad(i):
        return chunk_copies(i, lambda c, slot, at: pltpu.make_async_copy(
            dzv.at[i, c], dz_ref.at[tile_at(2 * slot + at, half)], dz_sem.at[i, c]))

    start_all(load_pair(0) + load_pre(0))
    loads = start_copies(load_sem, (w2_ref, w2v), (w1_ref, w1v), (dout_hbm, dout_ref), (mid_hbm, mid_ref))
    for i in range(1, 4):
        start_all(load_pre(i))
    start_all(load_pair(1))
    own_copy.start()
    gb1_ref[...] = jnp.zeros_like(gb1_ref)
    vec_ref[...] = jnp.zeros_like(vec_ref)
    loads[0].wait()

    def pair_step(i):
        wait_all(load_pair(i) + load_pre(i))

        def grad_act(n):
            cols = tile_at(n, TILE)
            acc = dot_t(ybuf[i % 2].reshape(2 * rows, model), w2v[cols, :])
            grad = (acc * gelu_slope(dzv[i, :, :, cols].reshape(2 * rows, TILE).astype(F32))).astype(BF16)
            dzv[i, :, :, cols] = grad.reshape(4, half, TILE)
            gb1_ref[:, cols] += jnp.sum(grad.astype(F32), **COLS)

        loop(hidden // TILE, grad_act)
        start_all(store_grad(i))

        @pl.when(i < 2)
        def _():
            start_all(load_pair(i + 2))

        @pl.when(i == 0)
        def _():
            loads[1].wait()

        @pl.when(i == 2)
        def _():
            gather.forward('near')

        scatter.between(i)

        @pl.when(i == 3)
        def _():
            scatter.add_diag()

        def grad_norm(n):
            cols = tile_at(n, TILE)
            scatter.store(i, cols, dot_t(dzv[i].reshape(2 * rows, hidden), w1v[cols, :]).astype(BF16))

        loop(model // TILE, grad_norm)
        scatter.after(i)

    loop(4, pair_step)

    gain = gain_ref[...].reshape(1, model)
    loads[2].wait()
    loads[3].wait()

    def norm_rows(at):
        grad = scatter.total(at)
        x_hat, inv_std = layer_norm_hat(mid_ref[at, :].astype(F32))
        dout_rows = dout_ref[at, :].astype(F32)
        mid = (dout_rows + layer_norm_bwd(grad, x_hat, inv_std, gain)).astype(BF16)
        dx1_ref[at, :] = mid
        for row, val in enumerate((grad * x_hat, grad, mid.astype(F32), dout_rows)):
            vec_ref[row + 2:row + 3, :] += jnp.sum(val, **COLS)

    scatter.norm_loop(norm_rows)
    for i in range(4):
        wait_all(store_grad(i))
    own_copy.wait()
    gather.wait_pair('near')
    gather.links.finish()
    scatter.links.finish()


def scatter_scratch(rows, model):
    return [pltpu.VMEM((8, rows, model), BF16), pltpu.VMEM((4, rows, model), BF16),
            pltpu.VMEM((2, rows // 2, model), BF16), pltpu.VMEM((2, rows, model), BF16)]


def mlp_call(dfull, d_out, x_mid, gain, h1, z_saved, w2, w1):
    rows, model = d_out.shape
    seq, hidden = z_saved.shape
    return comm_call(
        mlp_kernel, "mlp_grads", 1, 60_000_000_000, (dfull, d_out, x_mid, gain, h1, z_saved, w2, w1),
        [HBM] * 3 + [VMEM] + [HBM] * 4,
        [shape((rows, model), BF16), shape((seq, hidden), BF16), shape((1, hidden), F32), shape((8, model), F32),
         shape(dfull.shape, BF16)],
        [VMEM, HBM, VMEM, VMEM, HBM],
        [pltpu.VMEM((hidden, model), BF16), pltpu.VMEM((model, hidden), BF16),
         pltpu.VMEM((4, 4, rows // 2, hidden), BF16), pltpu.VMEM((2, 4, rows // 2, model), BF16)]
        + scatter_scratch(rows, model) + [pltpu.VMEM((rows, model), BF16)] * 2
        + [DMA((4,))] + [DMA((4, 4))] * 3 + [DMA(())] + [COMM] * 4)


def gelu(pre_act):
    return 0.5 * pre_act * (1.0 + jnp.tanh(GELU_SCALE * (pre_act + GELU_COEF * pre_act * pre_act * pre_act)))


def ctx_kernel(dx1_ref, wo_ref, z_ref, dfull, mfull, do_ref, dw2_ref,
               mbuf, zv, ut, yv, obuf, own_sem, m_sem, load_sem, out_sem, *comm_sems):
    place = Place()
    place.barrier()
    rows, model = dx1_ref.shape
    gather = Gather(place, dx1_ref, mfull, *comm_sems)
    gather.start()
    own_copy = pltpu.make_async_copy(dx1_ref, mfull.at[place.me], own_sem)
    own_copy.start()

    loads = [pltpu.make_async_copy(z_ref, zv, load_sem.at[0]), pltpu.make_async_copy(dfull, yv, load_sem.at[1])]
    for copy in loads:
        copy.start()
    tiles = Tiles(obuf, dw2_ref, out_sem)
    count = model // OUT_TILE

    def turn(n):
        cols = tile_at(n, 256)
        ut[cols, :] = gelu(zv[:, cols].astype(F32)).astype(BF16).T

    def weight_tile(n):
        cols = tile_at(n, OUT_TILE)
        tiles.put(n, lambda: dot(ut[...], flat_cols(yv, cols)))

    loads[0].wait()
    loop(ut.shape[DIM0] // 256, turn)
    gather.relay()
    loads[1].wait()
    loop(count, weight_tile)
    gather.forward('X')
    gather.forward('Y')
    own_copy.wait()
    gather.links.wait('CO')

    def grad_ctx(i):
        @pl.when(i == 1)
        def _():
            gather.links.wait('CY')

        @pl.when(i == 2)
        def _():
            gather.links.wait('CX')

        @pl.when(i == 3)
        def _():
            gather.forward('D')
            gather.links.wait('CD')

        pair = place.pair_at(3 - i)
        copy = pltpu.make_async_copy(mfull.at[pl.ds(2 * pair, 2)], mbuf, m_sem)
        copy.start()
        copy.wait()
        do_ref[:, tile_at(pair, 2 * rows)] = dot_t(wo_ref[...], mbuf[...].reshape(2 * rows, model)).astype(BF16)

    loop(4, grad_ctx)
    tiles.finish(count)
    gather.links.finish()


def ctx_call(dx1, w_rows, z_saved, dfull):
    rows, model = dx1.shape
    feats = w_rows.shape[DIM0]
    seq, hidden = z_saved.shape
    return comm_call(
        ctx_kernel, "ctx_grads", 2, 30_000_000_000, (dx1, w_rows, z_saved, dfull), [VMEM] * 2 + [HBM] * 2,
        [shape((seq // rows, rows, model), BF16), shape((feats, seq), BF16), shape((hidden, model), F32)], [HBM, VMEM, HBM],
        [pltpu.VMEM((2, rows, model), BF16), pltpu.VMEM((seq, hidden), BF16), pltpu.VMEM((hidden, seq), BF16),
         pltpu.VMEM((seq // rows, rows, model), BF16), pltpu.VMEM((2, hidden, OUT_TILE), F32),
         DMA(()), DMA(()), PAIR, PAIR] + [COMM] * 2)


def bwd_kernel(h1_ref, q_hbm, k_hbm, v_hbm, do_hbm, wide_hbm, max_ref, inv_ref, dz_ref, h2_in,
               h2full, h1full, out_ref, dw1_ref,
               k_rows, v_rows, q_rows, do_rows, delta, dq_acc, dk_acc, dv_acc, tok, dzv, wbuf,
               q_ref, k_ref, v_ref, do_ref, wide_ref, own_sem, head_sem, load_sem, out_sem, *comm_sems):
    place = Place()
    place.barrier()
    gather1 = ThirdGather(place, h1full, *comm_sems[0:2])
    gather2 = ThirdGather(place, h2full, *comm_sems[2:4])
    gather2.start('rest', None)
    gather2.start('diag', None)
    gather1.start('near', h1_ref)
    gather1.start('rest', h1_ref)
    loads = start_copies(head_sem, (k_hbm, k_ref), (v_hbm, v_ref), (q_hbm, q_ref), (do_hbm, do_ref), (wide_hbm, wide_ref))
    own_copy = pltpu.make_async_copy(h1_ref, h1full.at[place.me], own_sem)
    own_copy.start()
    heads, dim, seq = q_ref.shape
    blocks = seq // BLK
    scale = dim ** -0.5
    exp_scale = scale * LOG2E

    def head(h):
        k_rows[...] = k_ref[h].T
        v_rows[...] = v_ref[h].T
        q_rows[...] = q_ref[h].T
        do_rows[...] = do_ref[h].T
        delta[...] = jnp.sum(do_ref[h].astype(F32) * wide_ref[h], **COLS)
        dq_acc[...] = jnp.zeros_like(dq_acc)
        dk_acc[...] = jnp.zeros_like(dk_acc)
        dv_acc[...] = jnp.zeros_like(dv_acc)

        def block(qi, ki, on_diag):
            q_at, k_at = tile_at(qi, BLK), tile_at(ki, BLK)
            scores = dot(k_rows[k_at, :], q_ref[h, :, q_at])
            if on_diag:
                scores = causal_fill(scores, -1e30)
            probs = jnp.exp2((scores - max_ref[h, :, q_at]) * exp_scale) * inv_ref[h, :, q_at]
            grad_probs = dot(v_rows[k_at, :], do_ref[h, :, q_at])
            dv_acc[k_at, :] += dot(probs.astype(BF16), do_rows[q_at, :])
            grad_scores = (probs * (grad_probs - delta[:, q_at]) * scale).astype(BF16)
            dk_acc[k_at, :] += dot(grad_scores, q_rows[q_at, :])
            dq_acc[:, q_at] += dot(k_ref[h, :, k_at], grad_scores)

        loop(blocks, lambda i: block(i, i, True))
        loop(blocks, lambda ki: loop(blocks, lambda qi: block(qi, ki, False), ki + 1))
        out_ref[0, h] = dq_acc[...].astype(BF16)
        out_ref[1, h] = dk_acc[...].astype(BF16).T
        out_ref[2, h] = dv_acc[...].astype(BF16).T

    load_grad, load_tok = [pltpu.make_async_copy(src, dst, load_sem.at[i])
                           for i, (src, dst) in enumerate(((dz_ref, dzv), (h2full, tok)))]
    for copy in loads:
        copy.wait()
    count = tok.shape[DIM2] // OUT_TILE
    tiles = Tiles(wbuf, dw1_ref, out_sem, rows=True)

    def fc1_tile(n):
        cols = tile_at(n, OUT_TILE)
        tiles.put(n, lambda: dot(flat_cols(tok, cols).T, dzv[...]))

    def head_step(h):
        head(h)

        @pl.when(h == 1)
        def _():
            load_grad.start()
            gather2.forward('rest')

        @pl.when(h == heads - 2)
        def _():
            gather2.forward('diag')
            gather2.wait_pair('rest')

    loop(heads - 1, head_step)
    gather2.wait_pair('diag')
    load_tok.start()
    head(heads - 1)
    load_grad.wait()
    load_tok.wait()
    loop(count, fc1_tile)
    for third in ('near', 'rest'):
        gather1.forward(third)
    for third in ('near', 'rest'):
        gather1.wait_pair(third)
    own_copy.wait()
    tiles.finish(count)
    gather1.links.finish()
    gather2.links.finish()


def bwd_call(h1, q_t, k_t, v_t, do_t, wide, row_max, row_inv, dz, h2full):
    heads, dim, seq = q_t.shape
    rows, model = h1.shape
    full = shape((seq // rows, rows, model), BF16)
    turned = pltpu.VMEM((seq, dim), BF16)
    hidden = dz.shape[DIM1]
    return comm_call(
        bwd_kernel, "attn_bwd", 3, 80_000_000_000,
        (h1, q_t, k_t, v_t, do_t, wide, row_max, row_inv, dz, h2full), [VMEM] + [HBM] * 5 + [VMEM] * 2 + [HBM] * 2,
        [full, full, shape((3, heads, dim, seq), BF16), shape((model, hidden), F32)], [HBM, HBM, VMEM, HBM],
        [turned] * 4 + [pltpu.VMEM((1, seq), F32), pltpu.VMEM((dim, seq), F32), pltpu.VMEM((seq, dim), F32),
                        pltpu.VMEM((seq, dim), F32), pltpu.VMEM((seq // rows, rows, model), BF16),
                        pltpu.VMEM((seq, hidden), BF16), pltpu.VMEM((2, OUT_TILE, hidden), F32),
                        *[pltpu.VMEM(q_t.shape, BF16)] * 4, pltpu.VMEM(wide.shape, F32),
                        DMA(()), DMA((5,)), PAIR, PAIR] + [COMM] * 4,
        aliases={9: 0})


def qkv_kernel(qkv_hbm, w_hbm, dx1_hbm, x_hbm, gain_ref, vec_ref, ctx_hbm, mfull, h1_in,
               dx_ref, vsum_ref, bias_ref, dwo_ref, dw_ref, h1full,
               turned, part, crecv, diag_recv, last_recv, vacc, vsend, vrecv, last_got, tok, obuf, wbuf,
               qkv_ref, w_ref, dx1_ref, x_ref, ctx_ref, vsem, last_sem, load_sem, in_sem, out_sem, *comm_sems):
    place = Place()
    place.barrier(everyone=True)
    rows, model = dx1_ref.shape
    scatter = Scatter(place, part, crecv, diag_recv, last_recv, *comm_sems[0:2])
    gather = ThirdGather(place, h1full, *comm_sems[2:4])
    gather.start('diag', None)
    inputs = start_copies(in_sem, (qkv_hbm, qkv_ref), (w_hbm, w_ref), (ctx_hbm, ctx_ref), (dx1_hbm, dx1_ref), (x_hbm, x_ref))
    loads = [pltpu.make_async_copy(src, tok, load_sem.at[i]) for i, src in enumerate((mfull, h1full))]
    tiles_o = Tiles(obuf, dwo_ref, out_sem.at[0])
    tiles = Tiles(wbuf, dw_ref, out_sem.at[1])
    count = model // OUT_TILE
    swaps = Links(place, vsem.at[0], vsem.at[1])
    inputs[0].wait()

    def vec_step(i):
        if i > 0:
            swaps.wait('CXY'[i - 1])
            vacc[...] += vrecv[i - 1]
        if i < 3:
            vsend[i] = vacc[...]

    def vec_send(i):
        swaps.send('CXY'[i], 'CXY'[i], vsend, vrecv, i)

    vacc[...] = vec_ref[...]
    vec_step(0)
    vec_send(0)

    def pair_step(i):
        for c in range(4):
            slot, at = place.chunk(i, c)
            turned[tile_at(c, rows // 2), :] = qkv_ref[:, tile_at(2 * slot + at, rows // 2)].T

        @pl.when(i == 0)
        def _():
            inputs[1].wait()

        @pl.when(i == 1)
        def _():
            loads[0].start()

        @pl.when(i == 3)
        def _():
            gather.forward('diag')

        for at in range(1, 3):
            @pl.when(i == at)
            def _():
                vec_step(at)
                vec_send(at)

        scatter.between(i)

        def grad_norm(n):
            cols = tile_at(n, TILE)
            scatter.store(i, cols, dot(turned[...], w_ref[:, cols]).astype(BF16))

        loop(model // TILE, grad_norm)
        scatter.after(i)

    loop(4, pair_step)
    loads[0].wait()
    for copy in inputs[2:]:
        copy.wait()

    def proj_tile(n):
        cols = tile_at(n, OUT_TILE)
        tiles_o.put(n, lambda: dot(ctx_ref[...], flat_cols(tok, cols)))

    def qkv_tile(n):
        cols = tile_at(n, OUT_TILE)
        tiles.put(n, lambda: dot(qkv_ref[...], flat_cols(tok, cols)))

    loop(count, proj_tile)
    scatter.add_diag()
    gather.wait_pair('diag')
    loads[1].start()
    ones = jnp.ones((8, qkv_ref.shape[DIM1]), BF16)
    kinds, heads, dim = bias_ref.shape
    for row in range(kinds * heads):
        feats = qkv_ref[row * dim:(row + 1) * dim, :]
        bias_ref[row // heads, row % heads, :] = dot_t(ones, feats)[0]
    loads[1].wait()
    loop(count, qkv_tile)
    vec_step(3)
    tiles_o.finish(count)
    gain = gain_ref[...].reshape(1, model)

    def norm_rows(at):
        grad = scatter.total(at)
        x_hat, inv_std = layer_norm_hat(x_ref[at, :].astype(F32))
        dx_ref[at, :] = (dx1_ref[at, :].astype(F32) + layer_norm_bwd(grad, x_hat, inv_std, gain)).astype(BF16)
        vacc[0:1, :] += jnp.sum(grad * x_hat, **COLS)
        vacc[1:2, :] += jnp.sum(grad, **COLS)

    scatter.norm_loop(norm_rows)
    finals = Links(place, last_sem.at[0], last_sem.at[1])
    last_got[0] = vacc[0:2, :]
    vsum_ref[2:6, :] = vacc[2:6, :]
    for k in range(1, 8):
        finals.send(k, k, (last_got, (0,)), (last_got, (k,)))
    tiles.finish(count)
    finals.wait(*range(1, 8))
    total = last_got[place.me]
    for source in range(1, 8):
        total += last_got[(place.me + 8 - source) % 8]
    vsum_ref[0:2, :] = total
    for links in (swaps, finals, scatter.links, gather.links):
        links.finish()


def qkv_call(heads, qkv_rows, w_rows, dx1, x_in, gain, vec, ctx_rows, mfull, h1full):
    rows, model = dx1.shape
    feats, seq = qkv_rows.shape
    proj = ctx_rows.shape[DIM0]
    return comm_call(
        qkv_kernel, "qkv_grads", 4, 30_000_000_000,
        (qkv_rows, w_rows, dx1, x_in, gain, vec, ctx_rows, mfull, h1full), [HBM] * 4 + [VMEM] * 2 + [HBM] * 3,
        [shape((rows, model), BF16), shape((6, model), F32), shape((3, heads, feats // (3 * heads)), F32), shape((proj, model), F32),
         shape((feats, model), F32), shape(h1full.shape, BF16)],
        [VMEM] * 3 + [HBM] * 3,
        [pltpu.VMEM((2 * rows, feats), BF16)] + scatter_scratch(rows, model)
        + [pltpu.VMEM((8, model), F32), pltpu.VMEM((3, 8, model), F32), pltpu.VMEM((3, 8, model), F32),
           pltpu.VMEM((8, 2, model), F32), pltpu.VMEM((8, rows, model), BF16),
           pltpu.VMEM((2, proj, OUT_TILE), F32), pltpu.VMEM((2, feats, OUT_TILE), F32),
           pltpu.VMEM((feats, seq), BF16), pltpu.VMEM((feats, model), BF16), pltpu.VMEM((rows, model), BF16),
           pltpu.VMEM((rows, model), BF16), pltpu.VMEM((proj, seq), BF16),
           DMA((2, 3)), DMA((2, 7)), PAIR, DMA((5,)), DMA((2, 2))] + [COMM] * 4,
        aliases={8: 5})


def finish_kernel(*refs):
    count = len(refs) // 3
    refs[2 * count - 1][...] = refs[count - 1][...].reshape(refs[2 * count - 1].shape)
    rings, single, (small_sem, in_sem, out_sem) = refs[2 * count:2 * count + 2], refs[2 * count + 2:-3], refs[-3:]
    chunks, used = [], [0, 0]
    small = [(src, buf, dst) for src, buf, dst in zip(refs[4:count - 1], single, refs[count + 4:2 * count - 1])]
    for i, (src, buf, _) in enumerate(small):
        pltpu.make_async_copy(src, buf, small_sem.at[0, i]).start()
    for src, dst in zip(refs[:4], refs[count:count + 4]):
        kind = 0 if src.shape[DIM1] == rings[0].shape[DIM2] else 1
        rows = rings[kind].shape[DIM1]
        for row in range(0, src.shape[DIM0], rows):
            chunks.append((src.at[pl.ds(row, rows)], dst.at[pl.ds(row, rows)], kind, used[kind]))
            used[kind] += 1

    def copy_in(src, dst, kind, at):
        slot = at % RING
        return pltpu.make_async_copy(src, rings[kind].at[slot], in_sem.at[kind, slot])

    def copy_out(src, dst, kind, at):
        slot = at % RING
        return pltpu.make_async_copy(rings[kind].at[slot], dst, out_sem.at[kind, slot])

    waiting = {}

    def start(chunk):
        key = (chunk[2], chunk[3] % RING)
        if key in waiting:
            copy_out(*waiting.pop(key)).wait()
        copy_in(*chunk).start()

    for chunk in chunks[:AHEAD]:
        start(chunk)
    for i, (src, buf, dst) in enumerate(small):
        pltpu.make_async_copy(src, buf, small_sem.at[0, i]).wait()
        pltpu.make_async_copy(buf, dst, small_sem.at[1, i]).start()
    for i, chunk in enumerate(chunks):
        copy_in(*chunk).wait()
        copy_out(*chunk).start()
        waiting[(chunk[2], chunk[3] % RING)] = chunk
        if i + AHEAD < len(chunks):
            start(chunks[i + AHEAD])
    for chunk in waiting.values():
        copy_out(*chunk).wait()
    for i, (_, buf, dst) in enumerate(small):
        pltpu.make_async_copy(buf, dst, small_sem.at[1, i]).wait()


RING = 8
AHEAD = 12


def finish_call(*arrays):
    wide = max(a.shape[DIM1] for a in arrays[:4])
    narrow = min(a.shape[DIM1] for a in arrays[:4])
    small = [pltpu.VMEM(a.shape, a.dtype) for a in arrays[4:-1]]
    return pl.pallas_call(
        finish_kernel, name="finish", in_specs=[HBM] * (len(arrays) - 1) + [VMEM], out_specs=[HBM] * (len(arrays) - 1) + [VMEM],
        out_shape=[shape(a.shape, a.dtype) for a in arrays[:-1]] + [shape(arrays[-1].shape[1:], F32)],
        scratch_shapes=[pltpu.VMEM((RING, 320, wide), F32), pltpu.VMEM((RING, 640, narrow), F32), *small,
                        DMA((2, len(small))), DMA((2, RING)), DMA((2, RING))],
        compiler_params=pltpu.CompilerParams(vmem_limit_bytes=66_000_000),
        cost_estimate=pl.CostEstimate(flops=1_000_000, bytes_accessed=72_000_000, transcendentals=0),
    )(*arrays)


def solution(mesh):
    def local_backward(x_in, x_mid, d_out, q_saved, k_saved, v_saved, z_saved, ln1_gain, ln1_bias, ln2_gain, ln2_bias, w_qkv, w_proj, w_fc1, w_fc2):
        x_in, x_mid, d_out, z_saved = x_in[0], x_mid[0], d_out[0], z_saved[0]
        heads, dim = q_saved.shape[2:]
        seq, model = z_saved.shape[DIM0], x_in.shape[DIM1]
        q_t, k_t, v_t = (v[0].transpose(1, 2, 0) for v in (q_saved, k_saved, v_saved))
        affine = (ln1_gain, ln1_bias, ln2_gain, ln2_bias)
        dfull, ctx_t, wide_t, row_max, row_inv, h1_local, h2_local = fwd_call(d_out, q_t, k_t, v_t, x_in, x_mid, affine)
        dx1, grad_pre, grad_bfc1, vec, h2_full = mlp_call(dfull, d_out, x_mid, ln2_gain, h2_local, z_saved, w_fc2, w_fc1)
        mfull, do_t, grad_wfc2 = ctx_call(dx1, w_proj.reshape(heads * dim, model), z_saved, dfull)
        _, h1_full, qkv_t, grad_wfc1 = bwd_call(
            h1_local, q_t, k_t, v_t, do_t.reshape(heads, dim, seq), wide_t, row_max, row_inv, grad_pre, h2_full)
        qkv_rows = qkv_t.reshape(3 * heads * dim, seq)
        w_rows = w_qkv.transpose(0, 2, 3, 1).reshape(3 * heads * dim, model)
        grad_x, grad_vecs, grad_bqkv, grad_wproj, grad_wqkv, _ = qkv_call(
            heads, qkv_rows, w_rows, dx1, x_in, ln1_gain, vec, ctx_t.reshape(heads * dim, seq), mfull, h1_full)
        grad_wfc2, grad_wfc1, grad_wqkv, grad_wproj, grad_x, grad_vecs, grad_bqkv, grad_bfc1 = finish_call(
            grad_wfc2, grad_wfc1, grad_wqkv, grad_wproj, grad_x, grad_vecs, grad_bqkv, grad_bfc1)
        grad_wproj = grad_wproj.reshape(heads, dim, model)
        grad_wqkv = grad_wqkv.reshape(3, heads, dim, model).transpose(0, 3, 1, 2)
        return grad_x[None], grad_wqkv, grad_bqkv, grad_wproj, grad_wfc1, grad_bfc1, grad_wfc2, grad_vecs

    tok_spec = P('dp', 'tp', None)
    head_spec = P('dp', None, 'tp', None)
    in_specs = (tok_spec, tok_spec, tok_spec, head_spec, head_spec, head_spec, P('dp', None, 'tp'),
                P(None), P(None), P(None), P(None),
                P(None, None, 'tp', None), P('tp', None, None), P(None, 'tp'), P('tp', None))
    out_specs = (tok_spec, P('dp', None, 'tp', None), P('dp', 'tp', None), P(('dp', 'tp'), None, None),
                 P('dp', 'tp'), P(('dp', 'tp')), P(('dp', 'tp'), None), P('dp', None))
    return jax.shard_map(local_backward, mesh=mesh, in_specs=in_specs, out_specs=out_specs, check_vma=False)
```

```python
import jax
import jax.numpy as jnp
from jax import lax
from jax.experimental import pallas as pl
from jax.experimental.pallas import tpu as pltpu
from jax.sharding import PartitionSpec as P

LN_EPS = 1e-5
GELU_COEF = 0.044715
GELU_SCALE = 0.7978845608028654
LOG2E = 1.4426950408889634
BLK = 512
F32 = jnp.float32
BF16 = jnp.bfloat16
DIM0, DIM1, DIM2 = range(3)
COLS = dict(axis=0, keepdims=True)
ROWS = dict(axis=-1, keepdims=True)


def layer_norm_bwd(grad_norm, x_hat, inv_std, norm_gain):
    grad_hat = grad_norm * norm_gain
    centered_grad = grad_hat - jnp.mean(grad_hat, **ROWS)
    return inv_std * (centered_grad - x_hat * jnp.mean(grad_hat * x_hat, **ROWS))


def dot(a, b):
    return jnp.dot(a, b, preferred_element_type=F32)


def causal_fill(scores, fill):
    key_ids = lax.broadcasted_iota(jnp.int32, scores.shape, 0)
    query_ids = lax.broadcasted_iota(jnp.int32, scores.shape, 1)
    return jnp.where(query_ids >= key_ids, scores, fill)


class Place:
    def __init__(self):
        self.group = lax.axis_index('dp')
        self.me = lax.axis_index('tp')
        self.core = self.me % 2
        self.dx = 2 - 4 * ((self.me // 2) % 2)
        self.dy = 4 - 8 * (self.me // 4)
        self.dc = 1 - 2 * self.core
        self.peer = {'X': self.me + self.dx, 'Y': self.me + self.dy, 'C': self.me + self.dc}
        self.peer.update({k: (self.me + k) % 8 for k in range(1, 8)})
        self.block = {'O': self.me, 'X': self.me + self.dx, 'Y': self.me + self.dy, 'D': self.me + self.dx + self.dy}
        self.pair = {key: val // 2 for key, val in self.block.items()}
        self.other = {key: val + self.dc for key, val in self.block.items()}
        self.x, self.y = (self.me // 2) % 2, self.me // 4

    def pair_at(self, i):
        flip_x, flip_y = 1 - i // 2, 1 - i % 2
        return 2 * (self.y + flip_y * (1 - 2 * self.y)) + self.x + flip_x * (1 - 2 * self.x)

    def chunk(self, i, c):
        mixed = i * (3 - i) // 2
        pair, half = (self.pair['X'], i - 1) if c < 2 else (self.pair['Y'], 2 - i)
        slot = (1 - mixed) * (2 * self.pair_at(i) + c // 2) + mixed * (2 * pair + c % 2)
        return slot, (1 - mixed) * (c % 2) + mixed * half

    def barrier(self, everyone=False):
        sem = pltpu.get_barrier_semaphore()
        keys = range(1, 8) if everyone else 'XYC'
        for key in keys:
            pl.semaphore_signal(sem, inc=1, device_id=(self.group, self.peer[key]), device_id_type=pl.DeviceIdType.MESH)
        pl.semaphore_wait(sem, len(keys))


class Links:
    def __init__(self, place, send_sem, recv_sem):
        self.place, self.send_sem, self.recv_sem = place, send_sem, recv_sem
        self.copies = {}

    def define(self, name, to, src, dst, *index):
        at = len(self.copies)

        def place_of(ref):
            ref, where = ref if isinstance(ref, tuple) else (ref, index)
            return ref.at[where] if where else ref

        def copy():
            return pltpu.make_async_remote_copy(
                src_ref=place_of(src), dst_ref=place_of(dst), send_sem=self.send_sem.at[at], recv_sem=self.recv_sem.at[at],
                device_id=(self.place.group, self.place.peer[to]), device_id_type=pl.DeviceIdType.MESH)

        self.copies[name] = copy

    def start(self, name):
        self.copies[name]().start()

    def send(self, name, *rest):
        self.define(name, *rest)
        self.start(name)

    def wait(self, *names):
        for name in names:
            self.copies[name]().wait_recv()

    def finish(self):
        for copy in self.copies.values():
            copy().wait_send()


class Gather:
    COPIES = 10

    def __init__(self, place, own, full, send_sem, recv_sem):
        self.place, self.own, self.full = place, own, full
        self.links = Links(place, send_sem, recv_sem)
        half = own.shape[DIM0] // 2
        self.first, self.second = pl.ds(0, half), pl.ds(half, half)

    def start(self):
        me, full, own, send = self.place.me, self.full, self.own, self.links.send
        for name, half in (('Xa', self.first), ('Yb', self.second), ('Xb', self.second), ('Ya', self.first)):
            send(name, name[0], (own, (half,)), (full, (me, half)))
        send('CO', 'C', (own, ()), (full, (me,)))

    def relay(self):
        links, full, block = self.links, self.full, self.place.block
        links.wait('Xa')
        links.send('Da', 'Y', full, full, block['X'], self.first)
        links.wait('Yb')
        links.send('Db', 'X', full, full, block['Y'], self.second)

    def forward(self, key):
        first, second = ('Xb', None) if key == 'X' else ('Ya', None) if key == 'Y' else ('Da', 'Db')
        self.links.wait(first)
        if second:
            self.links.wait(second)
        self.links.send('C' + key, 'C', self.full, self.full, self.place.block[key])


class ThirdGather:
    def __init__(self, place, full, send_sem, recv_sem):
        self.place, self.full = place, full
        self.links = Links(place, send_sem, recv_sem)
        half = full.shape[DIM1] // 2
        self.first, self.second = pl.ds(0, half), pl.ds(half, half)

    def start(self, third, own):
        me, full, block = self.place.me, self.full, self.place.block
        near = {'near': {'X': self.first, 'Y': self.second}, 'rest': {'X': self.second, 'Y': self.first}}.get(third)
        for key in 'XY':
            if near is None:
                slot, half = (block['Y'], self.second) if key == 'X' else (block['X'], self.first)
                self.links.send(third + key, key, full, full, slot, half)
            else:
                src = (full, (me, near[key])) if own is None else (own, (near[key],))
                self.links.send(third + key, key, src, (full, (me, near[key])))
        if third == 'near':
            self.links.send('CO', 'C', (own, ()), (full, (me,)))

    def forward(self, third):
        block = self.place.block
        for key in 'XY':
            self.links.wait(third + key)
            half = self.first if (third == 'near') == (key == 'X') else self.second
            slot = block[key]
            if third == 'diag':
                slot, half = block['D'], (self.second if key == 'X' else self.first)
            self.links.send('C' + third + key, 'C', self.full, self.full, slot, half)

    def wait_pair(self, third):
        self.links.wait('C' + third + 'X', 'C' + third + 'Y', *(('CO',) if third == 'near' else ()))


CRECV = dict(O=0, Xa=1, Xb=1, Ya=2, Yb=2, D=3)


class Scatter:
    COPIES = 10

    def __init__(self, place, part, crecv, diag_recv, last_recv, send_sem, recv_sem):
        self.place, self.part, self.crecv = place, part, crecv
        self.diag_recv, self.last_recv = diag_recv, last_recv
        self.links = Links(place, send_sem, recv_sem)
        half = part.shape[DIM1] // 2
        self.half = {'a': pl.ds(0, half), 'b': pl.ds(half, half)}
        for name, at in CRECV.items():
            index = (at,) if len(name) == 1 else (at, self.half[name[1]])
            self.links.define('C' + name, 'C', (part, (place.other[name[0]],) + index[1:]), (crecv, index))

    def add_rows(self, slot, start, count, other, other_start):
        step = 64

        def body(i, carry):
            here = pl.ds(pl.multiple_of(start + i * step, step), step)
            there = pl.ds(pl.multiple_of(other_start + i * step, step), step)
            total = self.part[slot, here, :].astype(F32) + other[there, :].astype(F32)
            self.part[slot, here, :] = total.astype(BF16)
            return carry

        lax.fori_loop(0, count // step, body, 0)

    def store(self, i, cols, rows):
        for c in range(4):
            slot, half = self.place.chunk(i, c)
            size = rows.shape[DIM0] // 4
            self.part[slot, tile_at(half, size), cols] = rows[c * size:(c + 1) * size]

    def swap(self, *names):
        for name in names:
            self.links.start('C' + name)

    def add_pair(self, name):
        self.links.wait('C' + name)
        rows = self.part.shape[DIM1]
        start, count = (0, rows) if len(name) == 1 else ((rows // 2) * 'ab'.index(name[1]), rows // 2)
        self.add_rows(self.place.block[name[0]], start, count, self.crecv.at[CRECV[name]], start)

    def send_half(self, key, half):
        at = self.half[half]
        self.links.send(key + half, key, (self.part, (self.place.block[key], at)), (self.last_recv, ('XY'.index(key), at)))

    def send_diag(self):
        for i, (key, half) in enumerate((('X', 'a'), ('Y', 'b'))):
            self.links.send('D' + half, key, (self.part, (self.place.block['D'], self.half[half])), (self.diag_recv, (i,)))

    def add_diag(self):
        self.add_pair('Xb')
        self.add_pair('Ya')
        rows = self.part.shape[DIM1] // 4
        for i, (half, key, start) in enumerate((('a', 'Y', 0), ('b', 'X', 2 * rows))):
            self.links.wait('D' + half)
            for quarter in range(2):
                off = quarter * rows
                self.add_rows(self.place.block[key], start + off, rows, self.diag_recv.at[i], off)
                at = pl.ds(start + off, rows)
                self.links.send(key + half + str(quarter), key, (self.part, (self.place.block[key], at)),
                                (self.last_recv, ('XY'.index(key), at)))

    def wait_last(self, quarter):
        if quarter == 0:
            self.links.wait('Xa', 'Yb', 'CO')
        self.links.wait('Ya' + str(quarter), 'Xb' + str(quarter))

    def norm_loop(self, body):
        rows = self.part.shape[DIM1]
        chunks = rows // LN_ROWS
        quarter = chunks // 4

        def step(i):
            for part in range(2):
                @pl.when(i == part * (chunks // 2))
                def _():
                    self.wait_last(part)

            part, j = i // (2 * quarter), i % (2 * quarter)
            body(tile_at((j // quarter) * 2 * quarter + part * quarter + j % quarter, LN_ROWS))

        loop(chunks, step)

    def between(self, i):
        @pl.when(i == 1)
        def _():
            self.add_pair('D')
            self.send_diag()

        @pl.when(i == 2)
        def _():
            for name in ('Xa', 'Yb'):
                self.add_pair(name)
                self.send_half(*name)

    def after(self, i):
        for at, names in enumerate((('D',), ('Xa', 'Yb'), ('Xb', 'Ya'), ('O',))):
            @pl.when(i == at)
            def _():
                self.swap(*names)

    def total(self, at):
        me = self.place.me
        return (self.part[me, at, :].astype(F32) + self.crecv[0, at, :].astype(F32)
                + self.last_recv[0, at, :].astype(F32) + self.last_recv[1, at, :].astype(F32))


def gelu_slope(pre_act):
    tanh_val = jnp.tanh(GELU_SCALE * (pre_act + GELU_COEF * pre_act * pre_act * pre_act))
    return 0.5 * (1.0 + tanh_val) + 0.5 * pre_act * (1.0 - tanh_val * tanh_val) * GELU_SCALE * (1.0 + 3.0 * GELU_COEF * pre_act * pre_act)


def layer_norm_hat(rows_f32):
    centered = rows_f32 - jnp.mean(rows_f32, **ROWS)
    inv_std = lax.rsqrt(jnp.mean(centered * centered, **ROWS) + LN_EPS)
    return centered * inv_std, inv_std


LN_ROWS = 32
TILE = 1280
VMEM = pl.BlockSpec(memory_space=pltpu.VMEM)
HBM = pl.BlockSpec(memory_space=pl.ANY)
DMA = pltpu.SemaphoreType.DMA
COMM = DMA((14,))
PAIR = DMA((2,))
shape = jax.ShapeDtypeStruct


def tile_at(i, size):
    return pl.ds(pl.multiple_of(i * size, size), size)


def start_all(copies):
    for copy in copies:
        copy.start()
    return copies


def wait_all(copies):
    for copy in copies:
        copy.wait()


def start_copies(sem, *pairs):
    return start_all([pltpu.make_async_copy(src, dst, sem.at[i]) for i, (src, dst) in enumerate(pairs)])


def loop(count, body, start=0):
    def step(i, carry):
        body(i)
        return carry

    lax.fori_loop(start, count, step, 0)


def comm_call(kernel, name, ident, flops, args, in_specs, out_shape, out_specs, scratch, aliases={}):
    return pl.pallas_call(
        kernel, in_specs=in_specs, out_specs=out_specs, out_shape=out_shape, scratch_shapes=scratch, name=name,
        input_output_aliases=aliases,
        compiler_params=pltpu.CompilerParams(collective_id=ident, has_side_effects=True, vmem_limit_bytes=66_000_000),
        cost_estimate=pl.CostEstimate(flops=flops, bytes_accessed=flops // 1000, transcendentals=flops // 1000),
    )(*args)


class Tiles:
    def __init__(self, buf, out, sem, rows=False):
        self.buf, self.out, self.sem, self.rows = buf, out, sem, rows

    def copy(self, n):
        size = self.buf.shape[1 if self.rows else 2]
        at = tile_at(n, size)
        dst = self.out.at[at] if self.rows else self.out.at[:, at]
        return pltpu.make_async_copy(self.buf.at[n % 2], dst, self.sem.at[n % 2])

    def put(self, n, value):
        @pl.when(n >= 2)
        def _():
            self.copy(n - 2).wait()

        self.buf[n % 2] = value()
        self.copy(n).start()

    def finish(self, count):
        self.copy(count - 2).wait()
        self.copy(count - 1).wait()


OUT_TILE = 512


def flat_cols(ref, cols):
    return ref[:, :, cols].reshape(ref.shape[DIM0] * ref.shape[DIM1], OUT_TILE)


def fwd_kernel(dout_ref, q_hbm, k_hbm, v_hbm, x_hbm, mid_hbm, gain1_ref, bias1_ref, gain2_ref, bias2_ref,
               dfull, ctx_out, wide_out, max_ref, inv_ref, h1_out, h2_out,
               k_rows, strip, q_ref, k_ref, v_ref, ctx_ref, x_ref, mid_ref, h1_ref, h2_ref, wide_ref,
               own_sem, load_sem, *comm_sems):
    place = Place()
    place.barrier()
    gather = Gather(place, dout_ref, dfull, *comm_sems)
    gather.start()
    loads = start_copies(load_sem, (x_hbm, x_ref), (mid_hbm, mid_ref), (k_hbm, k_ref), (q_hbm, q_ref), (v_hbm, v_ref))
    own_copy = pltpu.make_async_copy(dout_ref, dfull.at[place.me], own_sem)
    own_copy.start()
    heads, dim, seq = q_ref.shape
    exp_scale = dim ** -0.5 * LOG2E
    loads[0].wait()
    loads[1].wait()
    affine = [ref[...].reshape(1, ref.shape[DIM0]) for ref in (gain1_ref, bias1_ref, gain2_ref, bias2_ref)]

    def norm_rows(i):
        at = tile_at(i, LN_ROWS)
        for row, (src, dst) in enumerate(((x_ref, h1_ref), (mid_ref, h2_ref))):
            x_hat, _ = layer_norm_hat(src[at, :].astype(F32))
            dst[at, :] = (x_hat * affine[2 * row] + affine[2 * row + 1]).astype(BF16)

    loop(x_ref.shape[DIM0] // LN_ROWS, norm_rows)
    for copy in loads[2:]:
        copy.wait()

    def head(h):
        k_rows[...] = k_ref[h].T

        def query_block(qi):
            q_at = tile_at(qi, BLK)
            q_blk = q_ref[h, :, q_at]

            def score_step(ki, run_max):
                at = tile_at(ki, BLK)
                blk = dot(k_rows[at, :], q_blk)
                strip[at, :] = blk
                return jnp.maximum(run_max, jnp.max(blk, **COLS))

            diag = causal_fill(dot(k_rows[q_at, :], q_blk), -1e30)
            strip[q_at, :] = diag
            row_max = lax.fori_loop(0, qi, score_step, jnp.max(diag, **COLS))

            def exp_step(ki, run_sum):
                at = tile_at(ki, BLK)
                probs = jnp.exp2((strip[at, :] - row_max) * exp_scale)
                strip[at, :] = probs
                return run_sum + jnp.sum(probs, **COLS)

            row_inv = 1.0 / lax.fori_loop(0, qi + 1, exp_step, jnp.zeros_like(row_max))

            def ctx_step(ki, carry):
                high, low = carry
                at = tile_at(ki, BLK)
                probs = strip[at, :] * row_inv
                probs_low = probs.astype(BF16)
                rest = (probs - probs_low.astype(F32)).astype(BF16)
                v_blk = v_ref[h, :, at]
                return high + dot(v_blk, probs_low), low + dot(v_blk, rest)

            zero = jnp.zeros((dim, BLK), F32)
            high, low = lax.fori_loop(0, qi + 1, ctx_step, (zero, zero))
            ctx_ref[h, :, q_at] = high.astype(BF16)
            wide_ref[h, :, q_at] = high + low
            max_ref[h, :, q_at] = row_max
            inv_ref[h, :, q_at] = row_inv

        loop(seq // BLK, query_block)

    def head_step(h):
        head(h)

        @pl.when(h == 1)
        def _():
            gather.relay()

        @pl.when(h == 2)
        def _():
            gather.forward('X')
            gather.forward('Y')

    loop(heads, head_step)
    gather.forward('D')
    results = start_copies(load_sem, (ctx_ref, ctx_out), (wide_ref, wide_out), (h1_ref, h1_out), (h2_ref, h2_out))
    gather.links.wait('CO', 'CX', 'CY', 'CD')
    own_copy.wait()
    wait_all(results)
    gather.links.finish()


def fwd_call(d_out, q_t, k_t, v_t, x_in, x_mid, affine):
    heads, dim, seq = q_t.shape
    rows, model = d_out.shape
    return comm_call(
        fwd_kernel, "attn_fwd", 0, 40_000_000_000, (d_out, q_t, k_t, v_t, x_in, x_mid, *affine),
        [VMEM] + [HBM] * 5 + [VMEM] * 4,
        [shape((seq // rows, rows, model), BF16), shape((heads, dim, seq), BF16), shape((heads, dim, seq), F32),
         shape((heads, 1, seq), F32), shape((heads, 1, seq), F32), shape((rows, model), BF16), shape((rows, model), BF16)],
        [HBM] * 3 + [VMEM] * 2 + [HBM] * 2,
        [pltpu.VMEM((seq, dim), BF16), pltpu.VMEM((seq, BLK), F32)] + [pltpu.VMEM(q_t.shape, BF16)] * 4
        + [pltpu.VMEM((rows, model), BF16)] * 4 + [pltpu.VMEM(q_t.shape, F32)] + [DMA(()), DMA((5,))] + [COMM] * 2)


def dot_t(a, b):
    return lax.dot_general(a, b, (((1,), (1,)), ((), ())), preferred_element_type=F32)


def mlp_kernel(dfull, dout_hbm, mid_hbm, gain_ref, h2_ref, z_ref, w2_ref, w1_ref,
               dx1_ref, dz_ref, gb1_ref, vec_ref, h2full,
               w2v, w1v, dzv, ybuf, part, crecv, diag_recv, last_recv, dout_ref, mid_ref,
               load_sem, y_sem, z_sem, dz_sem, own_sem, *comm_sems):
    place = Place()
    place.barrier()
    rows, model = dout_hbm.shape
    hidden = w2v.shape[DIM0]
    scatter = Scatter(place, part, crecv, diag_recv, last_recv, *comm_sems[0:2])
    gather = ThirdGather(place, h2full, *comm_sems[2:4])
    gather.start('near', h2_ref)
    own_copy = pltpu.make_async_copy(h2_ref, h2full.at[place.me], own_sem)

    half = rows // 2

    def chunk_copies(i, copy):
        return [copy(c, *place.chunk(i, c)) for c in range(4)]

    def load_pair(i):
        return chunk_copies(i, lambda c, slot, at: pltpu.make_async_copy(
            dfull.at[slot, tile_at(at, half)], ybuf.at[i % 2, c], y_sem.at[i, c]))

    def load_pre(i):
        return chunk_copies(i, lambda c, slot, at: pltpu.make_async_copy(
            z_ref.at[tile_at(2 * slot + at, half)], dzv.at[i, c], z_sem.at[i, c]))

    def store_grad(i):
        return chunk_copies(i, lambda c, slot, at: pltpu.make_async_copy(
            dzv.at[i, c], dz_ref.at[tile_at(2 * slot + at, half)], dz_sem.at[i, c]))

    start_all(load_pair(0) + load_pre(0))
    loads = start_copies(load_sem, (w2_ref, w2v), (w1_ref, w1v), (dout_hbm, dout_ref), (mid_hbm, mid_ref))
    for i in range(1, 4):
        start_all(load_pre(i))
    start_all(load_pair(1))
    own_copy.start()
    gb1_ref[...] = jnp.zeros_like(gb1_ref)
    vec_ref[...] = jnp.zeros_like(vec_ref)
    loads[0].wait()

    def pair_step(i):
        wait_all(load_pair(i) + load_pre(i))

        def grad_act(n):
            cols = tile_at(n, TILE)
            acc = dot_t(ybuf[i % 2].reshape(2 * rows, model), w2v[cols, :])
            grad = (acc * gelu_slope(dzv[i, :, :, cols].reshape(2 * rows, TILE).astype(F32))).astype(BF16)
            dzv[i, :, :, cols] = grad.reshape(4, half, TILE)
            gb1_ref[:, cols] += jnp.sum(grad.astype(F32), **COLS)

        loop(hidden // TILE, grad_act)
        start_all(store_grad(i))

        @pl.when(i < 2)
        def _():
            start_all(load_pair(i + 2))

        @pl.when(i == 0)
        def _():
            loads[1].wait()

        @pl.when(i == 2)
        def _():
            gather.forward('near')

        scatter.between(i)

        @pl.when(i == 3)
        def _():
            scatter.add_diag()

        def grad_norm(n):
            cols = tile_at(n, TILE)
            scatter.store(i, cols, dot_t(dzv[i].reshape(2 * rows, hidden), w1v[cols, :]).astype(BF16))

        loop(model // TILE, grad_norm)
        scatter.after(i)

    loop(4, pair_step)

    gain = gain_ref[...].reshape(1, model)
    loads[2].wait()
    loads[3].wait()

    def norm_rows(at):
        grad = scatter.total(at)
        x_hat, inv_std = layer_norm_hat(mid_ref[at, :].astype(F32))
        dout_rows = dout_ref[at, :].astype(F32)
        mid = (dout_rows + layer_norm_bwd(grad, x_hat, inv_std, gain)).astype(BF16)
        dx1_ref[at, :] = mid
        for row, val in enumerate((grad * x_hat, grad, mid.astype(F32), dout_rows)):
            vec_ref[row + 2:row + 3, :] += jnp.sum(val, **COLS)

    scatter.norm_loop(norm_rows)
    for i in range(4):
        wait_all(store_grad(i))
    own_copy.wait()
    gather.wait_pair('near')
    gather.links.finish()
    scatter.links.finish()


def scatter_scratch(rows, model):
    return [pltpu.VMEM((8, rows, model), BF16), pltpu.VMEM((4, rows, model), BF16),
            pltpu.VMEM((2, rows // 2, model), BF16), pltpu.VMEM((2, rows, model), BF16)]


def mlp_call(dfull, d_out, x_mid, gain, h1, z_saved, w2, w1):
    rows, model = d_out.shape
    seq, hidden = z_saved.shape
    return comm_call(
        mlp_kernel, "mlp_grads", 1, 60_000_000_000, (dfull, d_out, x_mid, gain, h1, z_saved, w2, w1),
        [HBM] * 3 + [VMEM] + [HBM] * 4,
        [shape((rows, model), BF16), shape((seq, hidden), BF16), shape((1, hidden), F32), shape((8, model), F32),
         shape(dfull.shape, BF16)],
        [VMEM, HBM, VMEM, VMEM, HBM],
        [pltpu.VMEM((hidden, model), BF16), pltpu.VMEM((model, hidden), BF16),
         pltpu.VMEM((4, 4, rows // 2, hidden), BF16), pltpu.VMEM((2, 4, rows // 2, model), BF16)]
        + scatter_scratch(rows, model) + [pltpu.VMEM((rows, model), BF16)] * 2
        + [DMA((4,))] + [DMA((4, 4))] * 3 + [DMA(())] + [COMM] * 4)


def gelu(pre_act):
    return 0.5 * pre_act * (1.0 + jnp.tanh(GELU_SCALE * (pre_act + GELU_COEF * pre_act * pre_act * pre_act)))


def ctx_kernel(dx1_ref, wo_ref, z_ref, dfull, mfull, do_ref, dw2_ref,
               mbuf, zv, ut, yv, obuf, own_sem, m_sem, load_sem, out_sem, *comm_sems):
    place = Place()
    place.barrier()
    rows, model = dx1_ref.shape
    gather = Gather(place, dx1_ref, mfull, *comm_sems)
    gather.start()
    own_copy = pltpu.make_async_copy(dx1_ref, mfull.at[place.me], own_sem)
    own_copy.start()

    loads = [pltpu.make_async_copy(z_ref, zv, load_sem.at[0]), pltpu.make_async_copy(dfull, yv, load_sem.at[1])]
    for copy in loads:
        copy.start()
    tiles = Tiles(obuf, dw2_ref, out_sem)
    count = model // OUT_TILE

    def turn(n):
        cols = tile_at(n, 256)
        ut[cols, :] = gelu(zv[:, cols].astype(F32)).astype(BF16).T

    def weight_tile(n):
        cols = tile_at(n, OUT_TILE)
        tiles.put(n, lambda: dot(ut[...], flat_cols(yv, cols)))

    loads[0].wait()
    loop(ut.shape[DIM0] // 256, turn)
    gather.relay()
    loads[1].wait()
    loop(count, weight_tile)
    gather.forward('X')
    gather.forward('Y')
    own_copy.wait()
    gather.links.wait('CO')

    def grad_ctx(i):
        @pl.when(i == 1)
        def _():
            gather.links.wait('CY')

        @pl.when(i == 2)
        def _():
            gather.links.wait('CX')

        @pl.when(i == 3)
        def _():
            gather.forward('D')
            gather.links.wait('CD')

        pair = place.pair_at(3 - i)
        copy = pltpu.make_async_copy(mfull.at[pl.ds(2 * pair, 2)], mbuf, m_sem)
        copy.start()
        copy.wait()
        do_ref[:, tile_at(pair, 2 * rows)] = dot_t(wo_ref[...], mbuf[...].reshape(2 * rows, model)).astype(BF16)

    loop(4, grad_ctx)
    tiles.finish(count)
    gather.links.finish()


def ctx_call(dx1, w_rows, z_saved, dfull):
    rows, model = dx1.shape
    feats = w_rows.shape[DIM0]
    seq, hidden = z_saved.shape
    return comm_call(
        ctx_kernel, "ctx_grads", 2, 30_000_000_000, (dx1, w_rows, z_saved, dfull), [VMEM] * 2 + [HBM] * 2,
        [shape((seq // rows, rows, model), BF16), shape((feats, seq), BF16), shape((hidden, model), F32)], [HBM, VMEM, HBM],
        [pltpu.VMEM((2, rows, model), BF16), pltpu.VMEM((seq, hidden), BF16), pltpu.VMEM((hidden, seq), BF16),
         pltpu.VMEM((seq // rows, rows, model), BF16), pltpu.VMEM((2, hidden, OUT_TILE), F32),
         DMA(()), DMA(()), PAIR, PAIR] + [COMM] * 2)


def bwd_kernel(h1_ref, q_hbm, k_hbm, v_hbm, do_hbm, wide_hbm, max_ref, inv_ref, dz_ref, h2_in,
               h2full, h1full, qkv_out, dw1_ref,
               k_rows, v_rows, q_rows, do_rows, delta, dq_acc, dk_acc, dv_acc, tok, dzv, wbuf,
               q_ref, k_ref, v_ref, do_ref, wide_ref, out_ref, own_sem, head_sem, load_sem, out_sem, *comm_sems):
    place = Place()
    place.barrier()
    gather1 = ThirdGather(place, h1full, *comm_sems[0:2])
    gather2 = ThirdGather(place, h2full, *comm_sems[2:4])
    gather2.start('rest', None)
    gather2.start('diag', None)
    gather1.start('near', h1_ref)
    gather1.start('rest', h1_ref)
    loads = start_copies(head_sem, (k_hbm, k_ref), (v_hbm, v_ref), (q_hbm, q_ref), (do_hbm, do_ref), (wide_hbm, wide_ref))
    own_copy = pltpu.make_async_copy(h1_ref, h1full.at[place.me], own_sem)
    own_copy.start()
    heads, dim, seq = q_ref.shape
    blocks = seq // BLK
    scale = dim ** -0.5
    exp_scale = scale * LOG2E

    def head(h):
        k_rows[...] = k_ref[h].T
        v_rows[...] = v_ref[h].T
        q_rows[...] = q_ref[h].T
        do_rows[...] = do_ref[h].T
        delta[...] = jnp.sum(do_ref[h].astype(F32) * wide_ref[h], **COLS)
        dq_acc[...] = jnp.zeros_like(dq_acc)
        dk_acc[...] = jnp.zeros_like(dk_acc)
        dv_acc[...] = jnp.zeros_like(dv_acc)

        def block(qi, ki, on_diag):
            q_at, k_at = tile_at(qi, BLK), tile_at(ki, BLK)
            scores = dot(k_rows[k_at, :], q_ref[h, :, q_at])
            if on_diag:
                scores = causal_fill(scores, -1e30)
            probs = jnp.exp2((scores - max_ref[h, :, q_at]) * exp_scale) * inv_ref[h, :, q_at]
            grad_probs = dot(v_rows[k_at, :], do_ref[h, :, q_at])
            dv_acc[k_at, :] += dot(probs.astype(BF16), do_rows[q_at, :])
            grad_scores = (probs * (grad_probs - delta[:, q_at]) * scale).astype(BF16)
            dk_acc[k_at, :] += dot(grad_scores, q_rows[q_at, :])
            dq_acc[:, q_at] += dot(k_ref[h, :, k_at], grad_scores)

        loop(blocks, lambda i: block(i, i, True))
        loop(blocks, lambda ki: loop(blocks, lambda qi: block(qi, ki, False), ki + 1))
        out_ref[0, h] = dq_acc[...].astype(BF16)
        out_ref[1, h] = dk_acc[...].astype(BF16).T
        out_ref[2, h] = dv_acc[...].astype(BF16).T

    load_grad, load_tok = [pltpu.make_async_copy(src, dst, load_sem.at[i])
                           for i, (src, dst) in enumerate(((dz_ref, dzv), (h2full, tok)))]
    for copy in loads:
        copy.wait()
    count = tok.shape[DIM2] // OUT_TILE
    tiles = Tiles(wbuf, dw1_ref, out_sem, rows=True)

    def fc1_tile(n):
        cols = tile_at(n, OUT_TILE)
        tiles.put(n, lambda: dot(flat_cols(tok, cols).T, dzv[...]))

    def head_step(h):
        head(h)

        @pl.when(h == 1)
        def _():
            load_grad.start()
            gather2.forward('rest')

        @pl.when(h == heads - 2)
        def _():
            gather2.forward('diag')
            gather2.wait_pair('rest')

    loop(heads - 1, head_step)
    gather2.wait_pair('diag')
    load_tok.start()
    head(heads - 1)
    load_grad.wait()
    load_tok.wait()
    results = start_copies(head_sem, (out_ref, qkv_out))
    loop(count, fc1_tile)
    for third in ('near', 'rest'):
        gather1.forward(third)
    for third in ('near', 'rest'):
        gather1.wait_pair(third)
    own_copy.wait()
    wait_all(results)
    tiles.finish(count)
    gather1.links.finish()
    gather2.links.finish()


def bwd_call(h1, q_t, k_t, v_t, do_t, wide, row_max, row_inv, dz, h2full):
    heads, dim, seq = q_t.shape
    rows, model = h1.shape
    full = shape((seq // rows, rows, model), BF16)
    turned = pltpu.VMEM((seq, dim), BF16)
    hidden = dz.shape[DIM1]
    return comm_call(
        bwd_kernel, "attn_bwd", 3, 80_000_000_000,
        (h1, q_t, k_t, v_t, do_t, wide, row_max, row_inv, dz, h2full), [VMEM] + [HBM] * 5 + [VMEM] * 2 + [HBM] * 2,
        [full, full, shape((3, heads, dim, seq), BF16), shape((model, hidden), F32)], [HBM] * 4,
        [turned] * 4 + [pltpu.VMEM((1, seq), F32), pltpu.VMEM((dim, seq), F32), pltpu.VMEM((seq, dim), F32),
                        pltpu.VMEM((seq, dim), F32), pltpu.VMEM((seq // rows, rows, model), BF16),
                        pltpu.VMEM((seq, hidden), BF16), pltpu.VMEM((2, OUT_TILE, hidden), F32),
                        *[pltpu.VMEM(q_t.shape, BF16)] * 4, pltpu.VMEM(wide.shape, F32), pltpu.VMEM((3, heads, dim, seq), BF16),
                        DMA(()), DMA((5,)), PAIR, PAIR] + [COMM] * 4,
        aliases={9: 0})


def qkv_kernel(qkv_hbm, w_hbm, dx1_hbm, x_hbm, gain_ref, vec_ref, ctx_hbm, mfull, h1_in,
               dx_ref, vsum_ref, bias_ref, dwo_ref, dw_ref, h1full,
               turned, part, crecv, diag_recv, last_recv, vacc, vsend, vrecv, last_got, tok, obuf, wbuf,
               qkv_ref, w_ref, dx1_ref, x_ref, ctx_ref, vsem, last_sem, load_sem, in_sem, out_sem, *comm_sems):
    place = Place()
    place.barrier(everyone=True)
    rows, model = dx1_ref.shape
    scatter = Scatter(place, part, crecv, diag_recv, last_recv, *comm_sems[0:2])
    gather = ThirdGather(place, h1full, *comm_sems[2:4])
    gather.start('diag', None)
    inputs = start_copies(in_sem, (qkv_hbm, qkv_ref), (w_hbm, w_ref), (ctx_hbm, ctx_ref), (dx1_hbm, dx1_ref), (x_hbm, x_ref))
    loads = [pltpu.make_async_copy(src, tok, load_sem.at[i]) for i, src in enumerate((mfull, h1full))]
    tiles_o = Tiles(obuf, dwo_ref, out_sem.at[0])
    tiles = Tiles(wbuf, dw_ref, out_sem.at[1])
    count = model // OUT_TILE
    swaps = Links(place, vsem.at[0], vsem.at[1])
    inputs[0].wait()

    def vec_step(i):
        if i > 0:
            swaps.wait('CXY'[i - 1])
            vacc[...] += vrecv[i - 1]
        if i < 3:
            vsend[i] = vacc[...]

    def vec_send(i):
        swaps.send('CXY'[i], 'CXY'[i], vsend, vrecv, i)

    vacc[...] = vec_ref[...]
    vec_step(0)
    vec_send(0)

    def pair_step(i):
        for c in range(4):
            slot, at = place.chunk(i, c)
            turned[tile_at(c, rows // 2), :] = qkv_ref[:, tile_at(2 * slot + at, rows // 2)].T

        @pl.when(i == 0)
        def _():
            inputs[1].wait()

        @pl.when(i == 1)
        def _():
            loads[0].start()

        @pl.when(i == 3)
        def _():
            gather.forward('diag')

        for at in range(1, 3):
            @pl.when(i == at)
            def _():
                vec_step(at)
                vec_send(at)

        scatter.between(i)

        def grad_norm(n):
            cols = tile_at(n, TILE)
            scatter.store(i, cols, dot(turned[...], w_ref[:, cols]).astype(BF16))

        loop(model // TILE, grad_norm)
        scatter.after(i)

    loop(4, pair_step)
    loads[0].wait()
    for copy in inputs[2:]:
        copy.wait()

    def proj_tile(n):
        cols = tile_at(n, OUT_TILE)
        tiles_o.put(n, lambda: dot(ctx_ref[...], flat_cols(tok, cols)))

    def qkv_tile(n):
        cols = tile_at(n, OUT_TILE)
        tiles.put(n, lambda: dot(qkv_ref[...], flat_cols(tok, cols)))

    loop(count, proj_tile)
    scatter.add_diag()
    gather.wait_pair('diag')
    loads[1].start()
    ones = jnp.ones((8, qkv_ref.shape[DIM1]), BF16)
    kinds, heads, dim = bias_ref.shape
    for row in range(kinds * heads):
        feats = qkv_ref[row * dim:(row + 1) * dim, :]
        bias_ref[row // heads, row % heads, :] = dot_t(ones, feats)[0]
    loads[1].wait()
    loop(count, qkv_tile)
    vec_step(3)
    tiles_o.finish(count)
    gain = gain_ref[...].reshape(1, model)

    def norm_rows(at):
        grad = scatter.total(at)
        x_hat, inv_std = layer_norm_hat(x_ref[at, :].astype(F32))
        dx_ref[at, :] = (dx1_ref[at, :].astype(F32) + layer_norm_bwd(grad, x_hat, inv_std, gain)).astype(BF16)
        vacc[0:1, :] += jnp.sum(grad * x_hat, **COLS)
        vacc[1:2, :] += jnp.sum(grad, **COLS)

    scatter.norm_loop(norm_rows)
    finals = Links(place, last_sem.at[0], last_sem.at[1])
    last_got[0] = vacc[0:2, :]
    vsum_ref[2:6, :] = vacc[2:6, :]
    for k in range(1, 8):
        finals.send(k, k, (last_got, (0,)), (last_got, (k,)))
    tiles.finish(count)
    finals.wait(*range(1, 8))
    total = last_got[place.me]
    for source in range(1, 8):
        total += last_got[(place.me + 8 - source) % 8]
    vsum_ref[0:2, :] = total
    for links in (swaps, finals, scatter.links, gather.links):
        links.finish()


def qkv_call(heads, qkv_rows, w_rows, dx1, x_in, gain, vec, ctx_rows, mfull, h1full):
    rows, model = dx1.shape
    feats, seq = qkv_rows.shape
    proj = ctx_rows.shape[DIM0]
    return comm_call(
        qkv_kernel, "qkv_grads", 4, 30_000_000_000,
        (qkv_rows, w_rows, dx1, x_in, gain, vec, ctx_rows, mfull, h1full), [HBM] * 4 + [VMEM] * 2 + [HBM] * 3,
        [shape((rows, model), BF16), shape((6, model), F32), shape((3, heads, feats // (3 * heads)), F32), shape((proj, model), F32),
         shape((feats, model), F32), shape(h1full.shape, BF16)],
        [VMEM] * 3 + [HBM] * 3,
        [pltpu.VMEM((2 * rows, feats), BF16)] + scatter_scratch(rows, model)
        + [pltpu.VMEM((8, model), F32), pltpu.VMEM((3, 8, model), F32), pltpu.VMEM((3, 8, model), F32),
           pltpu.VMEM((8, 2, model), F32), pltpu.VMEM((8, rows, model), BF16),
           pltpu.VMEM((2, proj, OUT_TILE), F32), pltpu.VMEM((2, feats, OUT_TILE), F32),
           pltpu.VMEM((feats, seq), BF16), pltpu.VMEM((feats, model), BF16), pltpu.VMEM((rows, model), BF16),
           pltpu.VMEM((rows, model), BF16), pltpu.VMEM((proj, seq), BF16),
           DMA((2, 3)), DMA((2, 7)), PAIR, DMA((5,)), DMA((2, 2))] + [COMM] * 4,
        aliases={8: 5})


def finish_kernel(*refs):
    count = len(refs) // 3
    refs[2 * count - 1][...] = refs[count - 1][...].reshape(refs[2 * count - 1].shape)
    rings, single, (small_sem, in_sem, out_sem) = refs[2 * count:2 * count + 2], refs[2 * count + 2:-3], refs[-3:]
    chunks, used = [], [0, 0]
    small = [(src, buf, dst) for src, buf, dst in zip(refs[4:count - 1], single, refs[count + 4:2 * count - 1])]
    for i, (src, buf, _) in enumerate(small):
        pltpu.make_async_copy(src, buf, small_sem.at[0, i]).start()
    for src, dst in zip(refs[:4], refs[count:count + 4]):
        kind = 0 if src.shape[DIM1] == rings[0].shape[DIM2] else 1
        rows = rings[kind].shape[DIM1]
        for row in range(0, src.shape[DIM0], rows):
            chunks.append((src.at[pl.ds(row, rows)], dst.at[pl.ds(row, rows)], kind, used[kind]))
            used[kind] += 1

    def copy_in(src, dst, kind, at):
        slot = at % RING
        return pltpu.make_async_copy(src, rings[kind].at[slot], in_sem.at[kind, slot])

    def copy_out(src, dst, kind, at):
        slot = at % RING
        return pltpu.make_async_copy(rings[kind].at[slot], dst, out_sem.at[kind, slot])

    waiting = {}

    def start(chunk):
        key = (chunk[2], chunk[3] % RING)
        if key in waiting:
            copy_out(*waiting.pop(key)).wait()
        copy_in(*chunk).start()

    for chunk in chunks[:AHEAD]:
        start(chunk)
    for i, (src, buf, dst) in enumerate(small):
        pltpu.make_async_copy(src, buf, small_sem.at[0, i]).wait()
        pltpu.make_async_copy(buf, dst, small_sem.at[1, i]).start()
    for i, chunk in enumerate(chunks):
        copy_in(*chunk).wait()
        copy_out(*chunk).start()
        waiting[(chunk[2], chunk[3] % RING)] = chunk
        if i + AHEAD < len(chunks):
            start(chunks[i + AHEAD])
    for chunk in waiting.values():
        copy_out(*chunk).wait()
    for i, (_, buf, dst) in enumerate(small):
        pltpu.make_async_copy(buf, dst, small_sem.at[1, i]).wait()


RING = 8
AHEAD = 12


def finish_call(*arrays):
    wide = max(a.shape[DIM1] for a in arrays[:4])
    narrow = min(a.shape[DIM1] for a in arrays[:4])
    small = [pltpu.VMEM(a.shape, a.dtype) for a in arrays[4:-1]]
    return pl.pallas_call(
        finish_kernel, name="finish", in_specs=[HBM] * (len(arrays) - 1) + [VMEM], out_specs=[HBM] * (len(arrays) - 1) + [VMEM],
        out_shape=[shape(a.shape, a.dtype) for a in arrays[:-1]] + [shape(arrays[-1].shape[1:], F32)],
        scratch_shapes=[pltpu.VMEM((RING, 320, wide), F32), pltpu.VMEM((RING, 640, narrow), F32), *small,
                        DMA((2, len(small))), DMA((2, RING)), DMA((2, RING))],
        compiler_params=pltpu.CompilerParams(vmem_limit_bytes=66_000_000),
        cost_estimate=pl.CostEstimate(flops=1_000_000, bytes_accessed=72_000_000, transcendentals=0),
    )(*arrays)


def solution(mesh):
    def local_backward(x_in, x_mid, d_out, q_saved, k_saved, v_saved, z_saved, ln1_gain, ln1_bias, ln2_gain, ln2_bias, w_qkv, w_proj, w_fc1, w_fc2):
        x_in, x_mid, d_out, z_saved = x_in[0], x_mid[0], d_out[0], z_saved[0]
        heads, dim = q_saved.shape[2:]
        seq, model = z_saved.shape[DIM0], x_in.shape[DIM1]
        q_t, k_t, v_t = (v[0].transpose(1, 2, 0) for v in (q_saved, k_saved, v_saved))
        affine = (ln1_gain, ln1_bias, ln2_gain, ln2_bias)
        dfull, ctx_t, wide_t, row_max, row_inv, h1_local, h2_local = fwd_call(d_out, q_t, k_t, v_t, x_in, x_mid, affine)
        dx1, grad_pre, grad_bfc1, vec, h2_full = mlp_call(dfull, d_out, x_mid, ln2_gain, h2_local, z_saved, w_fc2, w_fc1)
        mfull, do_t, grad_wfc2 = ctx_call(dx1, w_proj.reshape(heads * dim, model), z_saved, dfull)
        _, h1_full, qkv_t, grad_wfc1 = bwd_call(
            h1_local, q_t, k_t, v_t, do_t.reshape(heads, dim, seq), wide_t, row_max, row_inv, grad_pre, h2_full)
        qkv_rows = qkv_t.reshape(3 * heads * dim, seq)
        w_rows = w_qkv.transpose(0, 2, 3, 1).reshape(3 * heads * dim, model)
        grad_x, grad_vecs, grad_bqkv, grad_wproj, grad_wqkv, _ = qkv_call(
            heads, qkv_rows, w_rows, dx1, x_in, ln1_gain, vec, ctx_t.reshape(heads * dim, seq), mfull, h1_full)
        grad_wfc2, grad_wfc1, grad_wqkv, grad_wproj, grad_x, grad_vecs, grad_bqkv, grad_bfc1 = finish_call(
            grad_wfc2, grad_wfc1, grad_wqkv, grad_wproj, grad_x, grad_vecs, grad_bqkv, grad_bfc1)
        grad_wproj = grad_wproj.reshape(heads, dim, model)
        grad_wqkv = grad_wqkv.reshape(3, heads, dim, model).transpose(0, 3, 1, 2)
        return grad_x[None], grad_wqkv, grad_bqkv, grad_wproj, grad_wfc1, grad_bfc1, grad_wfc2, grad_vecs

    tok_spec = P('dp', 'tp', None)
    head_spec = P('dp', None, 'tp', None)
    in_specs = (tok_spec, tok_spec, tok_spec, head_spec, head_spec, head_spec, P('dp', None, 'tp'),
                P(None), P(None), P(None), P(None),
                P(None, None, 'tp', None), P('tp', None, None), P(None, 'tp'), P('tp', None))
    out_specs = (tok_spec, P('dp', None, 'tp', None), P('dp', 'tp', None), P(('dp', 'tp'), None, None),
                 P('dp', 'tp'), P(('dp', 'tp')), P(('dp', 'tp'), None), P('dp', None))
    return jax.shard_map(local_backward, mesh=mesh, in_specs=in_specs, out_specs=out_specs, check_vma=False)
```

```python
import jax
import jax.numpy as jnp
from jax import lax
from jax.experimental import pallas as pl
from jax.experimental.pallas import tpu as pltpu
from jax.sharding import PartitionSpec as P

LN_EPS = 1e-5
GELU_COEF = 0.044715
GELU_SCALE = 0.7978845608028654
LOG2E = 1.4426950408889634
BLK = 512
F32 = jnp.float32
BF16 = jnp.bfloat16
DIM0, DIM1, DIM2 = range(3)
COLS = dict(axis=0, keepdims=True)
ROWS = dict(axis=-1, keepdims=True)


def layer_norm_bwd(grad_norm, x_hat, inv_std, norm_gain):
    grad_hat = grad_norm * norm_gain
    centered_grad = grad_hat - jnp.mean(grad_hat, **ROWS)
    return inv_std * (centered_grad - x_hat * jnp.mean(grad_hat * x_hat, **ROWS))


def dot(a, b):
    return jnp.dot(a, b, preferred_element_type=F32)


def causal_fill(scores, fill):
    key_ids = lax.broadcasted_iota(jnp.int32, scores.shape, 0)
    query_ids = lax.broadcasted_iota(jnp.int32, scores.shape, 1)
    return jnp.where(query_ids >= key_ids, scores, fill)


class Place:
    def __init__(self):
        self.group = lax.axis_index('dp')
        self.me = lax.axis_index('tp')
        self.core = self.me % 2
        self.dx = 2 - 4 * ((self.me // 2) % 2)
        self.dy = 4 - 8 * (self.me // 4)
        self.dc = 1 - 2 * self.core
        self.peer = {'X': self.me + self.dx, 'Y': self.me + self.dy, 'C': self.me + self.dc}
        self.peer.update({k: (self.me + k) % 8 for k in range(1, 8)})
        self.block = {'O': self.me, 'X': self.me + self.dx, 'Y': self.me + self.dy, 'D': self.me + self.dx + self.dy}
        self.pair = {key: val // 2 for key, val in self.block.items()}
        self.other = {key: val + self.dc for key, val in self.block.items()}
        self.x, self.y = (self.me // 2) % 2, self.me // 4

    def pair_at(self, i):
        flip_x, flip_y = 1 - i // 2, 1 - i % 2
        return 2 * (self.y + flip_y * (1 - 2 * self.y)) + self.x + flip_x * (1 - 2 * self.x)

    def chunk(self, i, c):
        mixed = i * (3 - i) // 2
        pair, half = (self.pair['X'], i - 1) if c < 2 else (self.pair['Y'], 2 - i)
        slot = (1 - mixed) * (2 * self.pair_at(i) + c // 2) + mixed * (2 * pair + c % 2)
        return slot, (1 - mixed) * (c % 2) + mixed * half

    def barrier(self, everyone=False):
        sem = pltpu.get_barrier_semaphore()
        keys = range(1, 8) if everyone else 'XYC'
        for key in keys:
            pl.semaphore_signal(sem, inc=1, device_id=(self.group, self.peer[key]), device_id_type=pl.DeviceIdType.MESH)
        pl.semaphore_wait(sem, len(keys))


class Links:
    def __init__(self, place, send_sem, recv_sem):
        self.place, self.send_sem, self.recv_sem = place, send_sem, recv_sem
        self.copies = {}

    def define(self, name, to, src, dst, *index):
        at = len(self.copies)

        def place_of(ref):
            ref, where = ref if isinstance(ref, tuple) else (ref, index)
            return ref.at[where] if where else ref

        def copy():
            return pltpu.make_async_remote_copy(
                src_ref=place_of(src), dst_ref=place_of(dst), send_sem=self.send_sem.at[at], recv_sem=self.recv_sem.at[at],
                device_id=(self.place.group, self.place.peer[to]), device_id_type=pl.DeviceIdType.MESH)

        self.copies[name] = copy

    def start(self, name):
        self.copies[name]().start()

    def send(self, name, *rest):
        self.define(name, *rest)
        self.start(name)

    def wait(self, *names):
        for name in names:
            self.copies[name]().wait_recv()

    def finish(self):
        for copy in self.copies.values():
            copy().wait_send()


class Gather:
    COPIES = 10

    def __init__(self, place, own, full, send_sem, recv_sem):
        self.place, self.own, self.full = place, own, full
        self.links = Links(place, send_sem, recv_sem)
        half = own.shape[DIM0] // 2
        self.first, self.second = pl.ds(0, half), pl.ds(half, half)

    def start(self):
        me, full, own, send = self.place.me, self.full, self.own, self.links.send
        for name, half in (('Xa', self.first), ('Yb', self.second), ('Xb', self.second), ('Ya', self.first)):
            send(name, name[0], (own, (half,)), (full, (me, half)))
        send('CO', 'C', (own, ()), (full, (me,)))

    def relay(self):
        links, full, block = self.links, self.full, self.place.block
        links.wait('Xa')
        links.send('Da', 'Y', full, full, block['X'], self.first)
        links.wait('Yb')
        links.send('Db', 'X', full, full, block['Y'], self.second)

    def forward(self, key):
        first, second = ('Xb', None) if key == 'X' else ('Ya', None) if key == 'Y' else ('Da', 'Db')
        self.links.wait(first)
        if second:
            self.links.wait(second)
        self.links.send('C' + key, 'C', self.full, self.full, self.place.block[key])


class ThirdGather:
    def __init__(self, place, full, send_sem, recv_sem):
        self.place, self.full = place, full
        self.links = Links(place, send_sem, recv_sem)
        half = full.shape[DIM1] // 2
        self.first, self.second = pl.ds(0, half), pl.ds(half, half)

    def start(self, third, own):
        me, full, block = self.place.me, self.full, self.place.block
        near = {'near': {'X': self.first, 'Y': self.second}, 'rest': {'X': self.second, 'Y': self.first}}.get(third)
        for key in 'XY':
            if near is None:
                slot, half = (block['Y'], self.second) if key == 'X' else (block['X'], self.first)
                self.links.send(third + key, key, full, full, slot, half)
            else:
                src = (full, (me, near[key])) if own is None else (own, (near[key],))
                self.links.send(third + key, key, src, (full, (me, near[key])))
        if third == 'near':
            self.links.send('CO', 'C', (own, ()), (full, (me,)))

    def forward(self, third):
        block = self.place.block
        for key in 'XY':
            self.links.wait(third + key)
            half = self.first if (third == 'near') == (key == 'X') else self.second
            slot = block[key]
            if third == 'diag':
                slot, half = block['D'], (self.second if key == 'X' else self.first)
            self.links.send('C' + third + key, 'C', self.full, self.full, slot, half)

    def wait_pair(self, third):
        self.links.wait('C' + third + 'X', 'C' + third + 'Y', *(('CO',) if third == 'near' else ()))


CRECV = dict(O=0, Xa=1, Xb=1, Ya=2, Yb=2, D=3)


class Scatter:
    COPIES = 10

    def __init__(self, place, part, crecv, diag_recv, last_recv, send_sem, recv_sem):
        self.place, self.part, self.crecv = place, part, crecv
        self.diag_recv, self.last_recv = diag_recv, last_recv
        self.links = Links(place, send_sem, recv_sem)
        half = part.shape[DIM1] // 2
        self.half = {'a': pl.ds(0, half), 'b': pl.ds(half, half)}
        for name, at in CRECV.items():
            index = (at,) if len(name) == 1 else (at, self.half[name[1]])
            self.links.define('C' + name, 'C', (part, (place.other[name[0]],) + index[1:]), (crecv, index))

    def add_rows(self, slot, start, count, other, other_start):
        step = 64

        def body(i, carry):
            here = pl.ds(pl.multiple_of(start + i * step, step), step)
            there = pl.ds(pl.multiple_of(other_start + i * step, step), step)
            total = self.part[slot, here, :].astype(F32) + other[there, :].astype(F32)
            self.part[slot, here, :] = total.astype(BF16)
            return carry

        lax.fori_loop(0, count // step, body, 0)

    def store(self, i, cols, rows):
        for c in range(4):
            slot, half = self.place.chunk(i, c)
            size = rows.shape[DIM0] // 4
            self.part[slot, tile_at(half, size), cols] = rows[c * size:(c + 1) * size]

    def swap(self, *names):
        for name in names:
            self.links.start('C' + name)

    def add_pair(self, name):
        self.links.wait('C' + name)
        rows = self.part.shape[DIM1]
        start, count = (0, rows) if len(name) == 1 else ((rows // 2) * 'ab'.index(name[1]), rows // 2)
        self.add_rows(self.place.block[name[0]], start, count, self.crecv.at[CRECV[name]], start)

    def send_half(self, key, half):
        at = self.half[half]
        self.links.send(key + half, key, (self.part, (self.place.block[key], at)), (self.last_recv, ('XY'.index(key), at)))

    def send_diag(self):
        for i, (key, half) in enumerate((('X', 'a'), ('Y', 'b'))):
            self.links.send('D' + half, key, (self.part, (self.place.block['D'], self.half[half])), (self.diag_recv, (i,)))

    def add_diag(self):
        self.add_pair('Xb')
        self.add_pair('Ya')
        rows = self.part.shape[DIM1] // 4
        for i, (half, key, start) in enumerate((('a', 'Y', 0), ('b', 'X', 2 * rows))):
            self.links.wait('D' + half)
            for quarter in range(2):
                off = quarter * rows
                self.add_rows(self.place.block[key], start + off, rows, self.diag_recv.at[i], off)
                at = pl.ds(start + off, rows)
                self.links.send(key + half + str(quarter), key, (self.part, (self.place.block[key], at)),
                                (self.last_recv, ('XY'.index(key), at)))

    def wait_last(self, quarter):
        if quarter == 0:
            self.links.wait('Xa', 'Yb', 'CO')
        self.links.wait('Ya' + str(quarter), 'Xb' + str(quarter))

    def norm_loop(self, body):
        rows = self.part.shape[DIM1]
        chunks = rows // LN_ROWS
        quarter = chunks // 4

        def step(i):
            for part in range(2):
                @pl.when(i == part * (chunks // 2))
                def _():
                    self.wait_last(part)

            part, j = i // (2 * quarter), i % (2 * quarter)
            body(tile_at((j // quarter) * 2 * quarter + part * quarter + j % quarter, LN_ROWS))

        loop(chunks, step)

    def between(self, i):
        @pl.when(i == 1)
        def _():
            self.add_pair('D')
            self.send_diag()

        @pl.when(i == 2)
        def _():
            for name in ('Xa', 'Yb'):
                self.add_pair(name)
                self.send_half(*name)

    def after(self, i):
        for at, names in enumerate((('D',), ('Xa', 'Yb'), ('Xb', 'Ya'), ('O',))):
            @pl.when(i == at)
            def _():
                self.swap(*names)

    def total(self, at):
        me = self.place.me
        return (self.part[me, at, :].astype(F32) + self.crecv[0, at, :].astype(F32)
                + self.last_recv[0, at, :].astype(F32) + self.last_recv[1, at, :].astype(F32))


def gelu_slope(pre_act):
    tanh_val = jnp.tanh(GELU_SCALE * (pre_act + GELU_COEF * pre_act * pre_act * pre_act))
    return 0.5 * (1.0 + tanh_val) + 0.5 * pre_act * (1.0 - tanh_val * tanh_val) * GELU_SCALE * (1.0 + 3.0 * GELU_COEF * pre_act * pre_act)


def layer_norm_hat(rows_f32):
    centered = rows_f32 - jnp.mean(rows_f32, **ROWS)
    inv_std = lax.rsqrt(jnp.mean(centered * centered, **ROWS) + LN_EPS)
    return centered * inv_std, inv_std


LN_ROWS = 32
TILE = 1280
VMEM = pl.BlockSpec(memory_space=pltpu.VMEM)
HBM = pl.BlockSpec(memory_space=pl.ANY)
DMA = pltpu.SemaphoreType.DMA
COMM = DMA((14,))
PAIR = DMA((2,))
shape = jax.ShapeDtypeStruct


def tile_at(i, size):
    return pl.ds(pl.multiple_of(i * size, size), size)


def start_all(copies):
    for copy in copies:
        copy.start()
    return copies


def wait_all(copies):
    for copy in copies:
        copy.wait()


def start_copies(sem, *pairs):
    return start_all([pltpu.make_async_copy(src, dst, sem.at[i]) for i, (src, dst) in enumerate(pairs)])


def loop(count, body, start=0):
    def step(i, carry):
        body(i)
        return carry

    lax.fori_loop(start, count, step, 0)


def comm_call(kernel, name, ident, flops, args, in_specs, out_shape, out_specs, scratch, aliases={}):
    return pl.pallas_call(
        kernel, in_specs=in_specs, out_specs=out_specs, out_shape=out_shape, scratch_shapes=scratch, name=name,
        input_output_aliases=aliases,
        compiler_params=pltpu.CompilerParams(collective_id=ident, has_side_effects=True, vmem_limit_bytes=66_000_000),
        cost_estimate=pl.CostEstimate(flops=flops, bytes_accessed=flops // 1000, transcendentals=flops // 1000),
    )(*args)


class Tiles:
    def __init__(self, buf, out, sem, rows=False):
        self.buf, self.out, self.sem, self.rows = buf, out, sem, rows

    def copy(self, n):
        size = self.buf.shape[1 if self.rows else 2]
        at = tile_at(n, size)
        dst = self.out.at[at] if self.rows else self.out.at[:, at]
        return pltpu.make_async_copy(self.buf.at[n % 2], dst, self.sem.at[n % 2])

    def put(self, n, value):
        @pl.when(n >= 2)
        def _():
            self.copy(n - 2).wait()

        self.buf[n % 2] = value()
        self.copy(n).start()

    def finish(self, count):
        self.copy(count - 2).wait()
        self.copy(count - 1).wait()


OUT_TILE = 512


def flat_cols(ref, cols):
    return ref[:, :, cols].reshape(ref.shape[DIM0] * ref.shape[DIM1], OUT_TILE)


def fwd_kernel(dout_ref, q_hbm, k_hbm, v_hbm, x_hbm, mid_hbm, gain1_ref, bias1_ref, gain2_ref, bias2_ref,
               dfull, ctx_out, wide_out, max_ref, inv_ref, h1_out, h2_out,
               k_rows, strip, q_ref, k_ref, v_ref, ctx_ref, x_ref, mid_ref, h1_ref, h2_ref, wide_ref,
               own_sem, load_sem, *comm_sems):
    place = Place()
    place.barrier()
    gather = Gather(place, dout_ref, dfull, *comm_sems)
    gather.start()
    loads = start_copies(load_sem, (x_hbm, x_ref), (mid_hbm, mid_ref), (k_hbm, k_ref), (q_hbm, q_ref), (v_hbm, v_ref))
    own_copy = pltpu.make_async_copy(dout_ref, dfull.at[place.me], own_sem)
    own_copy.start()
    heads, dim, seq = q_ref.shape
    exp_scale = dim ** -0.5 * LOG2E
    loads[0].wait()
    loads[1].wait()
    affine = [ref[...].reshape(1, ref.shape[DIM0]) for ref in (gain1_ref, bias1_ref, gain2_ref, bias2_ref)]

    def norm_rows(i):
        at = tile_at(i, LN_ROWS)
        for row, (src, dst) in enumerate(((x_ref, h1_ref), (mid_ref, h2_ref))):
            x_hat, _ = layer_norm_hat(src[at, :].astype(F32))
            dst[at, :] = (x_hat * affine[2 * row] + affine[2 * row + 1]).astype(BF16)

    loop(x_ref.shape[DIM0] // LN_ROWS, norm_rows)
    for copy in loads[2:]:
        copy.wait()

    def head(h):
        k_rows[...] = k_ref[h].T

        def query_block(qi):
            q_at = tile_at(qi, BLK)
            q_blk = q_ref[h, :, q_at]

            def score_step(ki, run_max):
                at = tile_at(ki, BLK)
                blk = dot(k_rows[at, :], q_blk)
                strip[at, :] = blk
                return jnp.maximum(run_max, jnp.max(blk, **COLS))

            diag = causal_fill(dot(k_rows[q_at, :], q_blk), -1e30)
            strip[q_at, :] = diag
            row_max = lax.fori_loop(0, qi, score_step, jnp.max(diag, **COLS))

            def exp_step(ki, run_sum):
                at = tile_at(ki, BLK)
                probs = jnp.exp2((strip[at, :] - row_max) * exp_scale)
                strip[at, :] = probs
                return run_sum + jnp.sum(probs, **COLS)

            row_inv = 1.0 / lax.fori_loop(0, qi + 1, exp_step, jnp.zeros_like(row_max))

            def ctx_step(ki, carry):
                high, low = carry
                at = tile_at(ki, BLK)
                probs = strip[at, :] * row_inv
                probs_low = probs.astype(BF16)
                rest = (probs - probs_low.astype(F32)).astype(BF16)
                v_blk = v_ref[h, :, at]
                return high + dot(v_blk, probs_low), low + dot(v_blk, rest)

            zero = jnp.zeros((dim, BLK), F32)
            high, low = lax.fori_loop(0, qi + 1, ctx_step, (zero, zero))
            ctx_ref[h, :, q_at] = high.astype(BF16)
            wide_ref[h, :, q_at] = high + low
            max_ref[h, :, q_at] = row_max
            inv_ref[h, :, q_at] = row_inv

        loop(seq // BLK, query_block)

    def head_step(h):
        head(h)

        @pl.when(h == 1)
        def _():
            gather.relay()

        @pl.when(h == 2)
        def _():
            gather.forward('X')
            gather.forward('Y')

    loop(heads, head_step)
    gather.forward('D')
    results = start_copies(load_sem, (ctx_ref, ctx_out), (wide_ref, wide_out), (h1_ref, h1_out), (h2_ref, h2_out))
    gather.links.wait('CO', 'CX', 'CY', 'CD')
    own_copy.wait()
    wait_all(results)
    gather.links.finish()


def fwd_call(d_out, q_t, k_t, v_t, x_in, x_mid, affine):
    heads, dim, seq = q_t.shape
    rows, model = d_out.shape
    return comm_call(
        fwd_kernel, "attn_fwd", 0, 40_000_000_000, (d_out, q_t, k_t, v_t, x_in, x_mid, *affine),
        [VMEM] + [HBM] * 5 + [VMEM] * 4,
        [shape((seq // rows, rows, model), BF16), shape((heads, dim, seq), BF16), shape((heads, dim, seq), F32),
         shape((heads, 1, seq), F32), shape((heads, 1, seq), F32), shape((rows, model), BF16), shape((rows, model), BF16)],
        [HBM] * 3 + [VMEM] * 2 + [HBM] * 2,
        [pltpu.VMEM((seq, dim), BF16), pltpu.VMEM((seq, BLK), F32)] + [pltpu.VMEM(q_t.shape, BF16)] * 4
        + [pltpu.VMEM((rows, model), BF16)] * 4 + [pltpu.VMEM(q_t.shape, F32)] + [DMA(()), DMA((5,))] + [COMM] * 2)


def dot_t(a, b):
    return lax.dot_general(a, b, (((1,), (1,)), ((), ())), preferred_element_type=F32)


def mlp_kernel(dfull, dout_hbm, mid_hbm, gain_ref, h2_ref, z_ref, w2_ref, w1_ref,
               dx1_ref, dz_ref, gb1_ref, vec_ref, h2full,
               w2v, w1v, dzv, ybuf, part, crecv, diag_recv, last_recv, dout_ref, mid_ref,
               load_sem, y_sem, z_sem, dz_sem, own_sem, *comm_sems):
    place = Place()
    place.barrier()
    rows, model = dout_hbm.shape
    hidden = w2v.shape[DIM0]
    scatter = Scatter(place, part, crecv, diag_recv, last_recv, *comm_sems[0:2])
    gather = ThirdGather(place, h2full, *comm_sems[2:4])
    gather.start('near', h2_ref)
    own_copy = pltpu.make_async_copy(h2_ref, h2full.at[place.me], own_sem)

    half = rows // 2

    def chunk_copies(i, copy):
        return [copy(c, *place.chunk(i, c)) for c in range(4)]

    def load_pair(i):
        return chunk_copies(i, lambda c, slot, at: pltpu.make_async_copy(
            dfull.at[slot, tile_at(at, half)], ybuf.at[i % 2, c], y_sem.at[i, c]))

    def load_pre(i):
        return chunk_copies(i, lambda c, slot, at: pltpu.make_async_copy(
            z_ref.at[tile_at(2 * slot + at, half)], dzv.at[i, c], z_sem.at[i, c]))

    def store_grad(i):
        return chunk_copies(i, lambda c, slot, at: pltpu.make_async_copy(
            dzv.at[i, c], dz_ref.at[tile_at(2 * slot + at, half)], dz_sem.at[i, c]))

    start_all(load_pair(0) + load_pre(0))
    loads = start_copies(load_sem, (w2_ref, w2v), (w1_ref, w1v), (dout_hbm, dout_ref), (mid_hbm, mid_ref))
    for i in range(1, 4):
        start_all(load_pre(i))
    start_all(load_pair(1))
    own_copy.start()
    gb1_ref[...] = jnp.zeros_like(gb1_ref)
    vec_ref[...] = jnp.zeros_like(vec_ref)
    loads[0].wait()

    def pair_step(i):
        wait_all(load_pair(i) + load_pre(i))

        def grad_act(n):
            cols = tile_at(n, TILE)
            acc = dot_t(ybuf[i % 2].reshape(2 * rows, model), w2v[cols, :])
            grad = (acc * gelu_slope(dzv[i, :, :, cols].reshape(2 * rows, TILE).astype(F32))).astype(BF16)
            dzv[i, :, :, cols] = grad.reshape(4, half, TILE)
            gb1_ref[:, cols] += jnp.sum(grad.astype(F32), **COLS)

        loop(hidden // TILE, grad_act)
        start_all(store_grad(i))

        @pl.when(i < 2)
        def _():
            start_all(load_pair(i + 2))

        @pl.when(i == 0)
        def _():
            loads[1].wait()

        @pl.when(i == 2)
        def _():
            gather.forward('near')

        scatter.between(i)

        @pl.when(i == 3)
        def _():
            scatter.add_diag()

        def grad_norm(n):
            cols = tile_at(n, TILE)
            scatter.store(i, cols, dot_t(dzv[i].reshape(2 * rows, hidden), w1v[cols, :]).astype(BF16))

        loop(model // TILE, grad_norm)
        scatter.after(i)

    loop(4, pair_step)

    gain = gain_ref[...].reshape(1, model)
    loads[2].wait()
    loads[3].wait()

    def norm_rows(at):
        grad = scatter.total(at)
        x_hat, inv_std = layer_norm_hat(mid_ref[at, :].astype(F32))
        dout_rows = dout_ref[at, :].astype(F32)
        mid = (dout_rows + layer_norm_bwd(grad, x_hat, inv_std, gain)).astype(BF16)
        dx1_ref[at, :] = mid
        for row, val in enumerate((grad * x_hat, grad, mid.astype(F32), dout_rows)):
            vec_ref[row + 2:row + 3, :] += jnp.sum(val, **COLS)

    scatter.norm_loop(norm_rows)
    for i in range(4):
        wait_all(store_grad(i))
    own_copy.wait()
    gather.wait_pair('near')
    gather.links.finish()
    scatter.links.finish()


def scatter_scratch(rows, model):
    return [pltpu.VMEM((8, rows, model), BF16), pltpu.VMEM((4, rows, model), BF16),
            pltpu.VMEM((2, rows // 2, model), BF16), pltpu.VMEM((2, rows, model), BF16)]


def mlp_call(dfull, d_out, x_mid, gain, h1, z_saved, w2, w1):
    rows, model = d_out.shape
    seq, hidden = z_saved.shape
    return comm_call(
        mlp_kernel, "mlp_grads", 1, 60_000_000_000, (dfull, d_out, x_mid, gain, h1, z_saved, w2, w1),
        [HBM] * 3 + [VMEM] + [HBM] * 4,
        [shape((rows, model), BF16), shape((seq, hidden), BF16), shape((1, hidden), F32), shape((8, model), F32),
         shape(dfull.shape, BF16)],
        [VMEM, HBM, VMEM, VMEM, HBM],
        [pltpu.VMEM((hidden, model), BF16), pltpu.VMEM((model, hidden), BF16),
         pltpu.VMEM((4, 4, rows // 2, hidden), BF16), pltpu.VMEM((2, 4, rows // 2, model), BF16)]
        + scatter_scratch(rows, model) + [pltpu.VMEM((rows, model), BF16)] * 2
        + [DMA((4,))] + [DMA((4, 4))] * 3 + [DMA(())] + [COMM] * 4)


def gelu(pre_act):
    return 0.5 * pre_act * (1.0 + jnp.tanh(GELU_SCALE * (pre_act + GELU_COEF * pre_act * pre_act * pre_act)))


def ctx_kernel(dx1_ref, wo_ref, z_ref, dfull, mfull, do_ref, dw2_ref,
               mbuf, zv, ut, yv, obuf, own_sem, m_sem, load_sem, out_sem, *comm_sems):
    place = Place()
    place.barrier()
    rows, model = dx1_ref.shape
    gather = Gather(place, dx1_ref, mfull, *comm_sems)
    gather.start()
    own_copy = pltpu.make_async_copy(dx1_ref, mfull.at[place.me], own_sem)
    own_copy.start()

    loads = [pltpu.make_async_copy(z_ref, zv, load_sem.at[0]), pltpu.make_async_copy(dfull, yv, load_sem.at[1])]
    for copy in loads:
        copy.start()
    tiles = Tiles(obuf, dw2_ref, out_sem)
    count = model // OUT_TILE

    def turn(n):
        cols = tile_at(n, 256)
        ut[cols, :] = gelu(zv[:, cols].astype(F32)).astype(BF16).T

    def weight_tile(n):
        cols = tile_at(n, OUT_TILE)
        tiles.put(n, lambda: dot(ut[...], flat_cols(yv, cols)))

    loads[0].wait()
    loop(ut.shape[DIM0] // 256, turn)
    gather.relay()
    loads[1].wait()
    loop(count, weight_tile)
    gather.forward('X')
    gather.forward('Y')
    own_copy.wait()
    gather.links.wait('CO')

    def grad_ctx(i):
        @pl.when(i == 1)
        def _():
            gather.links.wait('CY')

        @pl.when(i == 2)
        def _():
            gather.links.wait('CX')

        @pl.when(i == 3)
        def _():
            gather.forward('D')
            gather.links.wait('CD')

        pair = place.pair_at(3 - i)
        copy = pltpu.make_async_copy(mfull.at[pl.ds(2 * pair, 2)], mbuf, m_sem)
        copy.start()
        copy.wait()
        do_ref[:, tile_at(pair, 2 * rows)] = dot_t(wo_ref[...], mbuf[...].reshape(2 * rows, model)).astype(BF16)

    loop(4, grad_ctx)
    tiles.finish(count)
    gather.links.finish()


def ctx_call(dx1, w_rows, z_saved, dfull):
    rows, model = dx1.shape
    feats = w_rows.shape[DIM0]
    seq, hidden = z_saved.shape
    return comm_call(
        ctx_kernel, "ctx_grads", 2, 30_000_000_000, (dx1, w_rows, z_saved, dfull), [VMEM] * 2 + [HBM] * 2,
        [shape((seq // rows, rows, model), BF16), shape((feats, seq), BF16), shape((hidden, model), F32)], [HBM, VMEM, HBM],
        [pltpu.VMEM((2, rows, model), BF16), pltpu.VMEM((seq, hidden), BF16), pltpu.VMEM((hidden, seq), BF16),
         pltpu.VMEM((seq // rows, rows, model), BF16), pltpu.VMEM((2, hidden, OUT_TILE), F32),
         DMA(()), DMA(()), PAIR, PAIR] + [COMM] * 2)


def bwd_kernel(h1_ref, q_hbm, k_hbm, v_hbm, do_hbm, wide_hbm, max_ref, inv_ref, dz_ref, h2_in,
               h2full, h1full, qkv_out, dw1_ref,
               k_rows, v_rows, q_rows, do_rows, delta, dq_acc, dk_acc, dv_acc, tok, dzv, wbuf,
               q_ref, k_ref, v_ref, do_ref, wide_ref, out_ref, own_sem, head_sem, load_sem, out_sem, *comm_sems):
    place = Place()
    place.barrier()
    gather1 = ThirdGather(place, h1full, *comm_sems[0:2])
    gather2 = ThirdGather(place, h2full, *comm_sems[2:4])
    gather2.start('rest', None)
    gather2.start('diag', None)
    gather1.start('near', h1_ref)
    gather1.start('rest', h1_ref)
    loads = start_copies(head_sem, (k_hbm, k_ref), (v_hbm, v_ref), (q_hbm, q_ref), (do_hbm, do_ref), (wide_hbm, wide_ref))
    own_copy = pltpu.make_async_copy(h1_ref, h1full.at[place.me], own_sem)
    own_copy.start()
    heads, dim, seq = q_ref.shape
    blocks = seq // BLK
    scale = dim ** -0.5
    exp_scale = scale * LOG2E

    def head(h):
        k_rows[...] = k_ref[h].T
        v_rows[...] = v_ref[h].T
        q_rows[...] = q_ref[h].T
        do_rows[...] = do_ref[h].T
        delta[...] = jnp.sum(do_ref[h].astype(F32) * wide_ref[h], **COLS)
        dq_acc[...] = jnp.zeros_like(dq_acc)
        dk_acc[...] = jnp.zeros_like(dk_acc)
        dv_acc[...] = jnp.zeros_like(dv_acc)

        def block(qi, ki, on_diag):
            q_at, k_at = tile_at(qi, BLK), tile_at(ki, BLK)
            scores = dot(k_rows[k_at, :], q_ref[h, :, q_at])
            if on_diag:
                scores = causal_fill(scores, -1e30)
            probs = jnp.exp2((scores - max_ref[h, :, q_at]) * exp_scale) * inv_ref[h, :, q_at]
            grad_probs = dot(v_rows[k_at, :], do_ref[h, :, q_at])
            dv_acc[k_at, :] += dot(probs.astype(BF16), do_rows[q_at, :])
            grad_scores = (probs * (grad_probs - delta[:, q_at]) * scale).astype(BF16)
            dk_acc[k_at, :] += dot(grad_scores, q_rows[q_at, :])
            dq_acc[:, q_at] += dot(k_ref[h, :, k_at], grad_scores)

        loop(blocks, lambda i: block(i, i, True))
        loop(blocks, lambda ki: loop(blocks, lambda qi: block(qi, ki, False), ki + 1))
        out_ref[0, h] = dq_acc[...].astype(BF16)
        out_ref[1, h] = dk_acc[...].astype(BF16).T
        out_ref[2, h] = dv_acc[...].astype(BF16).T

    load_grad, load_tok = [pltpu.make_async_copy(src, dst, load_sem.at[i])
                           for i, (src, dst) in enumerate(((dz_ref, dzv), (h2full, tok)))]
    for copy in loads:
        copy.wait()
    count = tok.shape[DIM2] // OUT_TILE
    tiles = Tiles(wbuf, dw1_ref, out_sem, rows=True)

    def fc1_tile(n):
        cols = tile_at(n, OUT_TILE)
        tiles.put(n, lambda: dot(flat_cols(tok, cols).T, dzv[...]))

    def head_step(h):
        head(h)

        @pl.when(h == 1)
        def _():
            load_grad.start()
            gather2.forward('rest')

        @pl.when(h == heads - 2)
        def _():
            gather2.forward('diag')
            gather2.wait_pair('rest')

    loop(heads - 1, head_step)
    gather2.wait_pair('diag')
    load_tok.start()
    head(heads - 1)
    load_grad.wait()
    load_tok.wait()
    results = start_copies(head_sem, (out_ref, qkv_out))
    loop(count, fc1_tile)
    for third in ('near', 'rest'):
        gather1.forward(third)
    for third in ('near', 'rest'):
        gather1.wait_pair(third)
    own_copy.wait()
    wait_all(results)
    tiles.finish(count)
    gather1.links.finish()
    gather2.links.finish()


def bwd_call(h1, q_t, k_t, v_t, do_t, wide, row_max, row_inv, dz, h2full):
    heads, dim, seq = q_t.shape
    rows, model = h1.shape
    full = shape((seq // rows, rows, model), BF16)
    turned = pltpu.VMEM((seq, dim), BF16)
    hidden = dz.shape[DIM1]
    return comm_call(
        bwd_kernel, "attn_bwd", 3, 80_000_000_000,
        (h1, q_t, k_t, v_t, do_t, wide, row_max, row_inv, dz, h2full), [VMEM] + [HBM] * 5 + [VMEM] * 2 + [HBM] * 2,
        [full, full, shape((3, heads, dim, seq), BF16), shape((model, hidden), F32)], [HBM] * 4,
        [turned] * 4 + [pltpu.VMEM((1, seq), F32), pltpu.VMEM((dim, seq), F32), pltpu.VMEM((seq, dim), F32),
                        pltpu.VMEM((seq, dim), F32), pltpu.VMEM((seq // rows, rows, model), BF16),
                        pltpu.VMEM((seq, hidden), BF16), pltpu.VMEM((2, OUT_TILE, hidden), F32),
                        *[pltpu.VMEM(q_t.shape, BF16)] * 4, pltpu.VMEM(wide.shape, F32), pltpu.VMEM((3, heads, dim, seq), BF16),
                        DMA(()), DMA((5,)), PAIR, PAIR] + [COMM] * 4,
        aliases={9: 0})


def qkv_kernel(qkv_hbm, w_hbm, dx1_hbm, x_hbm, gain_ref, vec_ref, ctx_hbm, mfull, h1_in,
               dx_ref, vsum_ref, bias_ref, dwo_ref, dw_ref, h1full,
               turned, part, crecv, diag_recv, last_recv, vacc, vsend, vrecv, last_got, tok, obuf, wbuf,
               qkv_ref, w_ref, dx1_ref, x_ref, ctx_ref, vsem, last_sem, load_sem, in_sem, out_sem, *comm_sems):
    place = Place()
    place.barrier(everyone=True)
    rows, model = dx1_ref.shape
    scatter = Scatter(place, part, crecv, diag_recv, last_recv, *comm_sems[0:2])
    gather = ThirdGather(place, h1full, *comm_sems[2:4])
    gather.start('diag', None)
    inputs = start_copies(in_sem, (qkv_hbm, qkv_ref), (w_hbm, w_ref), (ctx_hbm, ctx_ref), (dx1_hbm, dx1_ref), (x_hbm, x_ref))
    loads = [pltpu.make_async_copy(src, tok, load_sem.at[i]) for i, src in enumerate((mfull, h1full))]
    tiles_o = Tiles(obuf, dwo_ref, out_sem.at[0])
    tiles = Tiles(wbuf, dw_ref, out_sem.at[1])
    count = model // OUT_TILE
    swaps = Links(place, vsem.at[0], vsem.at[1])
    inputs[0].wait()

    def vec_step(i):
        if i > 0:
            swaps.wait('CXY'[i - 1])
            vacc[...] += vrecv[i - 1]
        if i < 3:
            vsend[i] = vacc[...]

    def vec_send(i):
        swaps.send('CXY'[i], 'CXY'[i], vsend, vrecv, i)

    vacc[...] = vec_ref[...]
    vec_step(0)
    vec_send(0)

    def pair_step(i):
        for c in range(4):
            slot, at = place.chunk(i, c)
            turned[tile_at(c, rows // 2), :] = qkv_ref[:, tile_at(2 * slot + at, rows // 2)].T

        @pl.when(i == 0)
        def _():
            inputs[1].wait()

        @pl.when(i == 1)
        def _():
            loads[0].start()

        @pl.when(i == 3)
        def _():
            gather.forward('diag')

        for at in range(1, 3):
            @pl.when(i == at)
            def _():
                vec_step(at)
                vec_send(at)

        scatter.between(i)

        def grad_norm(n):
            cols = tile_at(n, TILE)
            scatter.store(i, cols, dot(turned[...], w_ref[:, cols]).astype(BF16))

        loop(model // TILE, grad_norm)
        scatter.after(i)

    loop(4, pair_step)
    loads[0].wait()
    for copy in inputs[2:]:
        copy.wait()

    def proj_tile(n):
        cols = tile_at(n, OUT_TILE)
        tiles_o.put(n, lambda: dot(ctx_ref[...], flat_cols(tok, cols)))

    def qkv_tile(n):
        cols = tile_at(n, OUT_TILE)
        tiles.put(n, lambda: dot(qkv_ref[...], flat_cols(tok, cols)))

    loop(count, proj_tile)
    scatter.add_diag()
    gather.wait_pair('diag')
    loads[1].start()
    ones = jnp.ones((8, qkv_ref.shape[DIM1]), BF16)
    kinds, heads, dim = bias_ref.shape
    for row in range(kinds * heads):
        feats = qkv_ref[row * dim:(row + 1) * dim, :]
        bias_ref[row // heads, row % heads, :] = dot_t(ones, feats)[0]
    loads[1].wait()
    loop(count, qkv_tile)
    vec_step(3)
    tiles_o.finish(count)
    gain = gain_ref[...].reshape(1, model)

    def norm_rows(at):
        grad = scatter.total(at)
        x_hat, inv_std = layer_norm_hat(x_ref[at, :].astype(F32))
        dx_ref[at, :] = (dx1_ref[at, :].astype(F32) + layer_norm_bwd(grad, x_hat, inv_std, gain)).astype(BF16)
        vacc[0:1, :] += jnp.sum(grad * x_hat, **COLS)
        vacc[1:2, :] += jnp.sum(grad, **COLS)

    scatter.norm_loop(norm_rows)
    finals = Links(place, last_sem.at[0], last_sem.at[1])
    last_got[0] = vacc[0:2, :]
    vsum_ref[2:6, :] = vacc[2:6, :]
    for k in range(1, 8):
        finals.send(k, k, (last_got, (0,)), (last_got, (k,)))
    tiles.finish(count)
    finals.wait(*range(1, 8))
    total = last_got[place.me]
    for source in range(1, 8):
        total += last_got[(place.me + 8 - source) % 8]
    vsum_ref[0:2, :] = total
    for links in (swaps, finals, scatter.links, gather.links):
        links.finish()


def qkv_call(heads, qkv_rows, w_rows, dx1, x_in, gain, vec, ctx_rows, mfull, h1full):
    rows, model = dx1.shape
    feats, seq = qkv_rows.shape
    proj = ctx_rows.shape[DIM0]
    return comm_call(
        qkv_kernel, "qkv_grads", 4, 30_000_000_000,
        (qkv_rows, w_rows, dx1, x_in, gain, vec, ctx_rows, mfull, h1full), [HBM] * 4 + [VMEM] * 2 + [HBM] * 3,
        [shape((rows, model), BF16), shape((6, model), F32), shape((3, heads, feats // (3 * heads)), F32), shape((proj, model), F32),
         shape((feats, model), F32), shape(h1full.shape, BF16)],
        [VMEM] * 3 + [HBM] * 3,
        [pltpu.VMEM((2 * rows, feats), BF16)] + scatter_scratch(rows, model)
        + [pltpu.VMEM((8, model), F32), pltpu.VMEM((3, 8, model), F32), pltpu.VMEM((3, 8, model), F32),
           pltpu.VMEM((8, 2, model), F32), pltpu.VMEM((8, rows, model), BF16),
           pltpu.VMEM((2, proj, OUT_TILE), F32), pltpu.VMEM((2, feats, OUT_TILE), F32),
           pltpu.VMEM((feats, seq), BF16), pltpu.VMEM((feats, model), BF16), pltpu.VMEM((rows, model), BF16),
           pltpu.VMEM((rows, model), BF16), pltpu.VMEM((proj, seq), BF16),
           DMA((2, 3)), DMA((2, 7)), PAIR, DMA((5,)), DMA((2, 2))] + [COMM] * 4,
        aliases={8: 5})


def finish_kernel(*refs):
    count = len(refs) // 3
    refs[2 * count - 1][...] = refs[count - 1][...].reshape(refs[2 * count - 1].shape)
    rings, single, (small_sem, in_sem, out_sem) = refs[2 * count:2 * count + 2], refs[2 * count + 2:-3], refs[-3:]
    chunks, used = [], [0, 0]
    small = [(src, buf, dst) for src, buf, dst in zip(refs[4:count - 1], single, refs[count + 4:2 * count - 1])]
    for i, (src, buf, _) in enumerate(small):
        pltpu.make_async_copy(src, buf, small_sem.at[0, i]).start()
    for src, dst in zip(refs[:4], refs[count:count + 4]):
        kind = 0 if src.shape[DIM1] == rings[0].shape[DIM2] else 1
        rows = rings[kind].shape[DIM1]
        for row in range(0, src.shape[DIM0], rows):
            chunks.append((src.at[pl.ds(row, rows)], dst.at[pl.ds(row, rows)], kind, used[kind]))
            used[kind] += 1

    def copy_in(src, dst, kind, at):
        slot = at % RING
        return pltpu.make_async_copy(src, rings[kind].at[slot], in_sem.at[kind, slot])

    def copy_out(src, dst, kind, at):
        slot = at % RING
        return pltpu.make_async_copy(rings[kind].at[slot], dst, out_sem.at[kind, slot])

    waiting = {}

    def start(chunk):
        key = (chunk[2], chunk[3] % RING)
        if key in waiting:
            copy_out(*waiting.pop(key)).wait()
        copy_in(*chunk).start()

    for chunk in chunks[:AHEAD]:
        start(chunk)
    for i, (src, buf, dst) in enumerate(small):
        pltpu.make_async_copy(src, buf, small_sem.at[0, i]).wait()
        pltpu.make_async_copy(buf, dst, small_sem.at[1, i]).start()
    for i, chunk in enumerate(chunks):
        copy_in(*chunk).wait()
        copy_out(*chunk).start()
        waiting[(chunk[2], chunk[3] % RING)] = chunk
        if i + AHEAD < len(chunks):
            start(chunks[i + AHEAD])
    for chunk in waiting.values():
        copy_out(*chunk).wait()
    for i, (_, buf, dst) in enumerate(small):
        pltpu.make_async_copy(buf, dst, small_sem.at[1, i]).wait()


RING = 16
AHEAD = 24


def finish_call(*arrays):
    wide = max(a.shape[DIM1] for a in arrays[:4])
    narrow = min(a.shape[DIM1] for a in arrays[:4])
    small = [pltpu.VMEM(a.shape, a.dtype) for a in arrays[4:-1]]
    return pl.pallas_call(
        finish_kernel, name="finish", in_specs=[HBM] * (len(arrays) - 1) + [VMEM], out_specs=[HBM] * (len(arrays) - 1) + [VMEM],
        out_shape=[shape(a.shape, a.dtype) for a in arrays[:-1]] + [shape(arrays[-1].shape[1:], F32)],
        scratch_shapes=[pltpu.VMEM((RING, 160, wide), F32), pltpu.VMEM((RING, 320, narrow), F32), *small,
                        DMA((2, len(small))), DMA((2, RING)), DMA((2, RING))],
        compiler_params=pltpu.CompilerParams(vmem_limit_bytes=66_000_000),
        cost_estimate=pl.CostEstimate(flops=1_000_000, bytes_accessed=72_000_000, transcendentals=0),
    )(*arrays)


def solution(mesh):
    def local_backward(x_in, x_mid, d_out, q_saved, k_saved, v_saved, z_saved, ln1_gain, ln1_bias, ln2_gain, ln2_bias, w_qkv, w_proj, w_fc1, w_fc2):
        x_in, x_mid, d_out, z_saved = x_in[0], x_mid[0], d_out[0], z_saved[0]
        heads, dim = q_saved.shape[2:]
        seq, model = z_saved.shape[DIM0], x_in.shape[DIM1]
        q_t, k_t, v_t = (v[0].transpose(1, 2, 0) for v in (q_saved, k_saved, v_saved))
        affine = (ln1_gain, ln1_bias, ln2_gain, ln2_bias)
        dfull, ctx_t, wide_t, row_max, row_inv, h1_local, h2_local = fwd_call(d_out, q_t, k_t, v_t, x_in, x_mid, affine)
        dx1, grad_pre, grad_bfc1, vec, h2_full = mlp_call(dfull, d_out, x_mid, ln2_gain, h2_local, z_saved, w_fc2, w_fc1)
        mfull, do_t, grad_wfc2 = ctx_call(dx1, w_proj.reshape(heads * dim, model), z_saved, dfull)
        _, h1_full, qkv_t, grad_wfc1 = bwd_call(
            h1_local, q_t, k_t, v_t, do_t.reshape(heads, dim, seq), wide_t, row_max, row_inv, grad_pre, h2_full)
        qkv_rows = qkv_t.reshape(3 * heads * dim, seq)
        w_rows = w_qkv.transpose(0, 2, 3, 1).reshape(3 * heads * dim, model)
        grad_x, grad_vecs, grad_bqkv, grad_wproj, grad_wqkv, _ = qkv_call(
            heads, qkv_rows, w_rows, dx1, x_in, ln1_gain, vec, ctx_t.reshape(heads * dim, seq), mfull, h1_full)
        grad_wfc2, grad_wfc1, grad_wqkv, grad_wproj, grad_x, grad_vecs, grad_bqkv, grad_bfc1 = finish_call(
            grad_wfc2, grad_wfc1, grad_wqkv, grad_wproj, grad_x, grad_vecs, grad_bqkv, grad_bfc1)
        grad_wproj = grad_wproj.reshape(heads, dim, model)
        grad_wqkv = grad_wqkv.reshape(3, heads, dim, model).transpose(0, 3, 1, 2)
        return grad_x[None], grad_wqkv, grad_bqkv, grad_wproj, grad_wfc1, grad_bfc1, grad_wfc2, grad_vecs

    tok_spec = P('dp', 'tp', None)
    head_spec = P('dp', None, 'tp', None)
    in_specs = (tok_spec, tok_spec, tok_spec, head_spec, head_spec, head_spec, P('dp', None, 'tp'),
                P(None), P(None), P(None), P(None),
                P(None, None, 'tp', None), P('tp', None, None), P(None, 'tp'), P('tp', None))
    out_specs = (tok_spec, P('dp', None, 'tp', None), P('dp', 'tp', None), P(('dp', 'tp'), None, None),
                 P('dp', 'tp'), P(('dp', 'tp')), P(('dp', 'tp'), None), P('dp', None))
    return jax.shard_map(local_backward, mesh=mesh, in_specs=in_specs, out_specs=out_specs, check_vma=False)
```
